128 devices in a mesh: seq: 32 (over z, y, core), head: 4 (over x).
Axes of the slice: x: 4, y: 4, z: 4, core: 2. Of those that a mesh axis runs over, the one named last changes fastest.
Arguments:
- tokens: bfloat16 [16384, 2560], P('seq'), may hold values from -6 to 6
- proj_inner: bfloat16 [2560, 5120], P(None, 'head'), may hold values from -0.125 to 0.125
- proj_gate: bfloat16 [2560, 5120], P(None, 'head'), may hold values from -0.125 to 0.125
- proj_bc: bfloat16 [2560, 256], replicated, may hold values from -0.03125 to 0.03125
- proj_step: bfloat16 [2560, 80], P(None, 'head'), may hold values from -0.125 to 0.125
- conv_inner: float32 [4, 5120], P(None, 'head'), may hold values from -3 to 3
- conv_bc: float32 [4, 256], replicated, may hold values from -3 to 3
- offset_inner: float32 [5120], P('head'), may hold values from -3 to 3
- offset_bc: float32 [256], replicated, may hold values from -1.2 to 1.2
- step_bias: float32 [80], P('head'), as said below
- decay_log: float32 [80], P('head'), as said below
- skip_gain: float32 [80], P('head'), may hold values from 0.5 to 2
- norm_weight: float32 [5120], P('head'), may hold values from 0.25 to 1.75
- out_weight: bfloat16 [5120, 2560], P('head'), may hold values from -0.078125 to 0.078125
Outputs:
- layer_out: bfloat16 [16384, 2560], P(('seq', 'head'))
The draws below stay inside these ranges and needn't reach their ends.
Inputs may be any that keep to these rules, and one draw needn't show every extreme that they name: step_bias holds one value for each head, the same for every token. decay_log holds one value for each head, the same for every token.
All inputs are finite; a program needn't handle non-finite values.
Results may differ from the reference program's by a relative error of at most 0.013.
Values may be sent and summed in bfloat16 or wider, within the bound.
No kernel may reach another device: no remote copies, remote signals or barrier semaphores. Data moves between devices by JAX's collectives and lax.ppermute only.
A program may use at most 128 MiB of HBM per device.

```python
import jax
import jax.numpy as jnp
from jax import lax

D = 2560
HEADS = 80
HEADDIM = 64
STATE = 128
KERNEL = 4
SPAN = 128
INNER = 5120
TOKENS = 16384


def head_tables(key):
    ranking = jax.random.permutation(jax.random.fold_in(key, 7), HEADS)
    jitter = jax.random.uniform(jax.random.fold_in(key, 11), (HEADS,), jnp.float32, -0.3, 0.3)
    slow_count = HEADS // 2
    slow_heads = ranking < slow_count
    step_target = jnp.where(slow_heads, 8.0 / TOKENS, 0.1)
    decay_target = jnp.where(slow_heads, 1.0 / TOKENS, 1.0 / 40.0)
    return (step_target, decay_target, jitter)


def draw_step_bias(key, part):
    step_target, decay_target, jitter = head_tables(key)
    return (jnp.log(jnp.expm1(step_target)) + jitter).astype(jnp.float32)


def draw_decay_log(key, part):
    step_target, decay_target, jitter = head_tables(key)
    actual_step = jnp.log1p(jnp.exp(jnp.log(jnp.expm1(step_target)) + jitter))
    return (jnp.log(decay_target) - jnp.log(actual_step) - 0.5).astype(jnp.float32)


def steps_of(own_key, dims, cuts, smallest, largest):
    def one(axis_at, blocks):
        steps = jax.random.uniform(jax.random.fold_in(jax.random.fold_in(own_key, 6), axis_at), (blocks,), jnp.float32, smallest / len(cuts), largest / len(cuts))
        return jnp.repeat(jnp.exp(steps), dims[axis_at] // blocks).reshape((-1,) + (1,) * (len(dims) - axis_at - 1))

    loudness = one(*cuts[0])
    for cut in cuts[1:]:
        loudness = loudness * one(*cut)
    return loudness


def normal_values(stream_key, shape, scale, limit, cuts=(), held_as=jnp.bfloat16):
    values = jax.random.normal(stream_key, shape, jnp.float32) * scale
    if len(cuts) > 0:
        values = steps_of(stream_key, shape, cuts, -0.22, 0.18) * values
    return jnp.clip(values, min=-limit, max=limit).astype(held_as)


def setup_inputs(seed: int = 0) -> dict:
    keys = jax.random.split(jax.random.key(seed), 15)
    return {
        "tokens": normal_values(keys[0], (TOKENS, D), 1.0, 6.0, ((0, 32),)),
        "proj_inner": normal_values(keys[1], (D, INNER), D ** -0.5, 0.125, ((1, 4),)),
        "proj_gate": normal_values(keys[2], (D, INNER), D ** -0.5, 0.125, ((1, 4),)),
        "proj_bc": normal_values(keys[3], (D, 2 * STATE), (16 * D) ** -0.5, 0.03125),
        "proj_step": normal_values(keys[4], (D, HEADS), D ** -0.5, 0.125, ((1, 4),)),
        "conv_inner": normal_values(keys[5], (KERNEL, INNER), KERNEL ** -0.5, 3.0, ((1, 4),), jnp.float32),
        "conv_bc": normal_values(keys[6], (KERNEL, 2 * STATE), KERNEL ** -0.5, 3.0, (), jnp.float32),
        "offset_inner": normal_values(keys[7], (INNER,), 0.5, 3.0, ((0, 4),), jnp.float32),
        "offset_bc": normal_values(keys[8], (2 * STATE,), 0.2, 1.2, (), jnp.float32),
        "step_bias": draw_step_bias(jax.random.fold_in(keys[14], 71), 0),
        "decay_log": draw_decay_log(jax.random.fold_in(keys[14], 71), 0),
        "skip_gain": jnp.clip(0.5 + 1.5 * jax.random.uniform(keys[11], (HEADS,), jnp.float32) ** steps_of(keys[11], (HEADS,), ((0, 4),), -0.2, 0.2), 0.5, 2.0),
        "norm_weight": jnp.clip(1.0 + 0.15 * jax.random.normal(keys[12], (INNER,), jnp.float32), 0.25, 1.75),
        "out_weight": normal_values(keys[13], (INNER, D), INNER ** -0.5, 0.078125, ((0, 4),)),
    }


def causal(padded, weight, offset, length):
    summed = jnp.zeros((length, weight.shape[1]), jnp.float32) + offset.astype(jnp.float32)[None, :]
    for tap_index in range(weight.shape[0]):
        summed = summed + weight[tap_index].astype(jnp.float32)[None, :] * padded[tap_index:tap_index + length].astype(jnp.float32)
    return jax.nn.silu(summed).astype(jnp.bfloat16)

def within_span(inner_c, write_c, read_c, step_c, cum_c):
    scores = jnp.dot(read_c, write_c.T, preferred_element_type=jnp.float32)
    cum_t = cum_c.T
    step_t = step_c.T
    log_gaps = cum_t[:, :, None] - cum_t[:, None, :]
    causal_mask = jnp.tril(jnp.ones((cum_c.shape[0], cum_c.shape[0]), bool))[None]
    decays = jnp.where(causal_mask, jnp.exp(jnp.where(causal_mask, log_gaps, 0.0)), 0.0)
    weights = (scores[None] * decays * step_t[:, None, :]).astype(jnp.bfloat16)
    return jnp.einsum('hij,jhp->ihp', weights.astype(jnp.float32), inner_c.astype(jnp.float32))

def reference(tokens, proj_inner, proj_gate, proj_bc, proj_step, conv_inner, conv_bc, offset_inner, offset_bc, step_bias, decay_log, skip_gain, norm_weight, out_weight):
    tok_rows = tokens.shape[0]
    inner_raw = jnp.dot(tokens, proj_inner, preferred_element_type=jnp.float32).astype(jnp.bfloat16)
    gate_raw = jnp.dot(tokens, proj_gate, preferred_element_type=jnp.float32).astype(jnp.bfloat16)
    bc_raw = jnp.dot(tokens, proj_bc, preferred_element_type=jnp.float32).astype(jnp.bfloat16)
    step_raw = jnp.dot(tokens, proj_step, preferred_element_type=jnp.float32)
    zeros_inner = jnp.zeros((KERNEL - 1, inner_raw.shape[1]), jnp.bfloat16)
    zeros_bc = jnp.zeros((KERNEL - 1, bc_raw.shape[1]), jnp.bfloat16)
    inner_conv = causal(jnp.concatenate([zeros_inner, inner_raw], 0), conv_inner, offset_inner, tok_rows)
    bc_conv = causal(jnp.concatenate([zeros_bc, bc_raw], 0), conv_bc, offset_bc, tok_rows)
    step_sizes = jax.nn.softplus(step_raw + step_bias[None, :])
    log_decay = -jnp.exp(decay_log)[None, :] * step_sizes
    span_total = tok_rows // SPAN
    inner_blocks = inner_conv.reshape(span_total, SPAN, HEADS, HEADDIM)
    write_blocks = bc_conv[:, :STATE].reshape(span_total, SPAN, STATE)
    read_blocks = bc_conv[:, STATE:].reshape(span_total, SPAN, STATE)
    step_blocks = step_sizes.reshape(span_total, SPAN, HEADS)
    cumulative = jnp.cumsum(log_decay.reshape(span_total, SPAN, HEADS), axis=1)

    def advance(carried, pieces):
        inner_c, write_c, read_c, step_c, cum_c = pieces
        intra_out = within_span(inner_c, write_c, read_c, step_c, cum_c)
        inter_out = jnp.exp(cum_c)[:, :, None] * jnp.einsum('in,hnp->ihp', read_c.astype(jnp.float32), carried, precision=lax.Precision.HIGHEST)
        end_weights = jnp.exp(cum_c[-1][None, :] - cum_c) * step_c
        local_states = jnp.einsum('jn,jh,jhp->hnp', write_c.astype(jnp.float32), end_weights, inner_c.astype(jnp.float32), precision=lax.Precision.HIGHEST)
        carried = jnp.exp(cum_c[-1])[:, None, None] * carried + local_states
        return (carried, intra_out + inter_out)
    start_state = jnp.zeros((HEADS, STATE, HEADDIM), jnp.float32)
    _, outputs = lax.scan(advance, start_state, (inner_blocks, write_blocks, read_blocks, step_blocks, cumulative))
    mixed_out = outputs.reshape(tok_rows, HEADS, HEADDIM) + skip_gain[None, :, None] * inner_conv.reshape(tok_rows, HEADS, HEADDIM).astype(jnp.float32)
    gated_pre = mixed_out.reshape(tok_rows, HEADS * HEADDIM) * jax.nn.silu(gate_raw.astype(jnp.float32))
    squares = lax.optimization_barrier(jnp.sum(gated_pre * gated_pre, axis=1))
    scale = 1.0 / jnp.sqrt(squares / (HEADS * HEADDIM) + 0.25)
    gated_out = (gated_pre * scale[:, None] * norm_weight[None, :]).astype(jnp.bfloat16)
    return jnp.dot(gated_out, out_weight, preferred_element_type=jnp.float32).astype(jnp.bfloat16)
```

```python
import functools

import jax
import jax.numpy as jnp
from jax import lax
from jax.experimental import pallas as pl
from jax.experimental.pallas import tpu as pltpu
from jax.sharding import Mesh
from jax.sharding import PartitionSpec as P

HEADS = 80
HEADDIM = 64
STATE = 128
KERNEL = 4
SPAN = 128
LANES = 128
EDGE = 8
BLOCK = 256
SEQ = ("seq_0", "seq_1", "seq_2")
SEQ_HEAD = ("seq_0", "seq_1", "seq_2", "head")

F32 = jnp.float32
BF16 = jnp.bfloat16


def dot(a, b):
    return jnp.dot(a, b, preferred_element_type=F32)


def silu(v):
    return v * (0.5 + 0.5 * jnp.tanh(0.5 * v))


def lane_pair(first, second):
    lane = lax.broadcasted_iota(jnp.int32, (first.shape[0], LANES), 1)
    return jnp.where(lane < HEADDIM, first, second)


def front_kernel(
    tok, edge, w_bc, w_step, w_in, taps, offset, taps_bc, offset_bc, step_bias, decay_log,
    x_out, bc_out, cum_out, dt_out, lead_out, local_out, prior_out, decay_out,
    padded, end_w, span_d, write_t,
):
    step = pl.program_id(0)
    rows = tok.shape[0]
    spans = rows // SPAN
    heads = step_bias.shape[1]
    per = BLOCK // HEADDIM
    groups = heads // per

    def conv(weight, tap, off):
        padded[EDGE:, :] = dot(tok[...], weight).astype(BF16).astype(F32)
        padded[:EDGE, :] = dot(edge[...], weight).astype(BF16).astype(F32)
        total = off + tap[0:1, :] * padded[EDGE - 3 : EDGE - 3 + rows, :]
        for k in range(1, KERNEL):
            total = total + tap[k : k + 1, :] * padded[EDGE - 3 + k : EDGE - 3 + k + rows, :]
        return silu(total).astype(BF16)

    @pl.when(step == 0)
    def _():
        bc = conv(w_bc[...], taps_bc, offset_bc[...])
        bc_out[...] = bc
        for s in range(spans):
            block = bc[s * SPAN : (s + 1) * SPAN, :STATE].astype(F32)
            write_t[s] = jnp.transpose(block).astype(BF16)
        v = dot(tok[...], w_step[...]) + step_bias[...]
        dt = jnp.maximum(v, 0.0) + jnp.log1p(jnp.exp(-jnp.abs(v)))
        log_decay = -jnp.exp(decay_log[...]) * dt
        cum_out[...] = jnp.zeros_like(cum_out)
        dt_out[...] = jnp.zeros_like(dt_out)
        lead_out[...] = jnp.zeros_like(lead_out)
        dt_out[:, :heads] = dt
        row = lax.broadcasted_iota(jnp.int32, (SPAN, SPAN), 0)
        col = lax.broadcasted_iota(jnp.int32, (SPAN, SPAN), 1)
        lower = (row >= col).astype(F32)
        lead = jnp.zeros((1, heads), F32)
        for s in range(spans):
            at = slice(s * SPAN, (s + 1) * SPAN)
            cum = jnp.dot(
                lower, log_decay[at], preferred_element_type=F32, precision=lax.Precision.HIGHEST
            )
            cum_out[at, :heads] = cum
            lead_out[at, :heads] = jnp.exp(cum + lead)
            last = cum[SPAN - 1 :, :]
            lead = lead + last
            ends = jnp.exp(last - cum) * dt[at]
            gone = jnp.exp(last)
            for g in range(groups):
                end_w[g, at, :per] = ends[:, g * per : (g + 1) * per]
                span_d[g, s : s + 1, :per] = gone[:, g * per : (g + 1) * per]
        total = jnp.exp(lead)
        for g in range(groups):
            span_d[g, spans : spans + 1, :per] = total[:, g * per : (g + 1) * per]

    @pl.when(step > 0)
    def _():
        g = step - 1
        x = conv(w_in[...], taps, offset[...])
        x_out[...] = x
        ends = end_w[g]
        gone = span_d[g]
        wide = jnp.concatenate(
            [lane_pair(ends[:, t : t + 1], ends[:, t + 1 : t + 2]) for t in range(0, per, 2)], axis=1
        )
        gone_wide = jnp.concatenate(
            [lane_pair(gone[:, t : t + 1], gone[:, t + 1 : t + 2]) for t in range(0, per, 2)], axis=1
        )
        weighted = (x.astype(F32) * wide).astype(BF16)
        running = jnp.zeros((STATE, BLOCK), F32)
        tiles = BLOCK // LANES
        for s in range(spans):
            if s > 0:
                for t in range(tiles):
                    prior_out[s - 1, t] = running[:, t * LANES : (t + 1) * LANES].astype(BF16)
            local = dot(write_t[s], weighted[s * SPAN : (s + 1) * SPAN])
            running = gone_wide[s : s + 1] * running + local
        for t in range(tiles):
            local_out[t] = running[:, t * LANES : (t + 1) * LANES].astype(BF16)
            decay_out[t] = jnp.broadcast_to(
                gone_wide[spans : spans + 1, t * LANES : (t + 1) * LANES], (8, LANES)
            )


def front(tokens, edge, w_bc, w_step, w_in, taps, offset, taps_bc, offset_bc, step_bias, decay_log):
    rows, width = tokens.shape
    channels = w_in.shape[1]
    heads = step_bias.shape[1]
    groups = channels // BLOCK
    spans = rows // SPAN
    tiles = channels // LANES
    per_block = BLOCK // LANES

    def whole(a):
        return pl.BlockSpec(a.shape, lambda i: (0,) * a.ndim)

    def late(shape, dim):
        return pl.BlockSpec(
            shape,
            lambda i: tuple(jnp.maximum(i - 1, 0) if d == dim else 0 for d in range(len(shape))),
        )

    head_shape = jax.ShapeDtypeStruct((rows, LANES), F32)
    head_spec = pl.BlockSpec((rows, LANES), lambda i: (0, 0))
    return pl.pallas_call(
        front_kernel,
        grid=(groups + 1,),
        in_specs=[
            whole(tokens), whole(edge), whole(w_bc), whole(w_step),
            late((width, BLOCK), 1), late((KERNEL, BLOCK), 1), late((1, BLOCK), 1),
            whole(taps_bc), whole(offset_bc), whole(step_bias), whole(decay_log),
        ],
        out_specs=[
            late((rows, BLOCK), 1),
            pl.BlockSpec((rows, 2 * STATE), lambda i: (0, 0)),
            head_spec, head_spec, head_spec,
            late((per_block, STATE, LANES), 0),
            late((spans - 1, per_block, STATE, LANES), 1),
            late((per_block, 8, LANES), 0),
        ],
        out_shape=[
            jax.ShapeDtypeStruct((rows, channels), BF16),
            jax.ShapeDtypeStruct((rows, 2 * STATE), BF16),
            head_shape, head_shape, head_shape,
            jax.ShapeDtypeStruct((tiles, STATE, LANES), BF16),
            jax.ShapeDtypeStruct((spans - 1, tiles, STATE, LANES), BF16),
            jax.ShapeDtypeStruct((tiles, 8, LANES), F32),
        ],
        scratch_shapes=[
            pltpu.VMEM((rows + EDGE, BLOCK), F32),
            pltpu.VMEM((groups, rows, LANES), F32),
            pltpu.VMEM((groups, 8, LANES), F32),
            pltpu.VMEM((spans, STATE, SPAN), BF16),
        ],
        compiler_params=pltpu.CompilerParams(vmem_limit_bytes=28 * 2**20),
        cost_estimate=pl.CostEstimate(
            flops=2 * rows * width * (channels + 2 * STATE + LANES),
            bytes_accessed=2 * width * (rows + channels + 2 * STATE),
            transcendentals=rows * channels,
        ),
        name="front",
    )(tokens, edge, w_bc, w_step, w_in, taps, offset, taps_bc, offset_bc, step_bias, decay_log)


def inside_kernel(first, x_ref, bc_ref, cum_ref, dt_ref, prior_ref, skip_ref, out_ref):
    tiles = x_ref.shape[1] // LANES
    write = bc_ref[:, :STATE]
    read = bc_ref[:, STATE:]
    scores = lax.dot_general(read, write, (((1,), (1,)), ((), ())), preferred_element_type=F32)
    row = lax.broadcasted_iota(jnp.int32, (SPAN, SPAN), 0)
    col = lax.broadcasted_iota(jnp.int32, (SPAN, SPAN), 1)
    scores = jnp.where(row >= col, scores, 0.0)
    cum = cum_ref[...]
    cum_t = jnp.transpose(cum)
    dt_t = jnp.transpose(dt_ref[...])
    grown = jnp.exp(cum)
    lane = lax.broadcasted_iota(jnp.int32, (SPAN, LANES), 1)
    for t in range(tiles):
        at = slice(t * LANES, (t + 1) * LANES)
        x = x_ref[:, at]
        both = []
        for h in (2 * t, 2 * t + 1):
            gap = jnp.minimum(cum[:, h : h + 1] - cum_t[h : h + 1, :], 0.0)
            both.append((scores * jnp.exp(gap) * dt_t[h : h + 1, :]).astype(BF16))
        zero = jnp.zeros_like(x)
        stacked = jnp.concatenate(
            [jnp.where(lane < HEADDIM, x, zero), jnp.where(lane < HEADDIM, zero, x)], axis=0
        )
        total = dot(jnp.concatenate(both, axis=1), stacked)
        total = total + skip_ref[:, at] * x.astype(F32)
        if not first:
            scale = jnp.where(
                lane < HEADDIM, grown[:, 2 * t : 2 * t + 1], grown[:, 2 * t + 1 : 2 * t + 2]
            )
            total = total + scale * dot(read, prior_ref[0, t])
        out_ref[:, at] = total


def inside(span, x, bc, cum, dt, prior, skip):
    channels = x.shape[1]
    tiles = channels // LANES
    at = lambda i: (span, 0)
    return pl.pallas_call(
        functools.partial(inside_kernel, span == 0),
        grid=(1,),
        in_specs=[
            pl.BlockSpec((SPAN, channels), at),
            pl.BlockSpec((SPAN, 2 * STATE), at),
            pl.BlockSpec((SPAN, LANES), at),
            pl.BlockSpec((SPAN, LANES), at),
            pl.BlockSpec((1, tiles, STATE, LANES), lambda i: (max(span - 1, 0), 0, 0, 0)),
            pl.BlockSpec((1, channels), lambda i: (0, 0)),
        ],
        out_specs=pl.BlockSpec((SPAN, channels), lambda i: (0, 0)),
        out_shape=jax.ShapeDtypeStruct((SPAN, channels), F32),
        compiler_params=pltpu.CompilerParams(vmem_limit_bytes=12 * 2**20),
        cost_estimate=pl.CostEstimate(
            flops=1_500_000_000, bytes_accessed=2 * SPAN * channels, transcendentals=0
        ),
        name="inside",
    )(x, bc, cum, dt, prior, skip)


def tail_kernel(
    which, bc_ref, lead_ref, local_ref, gate_ref, state_ref, norm_ref, w_ref,
    left_ref, right_ref, squares_ref, gated,
):
    del which
    n = pl.program_id(1)
    tiles = local_ref.shape[2] // LANES

    @pl.when(n == 0)
    def _():
        read = bc_ref[:, STATE:]
        lead = lead_ref[...]
        squares = jnp.zeros((SPAN, LANES), F32)
        for t in range(tiles):
            at = slice(t * LANES, (t + 1) * LANES)
            scale = lane_pair(lead[:, 2 * t : 2 * t + 1], lead[:, 2 * t + 1 : 2 * t + 2])
            mixed = local_ref[0, :, at] + scale * dot(read, state_ref[t])
            pre = mixed * silu(gate_ref[:, at].astype(F32))
            squares = squares + pre * pre
            gated[:, at] = (pre * norm_ref[:, at]).astype(BF16)
        total = jnp.sum(squares, axis=1, keepdims=True)
        squares_ref[0] = jnp.transpose(jnp.broadcast_to(total, (SPAN, LANES)))[:8]

    part = dot(gated[...], w_ref[...]).astype(BF16)
    half = pl.num_programs(1) // 2

    @pl.when(n < half)
    def _():
        left_ref[0] = part

    @pl.when(n >= half)
    def _():
        right_ref[0] = part


def tail(which, bc, lead, local, gate, state, norm, weight):
    count = which.shape[0]
    channels = local.shape[2]
    width = weight.shape[1]
    tiles = channels // LANES
    parts = 4
    block = width // parts
    half = parts // 2
    at = lambda i, n, w: (w[i], 0)
    fixed = lambda i, n, w: (0, 0)
    side = jax.ShapeDtypeStruct((count, SPAN, width // 2), BF16)
    return pl.pallas_call(
        tail_kernel,
        grid_spec=pltpu.PrefetchScalarGridSpec(
            num_scalar_prefetch=1,
            grid=(count, parts),
            in_specs=[
                pl.BlockSpec((SPAN, 2 * STATE), at),
                pl.BlockSpec((SPAN, LANES), at),
                pl.BlockSpec((1, SPAN, channels), lambda i, n, w: (w[i], 0, 0)),
                pl.BlockSpec((SPAN, channels), at),
                pl.BlockSpec((tiles, STATE, LANES), lambda i, n, w: (0, 0, 0)),
                pl.BlockSpec((1, channels), fixed),
                pl.BlockSpec((channels, block), lambda i, n, w: (0, n)),
            ],
            out_specs=[
                pl.BlockSpec(
                    (1, SPAN, block), lambda i, n, w: (i, 0, jnp.minimum(n, half - 1))
                ),
                pl.BlockSpec(
                    (1, SPAN, block), lambda i, n, w: (i, 0, jnp.maximum(n - half, 0))
                ),
                pl.BlockSpec((1, 8, LANES), lambda i, n, w: (i, 0, 0)),
            ],
            scratch_shapes=[pltpu.VMEM((SPAN, channels), BF16)],
        ),
        out_shape=[side, side, jax.ShapeDtypeStruct((count, 8, LANES), F32)],
        compiler_params=pltpu.CompilerParams(vmem_limit_bytes=20 * 2**20),
        cost_estimate=pl.CostEstimate(
            flops=2 * count * SPAN * channels * width,
            bytes_accessed=2 * channels * width,
            transcendentals=0,
        ),
        name="tail",
    )(which, bc, lead, local, gate, state, norm, weight)


def ring(value, axis, distance):
    size = lax.axis_size(axis)
    return lax.ppermute(value, axis, [(i, (i + distance) % size) for i in range(size)])


def onward(value, axis, distance):
    size = lax.axis_size(axis)
    return lax.ppermute(
        value, axis, [(i, i + distance) for i in range(size) if i + distance < size]
    )


def pick(values, index):
    out = values[0]
    for k in range(1, len(values)):
        out = jnp.where(index == k, values[k], out)
    return out


def packed(state, decay):
    tiles = state.shape[0]
    high = decay.astype(BF16)
    low = (decay - high.astype(F32)).astype(BF16)
    spare = jnp.zeros((16 - 2 * tiles, LANES), BF16)
    return jnp.concatenate([state.astype(BF16).reshape(-1, LANES), high, low, spare], 0)


def unpacked(message, tiles):
    rows = message.shape[0] - 16
    state = message[:rows].reshape(tiles, rows // tiles, LANES).astype(F32)
    high = message[rows : rows + tiles].astype(F32)
    low = message[rows + tiles : rows + 2 * tiles].astype(F32)
    return state, (high + low)[:, None, :]


def incoming_state(local, decay):
    z_axis, y_axis, c_axis = SEQ
    z, y, c = (lax.axis_index(a) for a in SEQ)
    ys, zs = lax.axis_size(y_axis), lax.axis_size(z_axis)
    tiles = local.shape[0] // 2
    first = c == 0
    here = jnp.where(first, local[:tiles], local[tiles:])
    there = jnp.where(first, local[tiles:], local[:tiles])
    here_d = jnp.where(first, decay[:tiles], decay[tiles:])
    there_d = jnp.where(first, decay[tiles:], decay[:tiles])

    got = ring(packed(there, there_d), c_axis, 1)
    other, other_d = unpacked(got, tiles)
    here, here_d = here.astype(F32), here_d[:, None, :]
    s0, d0 = jnp.where(first, here, other), jnp.where(first, here_d, other_d)
    s1, d1 = jnp.where(first, other, here), jnp.where(first, other_d, here_d)
    chip, chip_d = d1 * s0 + s1, d0 * d1

    part = STATE // ys
    quarters = [chip[:, q * part : (q + 1) * part] for q in range(ys)]
    sent = [pick(quarters, (y + k) % ys) for k in range(ys)]
    got = [
        unpacked(ring(packed(sent[k], chip_d[:, 0]), y_axis, k), tiles) for k in range(1, ys)
    ]
    by_shift = [(sent[0], chip_d)] + got
    states = [pick([g[0] for g in by_shift], (y - q) % ys) for q in range(ys)]
    decays = [pick([g[1] for g in by_shift], (y - q) % ys) for q in range(ys)]
    plane, plane_d = states[0], decays[0]
    for q in range(1, ys):
        plane, plane_d = decays[q] * plane + states[q], decays[q] * plane_d

    message = packed(plane, plane_d[:, 0])
    got = [unpacked(onward(message, z_axis, k), tiles) for k in range(1, zs)]
    before = jnp.zeros_like(plane)
    for q in range(zs - 1):
        s = pick([g[0] for g in got], z - q - 1)
        d = pick([g[1] for g in got], z - q - 1)
        before = jnp.where(q < z, d * before + s, before)

    prefix = [before]
    for q in range(ys - 1):
        prefix.append(decays[q] * prefix[-1] + states[q])
    sent = [pick(prefix, (y + k) % ys).astype(BF16) for k in range(ys)]
    got = [sent[0]] + [ring(sent[k], y_axis, k) for k in range(1, ys)]
    chip_in = jnp.concatenate([pick(got, (y - q) % ys) for q in range(ys)], axis=1)
    second_in = (d0 * chip_in.astype(F32) + s0).astype(BF16)
    mine = jnp.where(first, chip_in, second_in)
    got = ring(jnp.where(first, second_in, chip_in), c_axis, 1)
    return jnp.concatenate([jnp.where(first, mine, got), jnp.where(first, got, mine)], axis=0)


def per_device(
    tokens,
    proj_inner,
    proj_gate,
    proj_bc,
    proj_step,
    conv_inner,
    conv_bc,
    offset_inner,
    offset_bc,
    step_bias,
    decay_log,
    skip_gain,
    norm_weight,
    out_weight,
):
    rows = tokens.shape[0]
    spans = rows // SPAN
    devices = lax.axis_size(SEQ)
    edge = lax.ppermute(tokens[rows - EDGE :], SEQ, [(i, i + 1) for i in range(devices - 1)])
    gate_raw = dot(tokens, proj_gate).astype(BF16)
    edge, gate_raw = lax.optimization_barrier((edge, gate_raw))
    x, bc, cum, dt, lead, local, prior, decay = front(
        tokens, edge, proj_bc, proj_step, proj_inner, conv_inner, offset_inner[None],
        conv_bc, offset_bc[None], step_bias[None], decay_log[None],
    )
    state = incoming_state(local, decay[:, 0])
    skip = jnp.repeat(skip_gain, HEADDIM)[None]
    inner = jnp.stack([inside(s, x, bc, cum, dt, prior, skip) for s in range(spans)])

    head = lax.axis_index("head")
    size = lax.axis_size("head")
    run = lambda which: tail(
        jnp.stack([(head + k) % size for k in which]).astype(jnp.int32),
        bc, lead, inner, gate_raw, state, norm_weight[None], out_weight,
    )
    far_left, far_right, far_sq = run((2,))
    relay_up = ring(far_left[0], "head", 1)
    relay_down = ring(far_right[0], "head", -1)
    near_left, near_right, near_sq = run((1, 3))
    direct_up = ring(near_right[0], "head", 1)
    direct_down = ring(near_left[1], "head", -1)
    up = ring((near_left[0].astype(F32) + relay_up.astype(F32)).astype(BF16), "head", 1)
    down = ring((near_right[1].astype(F32) + relay_down.astype(F32)).astype(BF16), "head", -1)
    own_left, own_right, own_sq = run((0,))
    squares = (
        own_sq[0, 0]
        + ring(near_sq[0], "head", 1)[0]
        + ring(near_sq[1], "head", -1)[0]
        + ring(far_sq[0], "head", 2)[0]
    )
    scale = lax.rsqrt(squares / (HEADS * HEADDIM) + 0.25)[:, None]
    left = own_left[0].astype(F32) + up.astype(F32) + direct_down.astype(F32)
    right = own_right[0].astype(F32) + direct_up.astype(F32) + down.astype(F32)
    return jnp.concatenate([(left * scale).astype(BF16), (right * scale).astype(BF16)], axis=1)


def solution(mesh):
    torus = Mesh(
        mesh.devices.reshape(4, 4, 2, mesh.shape["head"]), ("seq_0", "seq_1", "seq_2", "head")
    )
    return jax.shard_map(
        per_device,
        mesh=torus,
        in_specs=(
            P(SEQ, None),
            P(None, "head"),
            P(None, "head"),
            P(),
            P(None, "head"),
            P(None, "head"),
            P(),
            P("head"),
            P(),
            P("head"),
            P("head"),
            P("head"),
            P("head"),
            P("head", None),
        ),
        out_specs=P(SEQ_HEAD, None),
        check_vma=False,
    )
```

```python
import functools

import jax
import jax.numpy as jnp
from jax import lax
from jax.experimental import pallas as pl
from jax.experimental.pallas import tpu as pltpu
from jax.sharding import Mesh
from jax.sharding import PartitionSpec as P


HEADS = 80
HEADDIM = 64
STATE = 128
KERNEL = 4
SPAN = 128
LANES = 128
EDGE = 8
BLOCK = 256
SEQ = ("seq_0", "seq_1", "seq_2")
SEQ_HEAD = ("seq_0", "seq_1", "seq_2", "head")

MIB = 2**20
RAW_LIMIT = 60 * MIB
GATE_LIMIT = 40 * MIB
FRONT_LIMIT = 24 * MIB
INSIDE_LIMIT = 8 * MIB
TAIL_LIMIT = 24 * MIB
SMALL_LIMIT = 8 * MIB


F32 = jnp.float32
BF16 = jnp.bfloat16


def dot(a, b):
    return jnp.dot(a, b, preferred_element_type=F32)


def silu(v):
    return v * (0.5 + 0.5 * jnp.tanh(0.5 * v))


def lane_pair(first, second):
    lane = lax.broadcasted_iota(jnp.int32, (first.shape[0], LANES), 1)
    return jnp.where(lane < HEADDIM, first, second)


def raw_kernel(tok, w_bc, w_step, w_in, in_out, bc_out, step_out, edge_out):
    step = pl.program_id(0)
    rows = tok.shape[0]

    @pl.when(step == 0)
    def _():
        bc = dot(tok[...], w_bc[...]).astype(BF16)
        bc_out[...] = bc
        edge_out[...] = bc[rows - EDGE :]
        heads = w_step.shape[0]
        step_out[:, :heads] = lax.dot_general(
            tok[...], w_step[...], (((1,), (1,)), ((), ())), preferred_element_type=F32
        )

    @pl.when(step > 0)
    def _():
        raw = dot(tok[...], w_in[...]).astype(BF16)
        in_out[...] = raw
        edge_out[...] = raw[rows - EDGE :]


def raw_projections(tokens, w_bc, w_step, w_in):
    rows, width = tokens.shape
    channels = w_in.shape[1]
    groups = channels // BLOCK
    before = lambda i: (0, jnp.maximum(i - 1, 0))
    fixed = lambda i: (0, 0)
    return pl.pallas_call(
        raw_kernel,
        grid=(groups + 1,),
        in_specs=[
            pl.BlockSpec(tokens.shape, fixed),
            pl.BlockSpec(w_bc.shape, fixed),
            pl.BlockSpec(w_step.shape, fixed),
            pl.BlockSpec((width, BLOCK), before),
        ],
        out_specs=[
            pl.BlockSpec((rows, BLOCK), before),
            pl.BlockSpec((rows, BLOCK), fixed),
            pl.BlockSpec((rows, LANES), fixed),
            pl.BlockSpec((EDGE, BLOCK), lambda i: (0, i)),
        ],
        out_shape=[
            jax.ShapeDtypeStruct((rows, channels), BF16),
            jax.ShapeDtypeStruct((rows, BLOCK), BF16),
            jax.ShapeDtypeStruct((rows, LANES), F32),
            jax.ShapeDtypeStruct((EDGE, channels + BLOCK), BF16),
        ],
        compiler_params=pltpu.CompilerParams(vmem_limit_bytes=RAW_LIMIT),
        cost_estimate=pl.CostEstimate(
            flops=2 * rows * width * (channels + BLOCK + LANES),
            bytes_accessed=2 * width * (rows + channels + BLOCK),
            transcendentals=0,
        ),
        name="raw",
    )(tokens, w_bc, w_step, w_in)


def gate_kernel(tok, w, out):
    out[...] = dot(tok[...], w[...]).astype(BF16)


def gate_projection(tokens, weight, start, count):
    rows, width = tokens.shape
    block = LANES
    return pl.pallas_call(
        gate_kernel,
        grid=(count // block,),
        in_specs=[
            pl.BlockSpec(tokens.shape, lambda i: (0, 0)),
            pl.BlockSpec((width, block), lambda i: (0, i + start // block)),
        ],
        out_specs=pl.BlockSpec((rows, block), lambda i: (0, i)),
        out_shape=jax.ShapeDtypeStruct((rows, count), BF16),
        compiler_params=pltpu.CompilerParams(vmem_limit_bytes=GATE_LIMIT),
        cost_estimate=pl.CostEstimate(
            flops=2 * rows * width * count,
            bytes_accessed=2 * width * (rows + count),
            transcendentals=0,
        ),
        name="gate",
    )(tokens, weight)


def front_kernel(
    raw_in, raw_bc, raw_step, edge, taps, offset, taps_bc, offset_bc, step_bias, decay_log,
    x_out, bc_out, cum_out, dt_out, lead_out, local_out, prior_out, decay_out,
    padded, end_w, span_d, write_t,
):
    step = pl.program_id(0)
    rows = raw_in.shape[0]
    spans = rows // SPAN
    heads = step_bias.shape[1]
    per = BLOCK // HEADDIM
    groups = heads // per

    def conv(raw, tap, off):
        padded[EDGE:, :] = raw[...].astype(F32)
        padded[:EDGE, :] = edge[...].astype(F32)
        total = off + tap[0:1, :] * padded[EDGE - 3 : EDGE - 3 + rows, :]
        for k in range(1, KERNEL):
            total = total + tap[k : k + 1, :] * padded[EDGE - 3 + k : EDGE - 3 + k + rows, :]
        return silu(total).astype(BF16)

    @pl.when(step == 0)
    def _():
        bc = conv(raw_bc, taps_bc, offset_bc[...])
        bc_out[...] = bc
        for s in range(spans):
            block = bc[s * SPAN : (s + 1) * SPAN, :STATE].astype(F32)
            write_t[s] = jnp.transpose(block).astype(BF16)
        v = raw_step[:, :heads] + step_bias[...]
        dt = jnp.maximum(v, 0.0) + jnp.log1p(jnp.exp(-jnp.abs(v)))
        log_decay = -jnp.exp(decay_log[...]) * dt
        cum_out[...] = jnp.zeros_like(cum_out)
        dt_out[...] = jnp.zeros_like(dt_out)
        lead_out[...] = jnp.zeros_like(lead_out)
        dt_out[:, :heads] = dt
        row = lax.broadcasted_iota(jnp.int32, (SPAN, SPAN), 0)
        col = lax.broadcasted_iota(jnp.int32, (SPAN, SPAN), 1)
        lower = (row >= col).astype(F32)
        lead = jnp.zeros((1, heads), F32)
        for s in range(spans):
            at = slice(s * SPAN, (s + 1) * SPAN)
            cum = jnp.dot(
                lower, log_decay[at], preferred_element_type=F32, precision=lax.Precision.HIGHEST
            )
            cum_out[at, :heads] = cum
            lead_out[at, :heads] = jnp.exp(cum + lead)
            last = cum[SPAN - 1 :, :]
            lead = lead + last
            ends = jnp.exp(last - cum) * dt[at]
            gone = jnp.exp(last)
            for g in range(groups):
                end_w[g, at, :per] = ends[:, g * per : (g + 1) * per]
                span_d[g, s : s + 1, :per] = gone[:, g * per : (g + 1) * per]
        total = jnp.exp(lead)
        for g in range(groups):
            span_d[g, spans : spans + 1, :per] = total[:, g * per : (g + 1) * per]

    @pl.when(step > 0)
    def _():
        g = step - 1
        x = conv(raw_in, taps, offset[...])
        x_out[...] = x
        ends = end_w[g]
        gone = span_d[g]
        wide = jnp.concatenate(
            [lane_pair(ends[:, t : t + 1], ends[:, t + 1 : t + 2]) for t in range(0, per, 2)], axis=1
        )
        gone_wide = jnp.concatenate(
            [lane_pair(gone[:, t : t + 1], gone[:, t + 1 : t + 2]) for t in range(0, per, 2)], axis=1
        )
        weighted = (x.astype(F32) * wide).astype(BF16)
        running = jnp.zeros((STATE, BLOCK), F32)
        tiles = BLOCK // LANES
        for s in range(spans):
            if s > 0:
                for t in range(tiles):
                    prior_out[s - 1, t] = running[:, t * LANES : (t + 1) * LANES].astype(BF16)
            local = dot(write_t[s], weighted[s * SPAN : (s + 1) * SPAN])
            running = gone_wide[s : s + 1] * running + local
        for t in range(tiles):
            local_out[t] = running[:, t * LANES : (t + 1) * LANES].astype(BF16)
            decay_out[t] = jnp.broadcast_to(
                gone_wide[spans : spans + 1, t * LANES : (t + 1) * LANES], (8, LANES)
            )


def front(raw_in, raw_bc, raw_step, edge, taps, offset, taps_bc, offset_bc, step_bias, decay_log):
    rows, channels = raw_in.shape
    groups = channels // BLOCK
    spans = rows // SPAN
    tiles = channels // LANES
    per_block = BLOCK // LANES

    def whole(a):
        return pl.BlockSpec(a.shape, lambda i: (0,) * a.ndim)

    def late(shape, dim):
        return pl.BlockSpec(
            shape,
            lambda i: tuple(jnp.maximum(i - 1, 0) if d == dim else 0 for d in range(len(shape))),
        )

    head_shape = jax.ShapeDtypeStruct((rows, LANES), F32)
    head_spec = pl.BlockSpec((rows, LANES), lambda i: (0, 0))
    return pl.pallas_call(
        front_kernel,
        grid=(groups + 1,),
        in_specs=[
            late((rows, BLOCK), 1), whole(raw_bc), whole(raw_step),
            pl.BlockSpec((EDGE, BLOCK), lambda i: (0, i)),
            late((KERNEL, BLOCK), 1), late((1, BLOCK), 1),
            whole(taps_bc), whole(offset_bc), whole(step_bias), whole(decay_log),
        ],
        out_specs=[
            late((rows, BLOCK), 1),
            pl.BlockSpec((rows, 2 * STATE), lambda i: (0, 0)),
            head_spec, head_spec, head_spec,
            late((per_block, STATE, LANES), 0),
            late((spans - 1, per_block, STATE, LANES), 1),
            late((per_block, 8, LANES), 0),
        ],
        out_shape=[
            jax.ShapeDtypeStruct((rows, channels), BF16),
            jax.ShapeDtypeStruct((rows, 2 * STATE), BF16),
            head_shape, head_shape, head_shape,
            jax.ShapeDtypeStruct((tiles, STATE, LANES), BF16),
            jax.ShapeDtypeStruct((spans - 1, tiles, STATE, LANES), BF16),
            jax.ShapeDtypeStruct((tiles, 8, LANES), F32),
        ],
        scratch_shapes=[
            pltpu.VMEM((rows + EDGE, BLOCK), F32),
            pltpu.VMEM((groups, rows, LANES), F32),
            pltpu.VMEM((groups, 8, LANES), F32),
            pltpu.VMEM((spans, STATE, SPAN), BF16),
        ],
        compiler_params=pltpu.CompilerParams(vmem_limit_bytes=FRONT_LIMIT),
        cost_estimate=pl.CostEstimate(
            flops=2 * rows * 2560 * channels,
            bytes_accessed=4 * rows * channels,
            transcendentals=rows * channels,
        ),
        name="front",
    )(raw_in, raw_bc, raw_step, edge, taps, offset, taps_bc, offset_bc, step_bias, decay_log)


def inside_kernel(first, x_ref, bc_ref, cum_ref, dt_ref, prior_ref, skip_ref, out_ref):
    tiles = x_ref.shape[1] // LANES
    write = bc_ref[:, :STATE]
    read = bc_ref[:, STATE:]
    scores = lax.dot_general(read, write, (((1,), (1,)), ((), ())), preferred_element_type=F32)
    row = lax.broadcasted_iota(jnp.int32, (SPAN, SPAN), 0)
    col = lax.broadcasted_iota(jnp.int32, (SPAN, SPAN), 1)
    scores = jnp.where(row >= col, scores, 0.0)
    cum = cum_ref[...]
    cum_t = jnp.transpose(cum)
    dt_t = jnp.transpose(dt_ref[...])
    grown = jnp.exp(cum)
    lane = lax.broadcasted_iota(jnp.int32, (SPAN, LANES), 1)
    for t in range(tiles):
        at = slice(t * LANES, (t + 1) * LANES)
        x = x_ref[:, at]
        both = []
        for h in (2 * t, 2 * t + 1):
            gap = jnp.minimum(cum[:, h : h + 1] - cum_t[h : h + 1, :], 0.0)
            both.append((scores * jnp.exp(gap) * dt_t[h : h + 1, :]).astype(BF16))
        zero = jnp.zeros_like(x)
        stacked = jnp.concatenate(
            [jnp.where(lane < HEADDIM, x, zero), jnp.where(lane < HEADDIM, zero, x)], axis=0
        )
        total = dot(jnp.concatenate(both, axis=1), stacked)
        total = total + skip_ref[:, at] * x.astype(F32)
        if not first:
            scale = jnp.where(
                lane < HEADDIM, grown[:, 2 * t : 2 * t + 1], grown[:, 2 * t + 1 : 2 * t + 2]
            )
            total = total + scale * dot(read, prior_ref[0, t])
        out_ref[:, at] = total


def inside(span, x, bc, cum, dt, prior, skip):
    channels = x.shape[1]
    tiles = channels // LANES
    at = lambda i: (span, 0)
    return pl.pallas_call(
        functools.partial(inside_kernel, span == 0),
        grid=(1,),
        in_specs=[
            pl.BlockSpec((SPAN, channels), at),
            pl.BlockSpec((SPAN, 2 * STATE), at),
            pl.BlockSpec((SPAN, LANES), at),
            pl.BlockSpec((SPAN, LANES), at),
            pl.BlockSpec((1, tiles, STATE, LANES), lambda i: (max(span - 1, 0), 0, 0, 0)),
            pl.BlockSpec((1, channels), lambda i: (0, 0)),
        ],
        out_specs=pl.BlockSpec((SPAN, channels), lambda i: (0, 0)),
        out_shape=jax.ShapeDtypeStruct((SPAN, channels), F32),
        compiler_params=pltpu.CompilerParams(vmem_limit_bytes=INSIDE_LIMIT),
        cost_estimate=pl.CostEstimate(
            flops=1_500_000_000, bytes_accessed=2 * SPAN * channels, transcendentals=0
        ),
        name="inside",
    )(x, bc, cum, dt, prior, skip)


def split3(v):
    high = v.astype(BF16)
    rest = v - high.astype(F32)
    mid = rest.astype(BF16)
    return high, mid, (rest - mid.astype(F32)).astype(BF16)


def joined(message, rows):
    return (
        message[rows : rows + 1].astype(F32)
        + message[rows + 1 : rows + 2].astype(F32)
        + message[rows + 2 : rows + 3].astype(F32)
    )


def squares_rows(total):
    index = lax.broadcasted_iota(jnp.int32, (16, LANES), 0)
    high, mid, low = (p.astype(F32) for p in split3(total))
    out = jnp.where(index == 0, high, jnp.where(index == 1, mid, jnp.where(index == 2, low, 0.0)))
    return out.astype(BF16)


def tail_kernel(
    inner_total, which, bc_ref, lead_ref, l0, l1, l2, l3, gate_a, gate_b, state_ref, norm_ref,
    w_ref, *refs,
):
    *outs, gated = refs
    count = which.shape[0]
    local_refs = (l0, l1, l2, l3)
    channels = l0.shape[1]
    tiles = channels // LANES
    half = tiles // 2
    sums = []
    for i in range(count):
        span = which[i]
        at_rows = pl.ds(pl.multiple_of(span * SPAN, SPAN), SPAN)
        read = bc_ref[at_rows, STATE:]
        lead = lead_ref[at_rows, :]
        squares = jnp.zeros((SPAN, LANES), F32)
        for t in range(tiles):
            at = slice(t * LANES, (t + 1) * LANES)
            scale = lane_pair(lead[:, 2 * t : 2 * t + 1], lead[:, 2 * t + 1 : 2 * t + 2])
            local = local_refs[0][:, at]
            for k in range(1, len(local_refs)):
                local = jnp.where(span == k, local_refs[k][:, at], local)
            mixed = local + scale * dot(read, state_ref[t])
            gate_ref = gate_a if t < half else gate_b
            gate = gate_ref[at_rows, (t % half) * LANES : (t % half + 1) * LANES].astype(F32)
            pre = mixed * silu(gate)
            squares = squares + pre * pre
            gated[i * SPAN : (i + 1) * SPAN, at] = (pre * norm_ref[:, at]).astype(BF16)
        total = jnp.sum(squares, axis=1, keepdims=True) * (1.0 / inner_total)
        sums.append(jnp.transpose(jnp.broadcast_to(total, (SPAN, LANES)))[:1])
    width = w_ref.shape[1]
    side_rows = width // 2 // LANES * SPAN
    for j in range(width // BLOCK):
        part = dot(gated[...], w_ref[:, j * BLOCK : (j + 1) * BLOCK]).astype(outs[0].dtype)
        for u in range(BLOCK // LANES):
            tile = j * (BLOCK // LANES) + u
            side, tile = divmod(tile, width // 2 // LANES)
            for i in range(count):
                outs[2 * i + side][tile * SPAN : (tile + 1) * SPAN, :] = part[
                    i * SPAN : (i + 1) * SPAN, u * LANES : (u + 1) * LANES
                ]
    for i in range(count):
        for side in range(2):
            out = outs[2 * i + side]
            if out.shape[0] == side_rows + 16:
                out[side_rows:, :] = squares_rows(sums[i])
    if len(outs) > 2 * count:
        outs[2 * count][...] = jnp.broadcast_to(sums[0], (8, LANES))


def tail(which, bc, lead, inner, gate, state, norm, weight, squares_in):
    count = which.shape[0]
    channels = inner[0].shape[1]
    width = weight.shape[1]
    side_rows = width // 2 // LANES * SPAN
    vmem = pl.BlockSpec(memory_space=pltpu.VMEM)
    shapes = []
    for i in range(count):
        for side in range(2):
            extra = 16 if (i, side) in squares_in else 0
            shapes.append(jax.ShapeDtypeStruct((side_rows + extra, LANES), BF16))
    if not squares_in:
        shapes.append(jax.ShapeDtypeStruct((8, LANES), F32))
    return pl.pallas_call(
        functools.partial(tail_kernel, HEADS * HEADDIM),
        in_specs=[pl.BlockSpec(memory_space=pltpu.SMEM)] + [vmem] * 11,
        out_specs=[vmem] * len(shapes),
        out_shape=shapes,
        scratch_shapes=[pltpu.VMEM((count * SPAN, channels), BF16)],
        compiler_params=pltpu.CompilerParams(vmem_limit_bytes=TAIL_LIMIT),
        cost_estimate=pl.CostEstimate(
            flops=2 * count * SPAN * channels * width,
            bytes_accessed=2 * channels * width,
            transcendentals=0,
        ),
    )(which, bc, lead, *inner, *gate, state, norm, weight)


def merge_kernel(a_ref, b_ref, b_squares, out_ref):
    rows = a_ref.shape[0] - 16
    out_ref[:rows, :] = (a_ref[:rows, :].astype(F32) + b_ref[:rows, :].astype(F32)).astype(BF16)
    total = joined(a_ref, rows)
    if b_squares:
        total = total + joined(b_ref, rows)
    out_ref[rows:, :] = squares_rows(total)


def merge(near, relayed, with_squares):
    vmem = pl.BlockSpec(memory_space=pltpu.VMEM)

    def body(a_ref, b_ref, out_ref):
        merge_kernel(a_ref, b_ref, with_squares, out_ref)

    return pl.pallas_call(
        body,
        in_specs=[vmem] * 2,
        out_specs=vmem,
        out_shape=jax.ShapeDtypeStruct(near.shape, BF16),
        compiler_params=pltpu.CompilerParams(vmem_limit_bytes=SMALL_LIMIT),
        cost_estimate=pl.CostEstimate(flops=1000000, bytes_accessed=10**6, transcendentals=0),
    )(near, relayed)


def final_kernel(own_l, own_r, own_sq, up, down, direct_l, direct_r, out_ref):
    rows = own_l.shape[0]
    tiles = rows // SPAN
    total = own_sq[0:1, :] + joined(up, rows) + joined(down, rows)
    scale = lax.rsqrt(total + 0.25)
    column = jnp.transpose(jnp.broadcast_to(scale, (LANES, SPAN)))
    for side, parts in enumerate(((own_l, up, direct_l), (own_r, direct_r, down))):
        for t in range(tiles):
            at = slice(t * SPAN, (t + 1) * SPAN)
            added = sum(p[at, :].astype(F32) for p in parts)
            to = slice((side * tiles + t) * LANES, (side * tiles + t + 1) * LANES)
            out_ref[:, to] = (added * column).astype(BF16)


def final(*parts):
    vmem = pl.BlockSpec(memory_space=pltpu.VMEM)
    tiles = parts[0].shape[0] // SPAN
    return pl.pallas_call(
        final_kernel,
        in_specs=[vmem] * len(parts),
        out_specs=vmem,
        out_shape=jax.ShapeDtypeStruct((SPAN, 2 * tiles * LANES), BF16),
        compiler_params=pltpu.CompilerParams(vmem_limit_bytes=SMALL_LIMIT),
        cost_estimate=pl.CostEstimate(flops=1000000, bytes_accessed=10**6, transcendentals=0),
        name="final",
    )(*parts)


def ring(value, axis, distance):
    size = lax.axis_size(axis)
    return lax.ppermute(value, axis, [(i, (i + distance) % size) for i in range(size)])


def onward(value, axis, distance):
    size = lax.axis_size(axis)
    return lax.ppermute(
        value, axis, [(i, i + distance) for i in range(size) if i + distance < size]
    )


def pick(values, index):
    out = values[0]
    for k in range(1, len(values)):
        out = jnp.where(index == k, values[k], out)
    return out


def packed(state, decay):
    tiles = state.shape[0]
    high = decay.astype(BF16)
    low = (decay - high.astype(F32)).astype(BF16)
    spare = jnp.zeros((16 - 2 * tiles, LANES), BF16)
    return jnp.concatenate([state.astype(BF16).reshape(-1, LANES), high, low, spare], 0)


def unpacked(message, tiles):
    rows = message.shape[0] - 16
    state = message[:rows].reshape(tiles, rows // tiles, LANES).astype(F32)
    high = message[rows : rows + tiles].astype(F32)
    low = message[rows + tiles : rows + 2 * tiles].astype(F32)
    return state, (high + low)[:, None, :]


def incoming_state(local, decay):
    z_axis, y_axis, c_axis = SEQ
    z, y, c = (lax.axis_index(a) for a in SEQ)
    ys, zs = lax.axis_size(y_axis), lax.axis_size(z_axis)
    tiles = local.shape[0] // 2
    first = c == 0
    here = jnp.where(first, local[:tiles], local[tiles:])
    there = jnp.where(first, local[tiles:], local[:tiles])
    here_d = jnp.where(first, decay[:tiles], decay[tiles:])
    there_d = jnp.where(first, decay[tiles:], decay[:tiles])

    got = ring(packed(there, there_d), c_axis, 1)
    other, other_d = unpacked(got, tiles)
    here, here_d = here.astype(F32), here_d[:, None, :]
    s0, d0 = jnp.where(first, here, other), jnp.where(first, here_d, other_d)
    s1, d1 = jnp.where(first, other, here), jnp.where(first, other_d, here_d)
    chip, chip_d = d1 * s0 + s1, d0 * d1

    part = STATE // ys
    quarters = [chip[:, q * part : (q + 1) * part] for q in range(ys)]
    sent = [pick(quarters, (y + k) % ys) for k in range(ys)]
    got = [
        unpacked(ring(packed(sent[k], chip_d[:, 0]), y_axis, k), tiles) for k in range(1, ys)
    ]
    by_shift = [(sent[0], chip_d)] + got
    states = [pick([g[0] for g in by_shift], (y - q) % ys) for q in range(ys)]
    decays = [pick([g[1] for g in by_shift], (y - q) % ys) for q in range(ys)]
    plane, plane_d = states[0], decays[0]
    for q in range(1, ys):
        plane, plane_d = decays[q] * plane + states[q], decays[q] * plane_d

    message = packed(plane, plane_d[:, 0])
    got = [unpacked(onward(message, z_axis, k), tiles) for k in range(1, zs)]
    before = jnp.zeros_like(plane)
    for q in range(zs - 1):
        s = pick([g[0] for g in got], z - q - 1)
        d = pick([g[1] for g in got], z - q - 1)
        before = jnp.where(q < z, d * before + s, before)

    prefix = [before]
    for q in range(ys - 1):
        prefix.append(decays[q] * prefix[-1] + states[q])
    sent = [pick(prefix, (y + k) % ys).astype(BF16) for k in range(ys)]
    got = [sent[0]] + [ring(sent[k], y_axis, k) for k in range(1, ys)]
    chip_in = jnp.concatenate([pick(got, (y - q) % ys) for q in range(ys)], axis=1)
    second_in = (d0 * chip_in.astype(F32) + s0).astype(BF16)
    mine = jnp.where(first, chip_in, second_in)
    got = ring(jnp.where(first, second_in, chip_in), c_axis, 1)
    return jnp.concatenate([jnp.where(first, mine, got), jnp.where(first, got, mine)], axis=0)


def per_device(
    tokens,
    proj_inner,
    proj_gate,
    proj_bc,
    proj_step,
    conv_inner,
    conv_bc,
    offset_inner,
    offset_bc,
    step_bias,
    decay_log,
    skip_gain,
    norm_weight,
    out_weight,
):
    rows = tokens.shape[0]
    spans = rows // SPAN
    channels = proj_inner.shape[1]
    devices = lax.axis_size(SEQ)
    raw_in, raw_bc, raw_step, edge = raw_projections(tokens, proj_bc, proj_step.T, proj_inner)
    edge = lax.ppermute(edge, SEQ, [(i, i + 1) for i in range(devices - 1)])
    gate_a = gate_projection(tokens, proj_gate, 0, channels // 2)
    x, bc, cum, dt, lead, local, prior, decay = front(
        raw_in, raw_bc, raw_step, edge, conv_inner, offset_inner[None],
        conv_bc, offset_bc[None], step_bias[None], decay_log[None],
    )
    gate_b = gate_projection(tokens, proj_gate, channels // 2, channels // 2)
    state = incoming_state(local, decay[:, 0])
    skip = jnp.repeat(skip_gain, HEADDIM)[None]
    inner = []
    for s in range(spans):
        inner.append(inside(s, x, bc, cum, dt, prior, skip))

    head = lax.axis_index("head")
    size = lax.axis_size("head")

    def run(which, squares_in):
        order = jnp.stack([(head + k) & (size - 1) for k in which]).astype(jnp.int32)
        return tail(
            order, bc, lead, inner, (gate_a, gate_b), state, norm_weight[None], out_weight,
            squares_in,
        )

    def moved(value, distance):
        return ring(value, "head", distance)

    far_left, far_right = run((2,), {(0, 0), (0, 1)})
    relay_up = moved(far_left, 1)
    relay_down = moved(far_right, -1)
    next_left, next_right, last_left, last_right = run((1, 3), {(0, 0), (1, 1)})
    direct_up = moved(next_right, 1)
    direct_down = moved(last_left, -1)
    own_left, own_right, own_squares = run((0,), set())
    up = merge(next_left, relay_up, True)
    up = moved(up, 1)
    down = merge(last_right, relay_down, False)
    down = moved(down, -1)
    return final(own_left, own_right, own_squares, up, down, direct_down, direct_up)


def solution(mesh):
    torus = Mesh(
        mesh.devices.reshape(4, 4, 2, mesh.shape["head"]), ("seq_0", "seq_1", "seq_2", "head")
    )
    return jax.shard_map(
        per_device,
        mesh=torus,
        in_specs=(
            P(SEQ, None),
            P(None, "head"),
            P(None, "head"),
            P(),
            P(None, "head"),
            P(None, "head"),
            P(),
            P("head"),
            P(),
            P("head"),
            P("head"),
            P("head"),
            P("head"),
            P("head", None),
        ),
        out_specs=P(SEQ_HEAD, None),
        check_vma=False,
    )
```

```python
import functools

import jax
import jax.numpy as jnp
from jax import lax
from jax.experimental import pallas as pl
from jax.experimental.pallas import tpu as pltpu
from jax.sharding import Mesh
from jax.sharding import PartitionSpec as P


HEADS = 80
HEADDIM = 64
STATE = 128
KERNEL = 4
SPAN = 128
LANES = 128
EDGE = 8
BLOCK = 256
SEQ = ("seq_0", "seq_1", "seq_2")
SEQ_HEAD = ("seq_0", "seq_1", "seq_2", "head")

MIB = 2**20
RAW_LIMIT = 24 * MIB
FRONT_LIMIT = 24 * MIB
INSIDE_LIMIT = 8 * MIB
TAIL_LIMIT = 24 * MIB
SMALL_LIMIT = 8 * MIB


F32 = jnp.float32
X_SPACE = pltpu.HBM
BF16 = jnp.bfloat16


def in_hbm(*arrays):
    return [pltpu.with_memory_space_constraint(a, pltpu.HBM) for a in arrays]


def dot(a, b):
    return jnp.dot(a, b, preferred_element_type=F32)


def silu(v):
    return v * (0.5 + 0.5 * jnp.tanh(0.5 * v))


def lane_pair(first, second):
    lane = lax.broadcasted_iota(jnp.int32, (first.shape[0], LANES), 1)
    return jnp.where(lane < HEADDIM, first, second)


def raw_kernel(
    tok_hbm, bc_hbm, step_hbm, in_hbm, gate_hbm,
    in_out, bc_out, step_out, edge_out, gate_out,
    tok, w_bc, w_step, w_wide, sems,
):
    rows = tok.shape[0]
    heads = w_step.shape[0]
    width = in_hbm.shape[1] // 2

    def part(k):
        source = in_hbm if k < 2 else gate_hbm
        at = slice(k % 2 * width, (k % 2 + 1) * width)
        return pltpu.make_async_copy(source.at[:, at], w_wide.at[k], sems.at[3 + k])

    first = [
        pltpu.make_async_copy(tok_hbm, tok, sems.at[0]),
        pltpu.make_async_copy(bc_hbm, w_bc, sems.at[1]),
        pltpu.make_async_copy(step_hbm, w_step, sems.at[2]),
    ]
    for copy in first:
        copy.start()
    for copy in first:
        copy.wait()
    part(0).start()
    bc = dot(tok[...], w_bc[...]).astype(BF16)
    bc_out[...] = bc
    edge_out[:, :BLOCK] = bc[rows - EDGE :]
    step_out[:, :heads] = lax.dot_general(
        tok[...], w_step[...], (((1,), (1,)), ((), ())), preferred_element_type=F32
    )
    for k in range(4):
        part(k).wait()
        if k < 3:
            part(k + 1).start()
        at = slice(k % 2 * width, (k % 2 + 1) * width)
        raw = dot(tok[...], w_wide[k]).astype(BF16)
        if k < 2:
            in_out[:, at] = raw
            edge_out[:, BLOCK + k * width : BLOCK + (k + 1) * width] = raw[rows - EDGE :]
        else:
            gate_out[:, at] = raw


def raw_projections(tokens, w_bc, w_step, w_in, w_gate):
    rows, width = tokens.shape
    channels = w_in.shape[1]
    vmem = pl.BlockSpec(memory_space=pltpu.VMEM)
    return pl.pallas_call(
        raw_kernel,
        in_specs=[pl.BlockSpec(memory_space=pltpu.HBM)] * 5,
        out_specs=[vmem] * 5,
        out_shape=[
            jax.ShapeDtypeStruct((rows, channels), BF16),
            jax.ShapeDtypeStruct((rows, BLOCK), BF16),
            jax.ShapeDtypeStruct((rows, LANES), F32),
            jax.ShapeDtypeStruct((EDGE, channels + BLOCK), BF16),
            jax.ShapeDtypeStruct((rows, channels), BF16),
        ],
        scratch_shapes=[
            pltpu.VMEM(tokens.shape, BF16),
            pltpu.VMEM(w_bc.shape, BF16),
            pltpu.VMEM(w_step.shape, BF16),
            pltpu.VMEM((4, width, channels // 2), BF16),
            pltpu.SemaphoreType.DMA((7,)),
        ],
        compiler_params=pltpu.CompilerParams(vmem_limit_bytes=RAW_LIMIT),
        cost_estimate=pl.CostEstimate(
            flops=2 * rows * width * (2 * channels + BLOCK + LANES),
            bytes_accessed=2 * width * (rows + 2 * channels + BLOCK),
            transcendentals=0,
        ),
        name="raw",
    )(*in_hbm(tokens, w_bc, w_step, w_in, w_gate))


def steps_kernel(raw_step, step_bias, decay_log, cum_out, dt_out, lead_out):
    rows = raw_step.shape[0]
    heads = step_bias.shape[1]
    v = raw_step[:, :heads] + step_bias[...]
    dt = jnp.maximum(v, 0.0) + jnp.log1p(jnp.exp(-jnp.abs(v)))
    log_decay = -jnp.exp(decay_log[...]) * dt
    cum_out[...] = jnp.zeros_like(cum_out)
    dt_out[...] = jnp.zeros_like(dt_out)
    lead_out[...] = jnp.zeros_like(lead_out)
    dt_out[:, :heads] = dt
    row = lax.broadcasted_iota(jnp.int32, (SPAN, SPAN), 0)
    col = lax.broadcasted_iota(jnp.int32, (SPAN, SPAN), 1)
    lower = (row >= col).astype(F32)
    lead = jnp.zeros((1, heads), F32)
    for s in range(rows // SPAN):
        at = slice(s * SPAN, (s + 1) * SPAN)
        cum = jnp.dot(
            lower, log_decay[at], preferred_element_type=F32, precision=lax.Precision.HIGHEST
        )
        cum_out[at, :heads] = cum
        lead_out[at, :heads] = jnp.exp(cum + lead)
        lead = lead + cum[SPAN - 1 :, :]


def steps(raw_step, step_bias, decay_log):
    vmem = pl.BlockSpec(memory_space=pltpu.VMEM)
    return pl.pallas_call(
        steps_kernel,
        in_specs=[vmem] * 3,
        out_specs=[vmem] * 3,
        out_shape=[jax.ShapeDtypeStruct(raw_step.shape, F32)] * 3,
        compiler_params=pltpu.CompilerParams(vmem_limit_bytes=SMALL_LIMIT),
        cost_estimate=pl.CostEstimate(flops=10**9, bytes_accessed=10**6, transcendentals=0),
        name="steps",
    )(raw_step, step_bias, decay_log)


def front_kernel(
    raw_in, raw_bc, edge, cum_ref, dt_ref, lead_ref, taps, offset, taps_bc, offset_bc,
    x_out, bc_out, local_out, prior_out, decay_out,
    padded, end_w, span_d, write_t,
):
    step = pl.program_id(0)
    rows = raw_in.shape[0]
    spans = rows // SPAN
    per = BLOCK // HEADDIM
    groups = end_w.shape[0]

    def conv(raw, tap, off):
        padded[EDGE:, :] = raw[...].astype(F32)
        padded[:EDGE, :] = edge[...].astype(F32)
        total = off + tap[0:1, :] * padded[EDGE - 3 : EDGE - 3 + rows, :]
        for k in range(1, KERNEL):
            total = total + tap[k : k + 1, :] * padded[EDGE - 3 + k : EDGE - 3 + k + rows, :]
        return silu(total).astype(BF16)

    @pl.when(step == 0)
    def _():
        bc = conv(raw_bc, taps_bc, offset_bc[...])
        bc_out[...] = bc
        for s in range(spans):
            block = bc[s * SPAN : (s + 1) * SPAN, :STATE].astype(F32)
            write_t[s] = jnp.transpose(block).astype(BF16)
        for s in range(spans):
            at = slice(s * SPAN, (s + 1) * SPAN)
            cum = cum_ref[at, :]
            last = cum[SPAN - 1 :, :]
            ends = jnp.exp(last - cum) * dt_ref[at, :]
            gone = jnp.exp(last)
            for g in range(groups):
                end_w[g, at, :per] = ends[:, g * per : (g + 1) * per]
                span_d[g, s : s + 1, :per] = gone[:, g * per : (g + 1) * per]
        for g in range(groups):
            span_d[g, spans : spans + 1, :per] = lead_ref[rows - 1 :, g * per : (g + 1) * per]

    @pl.when(step > 0)
    def _():
        g = step - 1
        x = conv(raw_in, taps, offset[...])
        x_out[...] = x
        ends = end_w[g]
        gone = span_d[g]
        wide = jnp.concatenate(
            [lane_pair(ends[:, t : t + 1], ends[:, t + 1 : t + 2]) for t in range(0, per, 2)], axis=1
        )
        gone_wide = jnp.concatenate(
            [lane_pair(gone[:, t : t + 1], gone[:, t + 1 : t + 2]) for t in range(0, per, 2)], axis=1
        )
        weighted = (x.astype(F32) * wide).astype(BF16)
        running = jnp.zeros((STATE, BLOCK), F32)
        tiles = BLOCK // LANES
        for s in range(spans):
            if s > 0:
                for t in range(tiles):
                    prior_out[s - 1, t] = running[:, t * LANES : (t + 1) * LANES].astype(BF16)
            local = dot(write_t[s], weighted[s * SPAN : (s + 1) * SPAN])
            running = gone_wide[s : s + 1] * running + local
        for t in range(tiles):
            local_out[t] = running[:, t * LANES : (t + 1) * LANES].astype(BF16)
            decay_out[t] = jnp.broadcast_to(
                gone_wide[spans : spans + 1, t * LANES : (t + 1) * LANES], (8, LANES)
            )


def front(raw_in, raw_bc, edge, cum, dt, lead, taps, offset, taps_bc, offset_bc):
    rows, channels = raw_in.shape
    groups = channels // BLOCK
    spans = rows // SPAN
    tiles = channels // LANES
    per_block = BLOCK // LANES

    def whole(a):
        return pl.BlockSpec(a.shape, lambda i: (0,) * a.ndim)

    def late(shape, dim):
        return pl.BlockSpec(
            shape,
            lambda i: tuple(jnp.maximum(i - 1, 0) if d == dim else 0 for d in range(len(shape))),
        )

    return pl.pallas_call(
        front_kernel,
        grid=(groups + 1,),
        in_specs=[
            late((rows, BLOCK), 1), whole(raw_bc),
            pl.BlockSpec((EDGE, BLOCK), lambda i: (0, i)),
            whole(cum), whole(dt), whole(lead),
            late((KERNEL, BLOCK), 1), late((1, BLOCK), 1),
            whole(taps_bc), whole(offset_bc),
        ],
        out_specs=[
            late((rows, BLOCK), 1),
            pl.BlockSpec((rows, 2 * STATE), lambda i: (0, 0)),
            late((per_block, STATE, LANES), 0),
            late((spans - 1, per_block, STATE, LANES), 1),
            late((per_block, 8, LANES), 0),
        ],
        out_shape=[
            X_SPACE((rows, channels), BF16),
            jax.ShapeDtypeStruct((rows, 2 * STATE), BF16),
            jax.ShapeDtypeStruct((tiles, STATE, LANES), BF16),
            X_SPACE((spans - 1, tiles, STATE, LANES), BF16),
            jax.ShapeDtypeStruct((tiles, 8, LANES), F32),
        ],
        scratch_shapes=[
            pltpu.VMEM((rows + EDGE, BLOCK), F32),
            pltpu.VMEM((groups, rows, LANES), F32),
            pltpu.VMEM((groups, 8, LANES), F32),
            pltpu.VMEM((spans, STATE, SPAN), BF16),
        ],
        compiler_params=pltpu.CompilerParams(vmem_limit_bytes=FRONT_LIMIT),
        cost_estimate=pl.CostEstimate(
            flops=2 * rows * 2560 * channels,
            bytes_accessed=4 * rows * channels,
            transcendentals=rows * channels,
        ),
        name="front",
    )(raw_in, raw_bc, edge, cum, dt, lead, taps, offset, taps_bc, offset_bc)


def inside_kernel(first, x_ref, bc_ref, cum_ref, dt_ref, prior_ref, skip_ref, out_ref):
    tiles = x_ref.shape[1] // LANES
    write = bc_ref[:, :STATE]
    read = bc_ref[:, STATE:]
    scores = lax.dot_general(read, write, (((1,), (1,)), ((), ())), preferred_element_type=F32)
    row = lax.broadcasted_iota(jnp.int32, (SPAN, SPAN), 0)
    col = lax.broadcasted_iota(jnp.int32, (SPAN, SPAN), 1)
    scores = jnp.where(row >= col, scores, 0.0)
    cum = cum_ref[...]
    cum_t = jnp.transpose(cum)
    dt_t = jnp.transpose(dt_ref[...])
    grown = jnp.exp(cum)
    lane = lax.broadcasted_iota(jnp.int32, (SPAN, LANES), 1)
    for t in range(tiles):
        at = slice(t * LANES, (t + 1) * LANES)
        x = x_ref[:, at]
        both = []
        for h in (2 * t, 2 * t + 1):
            gap = jnp.minimum(cum[:, h : h + 1] - cum_t[h : h + 1, :], 0.0)
            both.append((scores * jnp.exp(gap) * dt_t[h : h + 1, :]).astype(BF16))
        zero = jnp.zeros_like(x)
        stacked = jnp.concatenate(
            [jnp.where(lane < HEADDIM, x, zero), jnp.where(lane < HEADDIM, zero, x)], axis=0
        )
        total = dot(jnp.concatenate(both, axis=1), stacked)
        total = total + skip_ref[:, at] * x.astype(F32)
        if not first:
            scale = jnp.where(
                lane < HEADDIM, grown[:, 2 * t : 2 * t + 1], grown[:, 2 * t + 1 : 2 * t + 2]
            )
            total = total + scale * dot(read, prior_ref[0, t])
        out_ref[:, at] = total


def inside(span, x, bc, cum, dt, prior, skip):
    channels = x.shape[1]
    tiles = channels // LANES
    at = lambda i: (span, 0)
    return pl.pallas_call(
        functools.partial(inside_kernel, span == 0),
        grid=(1,),
        in_specs=[
            pl.BlockSpec((SPAN, channels), at),
            pl.BlockSpec((SPAN, 2 * STATE), at),
            pl.BlockSpec((SPAN, LANES), at),
            pl.BlockSpec((SPAN, LANES), at),
            pl.BlockSpec((1, tiles, STATE, LANES), lambda i: (max(span - 1, 0), 0, 0, 0)),
            pl.BlockSpec((1, channels), lambda i: (0, 0)),
        ],
        out_specs=pl.BlockSpec((SPAN, channels), lambda i: (0, 0)),
        out_shape=jax.ShapeDtypeStruct((SPAN, channels), F32),
        compiler_params=pltpu.CompilerParams(vmem_limit_bytes=INSIDE_LIMIT),
        cost_estimate=pl.CostEstimate(
            flops=1_500_000_000, bytes_accessed=2 * SPAN * channels, transcendentals=0
        ),
        name="inside",
    )(*in_hbm(x), bc, cum, dt, *in_hbm(prior), skip)


def split3(v):
    high = v.astype(BF16)
    rest = v - high.astype(F32)
    mid = rest.astype(BF16)
    return high, mid, (rest - mid.astype(F32)).astype(BF16)


def joined(message, rows):
    return (
        message[rows : rows + 1].astype(F32)
        + message[rows + 1 : rows + 2].astype(F32)
        + message[rows + 2 : rows + 3].astype(F32)
    )


def squares_rows(total):
    index = lax.broadcasted_iota(jnp.int32, (16, LANES), 0)
    high, mid, low = (p.astype(F32) for p in split3(total))
    out = jnp.where(index == 0, high, jnp.where(index == 1, mid, jnp.where(index == 2, low, 0.0)))
    return out.astype(BF16)


def tail_kernel(
    inner_total, which, bc_ref, lead_ref, l0, l1, l2, l3, gate_ref, state_ref, norm_ref,
    w_ref, *refs,
):
    *outs, gated = refs
    count = which.shape[0]
    local_refs = (l0, l1, l2, l3)
    channels = l0.shape[1]
    tiles = channels // LANES
    sums = []
    for i in range(count):
        span = which[i]
        at_rows = pl.ds(pl.multiple_of(span * SPAN, SPAN), SPAN)
        read = bc_ref[at_rows, STATE:]
        lead = lead_ref[at_rows, :]
        squares = jnp.zeros((SPAN, LANES), F32)
        for t in range(tiles):
            at = slice(t * LANES, (t + 1) * LANES)
            scale = lane_pair(lead[:, 2 * t : 2 * t + 1], lead[:, 2 * t + 1 : 2 * t + 2])
            local = local_refs[0][:, at]
            for k in range(1, len(local_refs)):
                local = jnp.where(span == k, local_refs[k][:, at], local)
            mixed = local + scale * dot(read, state_ref[t])
            gate = gate_ref[at_rows, at].astype(F32)
            pre = mixed * silu(gate)
            squares = squares + pre * pre
            gated[i * SPAN : (i + 1) * SPAN, at] = (pre * norm_ref[:, at]).astype(BF16)
        total = jnp.sum(squares, axis=1, keepdims=True) * (1.0 / inner_total)
        sums.append(jnp.transpose(jnp.broadcast_to(total, (SPAN, LANES)))[:1])
    width = w_ref.shape[1]
    side_rows = width // 2 // LANES * SPAN
    for j in range(width // BLOCK):
        part = dot(gated[...], w_ref[:, j * BLOCK : (j + 1) * BLOCK]).astype(outs[0].dtype)
        for u in range(BLOCK // LANES):
            tile = j * (BLOCK // LANES) + u
            side, tile = divmod(tile, width // 2 // LANES)
            for i in range(count):
                outs[2 * i + side][tile * SPAN : (tile + 1) * SPAN, :] = part[
                    i * SPAN : (i + 1) * SPAN, u * LANES : (u + 1) * LANES
                ]
    for i in range(count):
        for side in range(2):
            out = outs[2 * i + side]
            if out.shape[0] == side_rows + 16:
                out[side_rows:, :] = squares_rows(sums[i])
    if len(outs) > 2 * count:
        outs[2 * count][...] = jnp.broadcast_to(sums[0], (8, LANES))


def tail(which, bc, lead, inner, gate, state, norm, weight, squares_in):
    count = which.shape[0]
    channels = inner[0].shape[1]
    width = weight.shape[1]
    side_rows = width // 2 // LANES * SPAN
    vmem = pl.BlockSpec(memory_space=pltpu.VMEM)
    shapes = []
    for i in range(count):
        for side in range(2):
            extra = 16 if (i, side) in squares_in else 0
            shapes.append(jax.ShapeDtypeStruct((side_rows + extra, LANES), BF16))
    if not squares_in:
        shapes.append(jax.ShapeDtypeStruct((8, LANES), F32))
    return pl.pallas_call(
        functools.partial(tail_kernel, HEADS * HEADDIM),
        in_specs=[pl.BlockSpec(memory_space=pltpu.SMEM)] + [vmem] * 10,
        out_specs=[vmem] * len(shapes),
        out_shape=shapes,
        scratch_shapes=[pltpu.VMEM((count * SPAN, channels), BF16)],
        compiler_params=pltpu.CompilerParams(vmem_limit_bytes=TAIL_LIMIT),
        cost_estimate=pl.CostEstimate(
            flops=2 * count * SPAN * channels * width,
            bytes_accessed=2 * channels * width,
            transcendentals=0,
        ),
    )(which, bc, lead, *inner, gate, state, norm, weight)


def merge_kernel(a_ref, b_ref, b_squares, out_ref):
    rows = a_ref.shape[0] - 16
    out_ref[:rows, :] = (a_ref[:rows, :].astype(F32) + b_ref[:rows, :].astype(F32)).astype(BF16)
    total = joined(a_ref, rows)
    if b_squares:
        total = total + joined(b_ref, rows)
    out_ref[rows:, :] = squares_rows(total)


def merge(near, relayed, with_squares):
    vmem = pl.BlockSpec(memory_space=pltpu.VMEM)

    def body(a_ref, b_ref, out_ref):
        merge_kernel(a_ref, b_ref, with_squares, out_ref)

    return pl.pallas_call(
        body,
        in_specs=[vmem] * 2,
        out_specs=vmem,
        out_shape=jax.ShapeDtypeStruct(near.shape, BF16),
        compiler_params=pltpu.CompilerParams(vmem_limit_bytes=SMALL_LIMIT),
        cost_estimate=pl.CostEstimate(flops=1000000, bytes_accessed=10**6, transcendentals=0),
    )(near, relayed)


def final_kernel(own_l, own_r, own_sq, up, down, direct_l, direct_r, out_ref):
    rows = own_l.shape[0]
    tiles = rows // SPAN
    total = own_sq[0:1, :] + joined(up, rows) + joined(down, rows)
    scale = lax.rsqrt(total + 0.25)
    column = jnp.transpose(jnp.broadcast_to(scale, (LANES, SPAN)))
    for side, parts in enumerate(((own_l, up, direct_l), (own_r, direct_r, down))):
        for t in range(tiles):
            at = slice(t * SPAN, (t + 1) * SPAN)
            added = sum(p[at, :].astype(F32) for p in parts)
            to = slice((side * tiles + t) * LANES, (side * tiles + t + 1) * LANES)
            out_ref[:, to] = (added * column).astype(BF16)


def final(*parts):
    vmem = pl.BlockSpec(memory_space=pltpu.VMEM)
    tiles = parts[0].shape[0] // SPAN
    return pl.pallas_call(
        final_kernel,
        in_specs=[vmem] * len(parts),
        out_specs=vmem,
        out_shape=jax.ShapeDtypeStruct((SPAN, 2 * tiles * LANES), BF16),
        compiler_params=pltpu.CompilerParams(vmem_limit_bytes=SMALL_LIMIT),
        cost_estimate=pl.CostEstimate(flops=1000000, bytes_accessed=10**6, transcendentals=0),
        name="final",
    )(*parts)


def ring(value, axis, distance):
    size = lax.axis_size(axis)
    return lax.ppermute(value, axis, [(i, (i + distance) % size) for i in range(size)])


def onward(value, axis, distance):
    size = lax.axis_size(axis)
    return lax.ppermute(
        value, axis, [(i, i + distance) for i in range(size) if i + distance < size]
    )


def pick(values, index):
    out = values[0]
    for k in range(1, len(values)):
        out = jnp.where(index == k, values[k], out)
    return out


def packed(state, decay):
    tiles = state.shape[0]
    high = decay.astype(BF16)
    low = (decay - high.astype(F32)).astype(BF16)
    spare = jnp.zeros((16 - 2 * tiles, LANES), BF16)
    return jnp.concatenate([state.astype(BF16).reshape(-1, LANES), high, low, spare], 0)


def unpacked(message, tiles):
    rows = message.shape[0] - 16
    state = message[:rows].reshape(tiles, rows // tiles, LANES).astype(F32)
    high = message[rows : rows + tiles].astype(F32)
    low = message[rows + tiles : rows + 2 * tiles].astype(F32)
    return state, (high + low)[:, None, :]


def incoming_state(local, decay):
    z_axis, y_axis, c_axis = SEQ
    z, y, c = (lax.axis_index(a) for a in SEQ)
    ys, zs = lax.axis_size(y_axis), lax.axis_size(z_axis)
    tiles = local.shape[0] // 2
    first = c == 0
    here = jnp.where(first, local[:tiles], local[tiles:])
    there = jnp.where(first, local[tiles:], local[:tiles])
    here_d = jnp.where(first, decay[:tiles], decay[tiles:])
    there_d = jnp.where(first, decay[tiles:], decay[:tiles])

    got = ring(packed(there, there_d), c_axis, 1)
    other, other_d = unpacked(got, tiles)
    here, here_d = here.astype(F32), here_d[:, None, :]
    s0, d0 = jnp.where(first, here, other), jnp.where(first, here_d, other_d)
    s1, d1 = jnp.where(first, other, here), jnp.where(first, other_d, here_d)
    chip, chip_d = d1 * s0 + s1, d0 * d1

    part = STATE // ys
    quarters = [chip[:, q * part : (q + 1) * part] for q in range(ys)]
    sent = [pick(quarters, (y + k) % ys) for k in range(ys)]
    messages = [packed(sent[k], chip_d[:, 0]) for k in range(1, ys)]
    got = [ring(message, y_axis, k + 1) for k, message in enumerate(messages)]
    got = [unpacked(message, tiles) for message in got]
    by_shift = [(sent[0], chip_d)] + got
    states = [pick([g[0] for g in by_shift], (y - q) % ys) for q in range(ys)]
    decays = [pick([g[1] for g in by_shift], (y - q) % ys) for q in range(ys)]
    plane, plane_d = states[0], decays[0]
    for q in range(1, ys):
        plane, plane_d = decays[q] * plane + states[q], decays[q] * plane_d

    message = packed(plane, plane_d[:, 0])
    got = [onward(message, z_axis, k) for k in range(1, zs)]
    got = [unpacked(message, tiles) for message in got]
    before = jnp.zeros_like(plane)
    for q in range(zs - 1):
        s = pick([g[0] for g in got], z - q - 1)
        d = pick([g[1] for g in got], z - q - 1)
        before = jnp.where(q < z, d * before + s, before)

    prefix = [before]
    for q in range(ys - 1):
        prefix.append(decays[q] * prefix[-1] + states[q])
    sent = [pick(prefix, (y + k) % ys).astype(BF16) for k in range(ys)]
    got = [sent[0]] + [ring(sent[k], y_axis, k) for k in range(1, ys)]
    chip_in = jnp.concatenate([pick(got, (y - q) % ys) for q in range(ys)], axis=1)
    second_in = (d0 * chip_in.astype(F32) + s0).astype(BF16)
    mine = jnp.where(first, chip_in, second_in)
    message = jnp.where(first, second_in, chip_in)
    got = ring(message, c_axis, 1)
    return jnp.concatenate([jnp.where(first, mine, got), jnp.where(first, got, mine)], axis=0)


def per_device(
    tokens,
    proj_inner,
    proj_gate,
    proj_bc,
    proj_step,
    conv_inner,
    conv_bc,
    offset_inner,
    offset_bc,
    step_bias,
    decay_log,
    skip_gain,
    norm_weight,
    out_weight,
):
    rows = tokens.shape[0]
    spans = rows // SPAN
    devices = lax.axis_size(SEQ)
    raw_in, raw_bc, raw_step, edge, gate = raw_projections(
        tokens, proj_bc, proj_step.T, proj_inner, proj_gate
    )
    edge = lax.ppermute(edge, SEQ, [(i, i + 1) for i in range(devices - 1)])
    cum, dt, lead = steps(raw_step, step_bias[None], decay_log[None])
    x, bc, local, prior, decay = front(
        raw_in, raw_bc, edge, cum, dt, lead, conv_inner, offset_inner[None],
        conv_bc, offset_bc[None],
    )
    state = incoming_state(local, decay[:, 0])
    skip = jnp.repeat(skip_gain, HEADDIM)[None]
    inner = []
    for s in range(spans):
        inner.append(inside(s, x, bc, cum, dt, prior, skip))

    head = lax.axis_index("head")
    size = lax.axis_size("head")

    def run(which, squares_in):
        order = jnp.stack([(head + k) & (size - 1) for k in which]).astype(jnp.int32)
        return tail(
            order, bc, lead, inner, gate, state, norm_weight[None], out_weight,
            squares_in,
        )

    def moved(value, distance):
        return ring(value, "head", distance)

    far_left, far_right = run((2,), {(0, 0), (0, 1)})
    relay_up = moved(far_left, 1)
    relay_down = moved(far_right, -1)
    next_left, next_right, last_left, last_right = run((1, 3), {(0, 0), (1, 1)})
    direct_up = moved(next_right, 1)
    direct_down = moved(last_left, -1)
    own_left, own_right, own_squares = run((0,), set())
    up = merge(next_left, relay_up, True)
    up = moved(up, 1)
    down = merge(last_right, relay_down, False)
    down = moved(down, -1)
    return final(own_left, own_right, own_squares, up, down, direct_down, direct_up)


def solution(mesh):
    torus = Mesh(
        mesh.devices.reshape(4, 4, 2, mesh.shape["head"]), ("seq_0", "seq_1", "seq_2", "head")
    )
    return jax.shard_map(
        per_device,
        mesh=torus,
        in_specs=(
            P(SEQ, None),
            P(None, "head"),
            P(None, "head"),
            P(),
            P(None, "head"),
            P(None, "head"),
            P(),
            P("head"),
            P(),
            P("head"),
            P("head"),
            P("head"),
            P("head"),
            P("head", None),
        ),
        out_specs=P(SEQ_HEAD, None),
        check_vma=False,
    )
```

```python
import functools

import jax
import jax.numpy as jnp
from jax import lax
from jax.experimental import pallas as pl
from jax.experimental.pallas import tpu as pltpu
from jax.sharding import Mesh
from jax.sharding import PartitionSpec as P


HEADS = 80
HEADDIM = 64
STATE = 128
KERNEL = 4
SPAN = 128
LANES = 128
EDGE = 8
BLOCK = 256
SEQ = ("seq_0", "seq_1", "seq_2")
SEQ_HEAD = ("seq_0", "seq_1", "seq_2", "head")

MIB = 2**20
RAW_LIMIT = 24 * MIB
FRONT_LIMIT = 24 * MIB
INSIDE_LIMIT = 12 * MIB
TAIL_LIMIT = 24 * MIB
SMALL_LIMIT = 8 * MIB


F32 = jnp.float32
BF16 = jnp.bfloat16


def in_hbm(*arrays):
    return [pltpu.with_memory_space_constraint(a, pltpu.HBM) for a in arrays]


def dot(a, b):
    return jnp.dot(a, b, preferred_element_type=F32)


def silu(v):
    return v * (0.5 + 0.5 * jnp.tanh(0.5 * v))


def lane_pair(first, second):
    lane = lax.broadcasted_iota(jnp.int32, (first.shape[0], LANES), 1)
    return jnp.where(lane < HEADDIM, first, second)


def raw_kernel(
    tok_hbm, bc_hbm, step_hbm, in_hbm, gate_hbm,
    in_out, bc_out, step_out, edge_out, gate_out,
    tok, w_bc, w_step, w_in, w_gate, inner, gate, sems,
):
    rows = tok.shape[0]
    heads = w_step.shape[0]
    first = [
        pltpu.make_async_copy(tok_hbm, tok, sems.at[0]),
        pltpu.make_async_copy(bc_hbm, w_bc, sems.at[1]),
        pltpu.make_async_copy(step_hbm, w_step, sems.at[2]),
    ]
    inner_copy = pltpu.make_async_copy(in_hbm, w_in, sems.at[3])
    gate_copy = pltpu.make_async_copy(gate_hbm, w_gate, sems.at[4])
    for copy in first:
        copy.start()
    for copy in first:
        copy.wait()
    inner_copy.start()
    bc = dot(tok[...], w_bc[...]).astype(BF16)
    bc_out[...] = bc
    edge_out[:, :BLOCK] = bc[rows - EDGE :]
    step_out[:, :heads] = lax.dot_general(
        tok[...], w_step[...], (((1,), (1,)), ((), ())), preferred_element_type=F32
    )
    inner_copy.wait()
    gate_copy.start()
    raw = dot(tok[...], w_in[...]).astype(BF16)
    inner[...] = raw
    edge_out[:, BLOCK:] = raw[rows - EDGE :]
    stored = [pltpu.make_async_copy(inner, in_out, sems.at[7])]
    stored[0].start()
    gate_copy.wait()
    half = rows // 2
    for k in range(2):
        at = slice(k * half, (k + 1) * half)
        gate[at, :] = dot(tok[at, :], w_gate[...]).astype(BF16)
        stored.append(pltpu.make_async_copy(gate.at[at, :], gate_out.at[at, :], sems.at[5 + k]))
        stored[-1].start()
    for copy in stored:
        copy.wait()


def raw_projections(tokens, w_bc, w_step, w_in, w_gate):
    rows, width = tokens.shape
    channels = w_in.shape[1]
    vmem = pl.BlockSpec(memory_space=pltpu.VMEM)
    hbm = pl.BlockSpec(memory_space=pltpu.HBM)
    return pl.pallas_call(
        raw_kernel,
        in_specs=[hbm] * 5,
        out_specs=[hbm] + [vmem] * 3 + [hbm],
        out_shape=[
            pltpu.HBM((rows, channels), BF16),
            jax.ShapeDtypeStruct((rows, BLOCK), BF16),
            jax.ShapeDtypeStruct((rows, LANES), F32),
            jax.ShapeDtypeStruct((EDGE, channels + BLOCK), BF16),
            pltpu.HBM((rows, channels), BF16),
        ],
        scratch_shapes=[
            pltpu.VMEM(tokens.shape, BF16),
            pltpu.VMEM(w_bc.shape, BF16),
            pltpu.VMEM(w_step.shape, BF16),
            pltpu.VMEM((width, channels), BF16),
            pltpu.VMEM((width, channels), BF16),
            pltpu.VMEM((rows, channels), BF16),
            pltpu.VMEM((rows, channels), BF16),
            pltpu.SemaphoreType.DMA((8,)),
        ],
        compiler_params=pltpu.CompilerParams(vmem_limit_bytes=RAW_LIMIT),
        cost_estimate=pl.CostEstimate(
            flops=2 * rows * width * (2 * channels + BLOCK + LANES),
            bytes_accessed=2 * width * (rows + 2 * channels + BLOCK),
            transcendentals=0,
        ),
        name="raw",
    )(*in_hbm(tokens, w_bc, w_step, w_in, w_gate))


def steps_kernel(raw_step, step_bias, decay_log, cum_out, dt_out, lead_out, *later):
    rows = raw_step.shape[0]
    heads = step_bias.shape[1]
    v = raw_step[:, :heads] + step_bias[...]
    dt = jnp.maximum(v, 0.0) + jnp.log1p(jnp.exp(-jnp.abs(v)))
    log_decay = -jnp.exp(decay_log[...]) * dt
    cum_out[...] = jnp.zeros_like(cum_out)
    dt_out[...] = jnp.zeros_like(dt_out)
    lead_out[...] = jnp.zeros_like(lead_out)
    dt_out[:, :heads] = dt
    row = lax.broadcasted_iota(jnp.int32, (SPAN, SPAN), 0)
    col = lax.broadcasted_iota(jnp.int32, (SPAN, SPAN), 1)
    lower = (row >= col).astype(F32)
    lead = jnp.zeros((1, heads), F32)
    for s in range(rows // SPAN):
        at = slice(s * SPAN, (s + 1) * SPAN)
        cum = jnp.dot(
            lower, log_decay[at], preferred_element_type=F32, precision=lax.Precision.HIGHEST
        )
        cum_out[at, :heads] = cum
        lead_out[at, :heads] = jnp.exp(cum + lead)
        lead = lead + cum[SPAN - 1 :, :]
    for out, value in zip(later, (cum_out, dt_out, lead_out)):
        out[...] = value[...]


def steps(raw_step, step_bias, decay_log):
    vmem = pl.BlockSpec(memory_space=pltpu.VMEM)
    return pl.pallas_call(
        steps_kernel,
        in_specs=[vmem] * 3,
        out_specs=[vmem] * 6,
        out_shape=[jax.ShapeDtypeStruct(raw_step.shape, F32)] * 3
        + [pltpu.HBM(raw_step.shape, F32)] * 3,
        compiler_params=pltpu.CompilerParams(vmem_limit_bytes=SMALL_LIMIT),
        cost_estimate=pl.CostEstimate(flops=10**9, bytes_accessed=10**6, transcendentals=0),
        name="steps",
    )(raw_step, step_bias, decay_log)


def front_kernel(
    raw_in, raw_bc, edge, cum_ref, dt_ref, lead_ref, taps, offset, taps_bc, offset_bc,
    x_out, bc_out, read_out, local_out, prior_out, decay_out,
    padded, end_w, span_d, write_t,
):
    step = pl.program_id(0)
    rows = raw_in.shape[0]
    spans = rows // SPAN
    per = BLOCK // HEADDIM
    groups = end_w.shape[0]

    def conv(raw, tap, off):
        padded[EDGE:, :] = raw[...].astype(F32)
        padded[:EDGE, :] = edge[...].astype(F32)
        total = off + tap[0:1, :] * padded[EDGE - 3 : EDGE - 3 + rows, :]
        for k in range(1, KERNEL):
            total = total + tap[k : k + 1, :] * padded[EDGE - 3 + k : EDGE - 3 + k + rows, :]
        return silu(total).astype(BF16)

    @pl.when(step == 0)
    def _():
        bc = conv(raw_bc, taps_bc, offset_bc[...])
        bc_out[...] = bc
        read_out[...] = bc[:, STATE:]
        for s in range(spans):
            block = bc[s * SPAN : (s + 1) * SPAN, :STATE].astype(F32)
            write_t[s] = jnp.transpose(block).astype(BF16)
        for s in range(spans):
            at = slice(s * SPAN, (s + 1) * SPAN)
            cum = cum_ref[at, :]
            last = cum[SPAN - 1 :, :]
            ends = jnp.exp(last - cum) * dt_ref[at, :]
            gone = jnp.exp(last)
            for g in range(groups):
                end_w[g, at, :per] = ends[:, g * per : (g + 1) * per]
                span_d[g, s : s + 1, :per] = gone[:, g * per : (g + 1) * per]
        for g in range(groups):
            span_d[g, spans : spans + 1, :per] = lead_ref[rows - 1 :, g * per : (g + 1) * per]

    @pl.when(step > 0)
    def _():
        g = step - 1
        x = conv(raw_in, taps, offset[...])
        x_out[...] = x
        ends = end_w[g]
        gone = span_d[g]
        wide = jnp.concatenate(
            [lane_pair(ends[:, t : t + 1], ends[:, t + 1 : t + 2]) for t in range(0, per, 2)], axis=1
        )
        gone_wide = jnp.concatenate(
            [lane_pair(gone[:, t : t + 1], gone[:, t + 1 : t + 2]) for t in range(0, per, 2)], axis=1
        )
        weighted = (x.astype(F32) * wide).astype(BF16)
        running = jnp.zeros((STATE, BLOCK), F32)
        tiles = BLOCK // LANES
        for s in range(spans):
            if s > 0:
                for t in range(tiles):
                    prior_out[s - 1, t] = running[:, t * LANES : (t + 1) * LANES].astype(BF16)
            local = dot(write_t[s], weighted[s * SPAN : (s + 1) * SPAN])
            running = gone_wide[s : s + 1] * running + local
        for t in range(tiles):
            local_out[t] = running[:, t * LANES : (t + 1) * LANES].astype(BF16)
            decay_out[t] = jnp.broadcast_to(
                gone_wide[spans : spans + 1, t * LANES : (t + 1) * LANES], (8, LANES)
            )


def front(raw_in, raw_bc, edge, cum, dt, lead, taps, offset, taps_bc, offset_bc):
    rows, channels = raw_in.shape
    groups = channels // BLOCK
    spans = rows // SPAN
    tiles = channels // LANES
    per_block = BLOCK // LANES

    def whole(a):
        return pl.BlockSpec(a.shape, lambda i: (0,) * a.ndim)

    def late(shape, dim):
        return pl.BlockSpec(
            shape,
            lambda i: tuple(jnp.maximum(i - 1, 0) if d == dim else 0 for d in range(len(shape))),
        )

    return pl.pallas_call(
        front_kernel,
        grid=(groups + 1,),
        in_specs=[
            late((rows, BLOCK), 1), whole(raw_bc),
            pl.BlockSpec((EDGE, BLOCK), lambda i: (0, i)),
            whole(cum), whole(dt), whole(lead),
            late((KERNEL, BLOCK), 1), late((1, BLOCK), 1),
            whole(taps_bc), whole(offset_bc),
        ],
        out_specs=[
            late((rows, BLOCK), 1),
            pl.BlockSpec((rows, 2 * STATE), lambda i: (0, 0)),
            pl.BlockSpec((rows, STATE), lambda i: (0, 0)),
            late((per_block, STATE, LANES), 0),
            late((spans - 1, per_block, STATE, LANES), 1),
            late((per_block, 8, LANES), 0),
        ],
        out_shape=[
            pltpu.HBM((rows, channels), BF16),
            pltpu.HBM((rows, 2 * STATE), BF16),
            pltpu.HBM((rows, STATE), BF16),
            jax.ShapeDtypeStruct((tiles, STATE, LANES), BF16),
            pltpu.HBM((spans - 1, tiles, STATE, LANES), BF16),
            jax.ShapeDtypeStruct((tiles, 8, LANES), F32),
        ],
        scratch_shapes=[
            pltpu.VMEM((rows + EDGE, BLOCK), F32),
            pltpu.VMEM((groups, rows, LANES), F32),
            pltpu.VMEM((groups, 8, LANES), F32),
            pltpu.VMEM((spans, STATE, SPAN), BF16),
        ],
        compiler_params=pltpu.CompilerParams(vmem_limit_bytes=FRONT_LIMIT),
        cost_estimate=pl.CostEstimate(
            flops=2 * rows * 2560 * channels,
            bytes_accessed=4 * rows * channels,
            transcendentals=rows * channels,
        ),
        name="front",
    )(*in_hbm(raw_in), raw_bc, edge, cum, dt, lead, taps, offset, taps_bc, offset_bc)


def inside_kernel(x_ref, bc_ref, cum_ref, dt_ref, prior_ref, skip_ref, out_ref):
    tiles = x_ref.shape[1] // LANES
    row = lax.broadcasted_iota(jnp.int32, (SPAN, SPAN), 0)
    col = lax.broadcasted_iota(jnp.int32, (SPAN, SPAN), 1)
    lane = lax.broadcasted_iota(jnp.int32, (SPAN, LANES), 1)
    write = bc_ref[:, :STATE]
    read = bc_ref[:, STATE:]
    scores = lax.dot_general(read, write, (((1,), (1,)), ((), ())), preferred_element_type=F32)
    scores = jnp.where(row >= col, scores, 0.0)
    cum = cum_ref[...]
    cum_t = jnp.transpose(cum)
    dt_t = jnp.transpose(dt_ref[...])
    grown = jnp.where(pl.program_id(0) > 0, jnp.exp(cum), 0.0)
    for t in range(tiles):
        at = slice(t * LANES, (t + 1) * LANES)
        x = x_ref[:, at]
        both = []
        for h in (2 * t, 2 * t + 1):
            gap = jnp.minimum(cum[:, h : h + 1] - cum_t[h : h + 1, :], 0.0)
            both.append((scores * jnp.exp(gap) * dt_t[h : h + 1, :]).astype(BF16))
        zero = jnp.zeros_like(x)
        stacked = jnp.concatenate(
            [jnp.where(lane < HEADDIM, x, zero), jnp.where(lane < HEADDIM, zero, x)], axis=0
        )
        total = dot(jnp.concatenate(both, axis=1), stacked)
        total = total + skip_ref[:, at] * x.astype(F32)
        scale = jnp.where(
            lane < HEADDIM, grown[:, 2 * t : 2 * t + 1], grown[:, 2 * t + 1 : 2 * t + 2]
        )
        out_ref[:, at] = total + scale * dot(read, prior_ref[0, t])


def inside(x, bc, cum, dt, prior, skip):
    rows, channels = x.shape
    tiles = channels // LANES
    at = lambda s: (s, 0)
    return pl.pallas_call(
        inside_kernel,
        grid=(rows // SPAN,),
        in_specs=[
            pl.BlockSpec((SPAN, channels), at),
            pl.BlockSpec((SPAN, 2 * STATE), at),
            pl.BlockSpec((SPAN, LANES), at),
            pl.BlockSpec((SPAN, LANES), at),
            pl.BlockSpec((1, tiles, STATE, LANES), lambda s: (jnp.maximum(s - 1, 0), 0, 0, 0)),
            pl.BlockSpec((1, channels), lambda s: (0, 0)),
        ],
        out_specs=pl.BlockSpec((SPAN, channels), at),
        out_shape=pltpu.HBM(x.shape, F32),
        compiler_params=pltpu.CompilerParams(vmem_limit_bytes=INSIDE_LIMIT),
        cost_estimate=pl.CostEstimate(
            flops=1_000_000, bytes_accessed=1_000_000, transcendentals=0
        ),
        name="inside",
    )(*in_hbm(x, bc, cum, dt, prior), skip)


def split3(v):
    high = v.astype(BF16)
    rest = v - high.astype(F32)
    mid = rest.astype(BF16)
    return high, mid, (rest - mid.astype(F32)).astype(BF16)


def joined(message, rows):
    return (
        message[rows : rows + 1].astype(F32)
        + message[rows + 1 : rows + 2].astype(F32)
        + message[rows + 2 : rows + 3].astype(F32)
    )


def squares_rows(total):
    index = lax.broadcasted_iota(jnp.int32, (16, LANES), 0)
    high, mid, low = (p.astype(F32) for p in split3(total))
    out = jnp.where(index == 0, high, jnp.where(index == 1, mid, jnp.where(index == 2, low, 0.0)))
    return out.astype(BF16)


def tail_kernel(
    inner_total, which, read_hbm, lead_hbm, local_hbm, gate_hbm, state_ref, norm_ref, w_hbm, *refs,
):
    *outs, read_ref, lead_ref, local_ref, gate_ref, gated, w_ref, sems, w_sems = refs
    count = which.shape[0]
    channels = local_ref.shape[1]
    tiles = channels // LANES
    side_width = w_ref.shape[2]
    side_rows = side_width // LANES * SPAN

    def rows_of(i):
        span = pl.ds(pl.multiple_of(which[i] * SPAN, SPAN), SPAN)
        pairs = (
            (read_hbm, read_ref), (lead_hbm, lead_ref), (local_hbm, local_ref), (gate_hbm, gate_ref)
        )
        return [
            pltpu.make_async_copy(
                source.at[span, :], target.at[pl.ds(i * SPAN, SPAN), :], sems.at[4 * i + k]
            )
            for k, (source, target) in enumerate(pairs)
        ]

    def weights(side):
        at = slice(side * side_width, (side + 1) * side_width)
        return pltpu.make_async_copy(w_hbm.at[:, at], w_ref.at[side], w_sems.at[side])

    copies = [rows_of(i) for i in range(count)]
    for group in copies:
        for copy in group:
            copy.start()
    weights(0).start()
    sums = []
    for i in range(count):
        for copy in copies[i]:
            copy.wait()
        if i == count - 1:
            weights(1).start()
        rows = slice(i * SPAN, (i + 1) * SPAN)
        read = read_ref[rows, :]
        lead = lead_ref[rows, :]
        squares = jnp.zeros((SPAN, LANES), F32)
        for t in range(tiles):
            at = slice(t * LANES, (t + 1) * LANES)
            scale = lane_pair(lead[:, 2 * t : 2 * t + 1], lead[:, 2 * t + 1 : 2 * t + 2])
            mixed = local_ref[rows, at] + scale * dot(read, state_ref[t])
            pre = mixed * silu(gate_ref[rows, at].astype(F32))
            squares = squares + pre * pre
            gated[rows, at] = (pre * norm_ref[:, at]).astype(BF16)
        total = jnp.sum(squares, axis=1, keepdims=True) * (1.0 / inner_total)
        sums.append(jnp.transpose(jnp.broadcast_to(total, (SPAN, LANES)))[:1])
    for side in range(2):
        weights(side).wait()
        for j in range(side_width // BLOCK):
            part = dot(gated[...], w_ref[side, :, j * BLOCK : (j + 1) * BLOCK])
            part = part.astype(outs[0].dtype)
            for u in range(BLOCK // LANES):
                tile = j * (BLOCK // LANES) + u
                for i in range(count):
                    outs[2 * i + side][tile * SPAN : (tile + 1) * SPAN, :] = part[
                        i * SPAN : (i + 1) * SPAN, u * LANES : (u + 1) * LANES
                    ]
    for i in range(count):
        for side in range(2):
            out = outs[2 * i + side]
            if out.shape[0] == side_rows + 16:
                out[side_rows:, :] = squares_rows(sums[i])
    if len(outs) > 2 * count:
        outs[2 * count][...] = jnp.broadcast_to(sums[0], (8, LANES))


def tail(which, read, lead, inner, gate, state, norm, weight, squares_in):
    count = which.shape[0]
    channels = inner.shape[1]
    width = weight.shape[1]
    side_rows = width // 2 // LANES * SPAN
    vmem = pl.BlockSpec(memory_space=pltpu.VMEM)
    hbm = pl.BlockSpec(memory_space=pltpu.HBM)
    shapes = []
    for i in range(count):
        for side in range(2):
            extra = 16 if (i, side) in squares_in else 0
            shapes.append(jax.ShapeDtypeStruct((side_rows + extra, LANES), BF16))
    if not squares_in:
        shapes.append(jax.ShapeDtypeStruct((8, LANES), F32))
    rows = count * SPAN
    return pl.pallas_call(
        functools.partial(tail_kernel, HEADS * HEADDIM),
        in_specs=[pl.BlockSpec(memory_space=pltpu.SMEM)] + [hbm] * 4 + [vmem] * 2 + [hbm],
        out_specs=[vmem] * len(shapes),
        out_shape=shapes,
        scratch_shapes=[
            pltpu.VMEM((rows, STATE), BF16),
            pltpu.VMEM((rows, LANES), F32),
            pltpu.VMEM((rows, channels), F32),
            pltpu.VMEM((rows, channels), BF16),
            pltpu.VMEM((rows, channels), BF16),
            pltpu.VMEM((2, channels, width // 2), BF16),
            pltpu.SemaphoreType.DMA((4 * count,)),
            pltpu.SemaphoreType.DMA((2,)),
        ],
        compiler_params=pltpu.CompilerParams(vmem_limit_bytes=TAIL_LIMIT),
        cost_estimate=pl.CostEstimate(
            flops=2 * count * SPAN * channels * width,
            bytes_accessed=2 * channels * width,
            transcendentals=0,
        ),
    )(which, *in_hbm(read, lead, inner, gate), state, norm, *in_hbm(weight))


def merge_kernel(a_ref, b_ref, b_squares, out_ref):
    rows = a_ref.shape[0] - 16
    out_ref[:rows, :] = (a_ref[:rows, :].astype(F32) + b_ref[:rows, :].astype(F32)).astype(BF16)
    total = joined(a_ref, rows)
    if b_squares:
        total = total + joined(b_ref, rows)
    out_ref[rows:, :] = squares_rows(total)


def merge(near, relayed, with_squares):
    vmem = pl.BlockSpec(memory_space=pltpu.VMEM)

    def body(a_ref, b_ref, out_ref):
        merge_kernel(a_ref, b_ref, with_squares, out_ref)

    return pl.pallas_call(
        body,
        in_specs=[vmem] * 2,
        out_specs=vmem,
        out_shape=jax.ShapeDtypeStruct(near.shape, BF16),
        compiler_params=pltpu.CompilerParams(vmem_limit_bytes=SMALL_LIMIT),
        cost_estimate=pl.CostEstimate(flops=1000000, bytes_accessed=10**6, transcendentals=0),
    )(near, relayed)


def final_kernel(own_l, own_r, own_sq, up, down, direct_l, direct_r, out_ref):
    rows = own_l.shape[0]
    tiles = rows // SPAN
    total = own_sq[0:1, :] + joined(up, rows) + joined(down, rows)
    scale = lax.rsqrt(total + 0.25)
    column = jnp.transpose(jnp.broadcast_to(scale, (LANES, SPAN)))
    for side, parts in enumerate(((own_l, up, direct_l), (own_r, direct_r, down))):
        for t in range(tiles):
            at = slice(t * SPAN, (t + 1) * SPAN)
            added = sum(p[at, :].astype(F32) for p in parts)
            to = slice((side * tiles + t) * LANES, (side * tiles + t + 1) * LANES)
            out_ref[:, to] = (added * column).astype(BF16)


def final(*parts):
    vmem = pl.BlockSpec(memory_space=pltpu.VMEM)
    tiles = parts[0].shape[0] // SPAN
    return pl.pallas_call(
        final_kernel,
        in_specs=[vmem] * len(parts),
        out_specs=vmem,
        out_shape=jax.ShapeDtypeStruct((SPAN, 2 * tiles * LANES), BF16),
        compiler_params=pltpu.CompilerParams(vmem_limit_bytes=SMALL_LIMIT),
        cost_estimate=pl.CostEstimate(flops=1000000, bytes_accessed=10**6, transcendentals=0),
        name="final",
    )(*parts)


def ring(value, axis, distance):
    size = lax.axis_size(axis)
    return lax.ppermute(value, axis, [(i, (i + distance) % size) for i in range(size)])


def pick(values, index):
    out = values[0]
    for k in range(1, len(values)):
        out = jnp.where(index == k, values[k], out)
    return out


def packed(state, decay):
    tiles = state.shape[0]
    high = decay.astype(BF16)
    low = (decay - high.astype(F32)).astype(BF16)
    spare = jnp.zeros((16 - 2 * tiles, LANES), BF16)
    return jnp.concatenate([state.astype(BF16).reshape(-1, LANES), high, low, spare], 0)


def unpacked(message, tiles):
    rows = message.shape[0] - 16
    state = message[:rows].reshape(tiles, rows // tiles, LANES).astype(F32)
    high = message[rows : rows + tiles].astype(F32)
    low = message[rows + tiles : rows + 2 * tiles].astype(F32)
    return state, (high + low)[:, None, :]


def incoming_state(local, decay):
    z_axis, y_axis, c_axis = SEQ
    z, y, c = (lax.axis_index(a) for a in SEQ)
    ys, zs = lax.axis_size(y_axis), lax.axis_size(z_axis)
    tiles = local.shape[0] // 2
    first = c == 0
    here = jnp.where(first, local[:tiles], local[tiles:])
    there = jnp.where(first, local[tiles:], local[:tiles])
    here_d = jnp.where(first, decay[:tiles], decay[tiles:])
    there_d = jnp.where(first, decay[tiles:], decay[:tiles])

    got = ring(packed(there, there_d), c_axis, 1)
    other, other_d = unpacked(got, tiles)
    here, here_d = here.astype(F32), here_d[:, None, :]
    s0, d0 = jnp.where(first, here, other), jnp.where(first, here_d, other_d)
    s1, d1 = jnp.where(first, other, here), jnp.where(first, other_d, here_d)
    chip, chip_d = d1 * s0 + s1, d0 * d1

    part = STATE // ys
    quarters = [chip[:, q * part : (q + 1) * part] for q in range(ys)]
    sent = [pick(quarters, (y + k) % ys) for k in range(ys)]
    messages = [packed(sent[k], chip_d[:, 0]) for k in range(1, ys)]
    got = [ring(message, y_axis, k + 1) for k, message in enumerate(messages)]
    got = [unpacked(message, tiles) for message in got]
    by_shift = [(sent[0], chip_d)] + got
    states = [pick([g[0] for g in by_shift], (y - q) % ys) for q in range(ys)]
    decays = [pick([g[1] for g in by_shift], (y - q) % ys) for q in range(ys)]
    plane, plane_d = states[0], decays[0]
    for q in range(1, ys):
        plane, plane_d = decays[q] * plane + states[q], decays[q] * plane_d

    message = packed(plane, plane_d[:, 0])
    got = [ring(message, z_axis, k) for k in range(1, zs)]
    got = [unpacked(message, tiles) for message in got]
    before = jnp.zeros_like(plane)
    for q in range(zs - 1):
        s = pick([g[0] for g in got], z - q - 1)
        d = pick([g[1] for g in got], z - q - 1)
        before = jnp.where(q < z, d * before + s, before)

    prefix = [before]
    for q in range(ys - 1):
        prefix.append(decays[q] * prefix[-1] + states[q])
    sent = [pick(prefix, (y + k) % ys).astype(BF16) for k in range(ys)]
    got = [sent[0]] + [ring(sent[k], y_axis, k) for k in range(1, ys)]
    chip_in = jnp.concatenate([pick(got, (y - q) % ys) for q in range(ys)], axis=1)
    second_in = (d0 * chip_in.astype(F32) + s0).astype(BF16)
    mine = jnp.where(first, chip_in, second_in)
    message = jnp.where(first, second_in, chip_in)
    got = ring(message, c_axis, 1)
    return jnp.concatenate([jnp.where(first, mine, got), jnp.where(first, got, mine)], axis=0)


def per_device(
    tokens,
    proj_inner,
    proj_gate,
    proj_bc,
    proj_step,
    conv_inner,
    conv_bc,
    offset_inner,
    offset_bc,
    step_bias,
    decay_log,
    skip_gain,
    norm_weight,
    out_weight,
):
    devices = lax.axis_size(SEQ)
    raw_in, raw_bc, raw_step, edge, gate = raw_projections(
        tokens, proj_bc, proj_step.T, proj_inner, proj_gate
    )
    edge = lax.ppermute(edge, SEQ, [(i, i + 1) for i in range(devices - 1)])
    cum, dt, lead, *later = steps(raw_step, step_bias[None], decay_log[None])
    x, bc, read, local, prior, decay = front(
        raw_in, raw_bc, edge, cum, dt, lead, conv_inner, offset_inner[None],
        conv_bc, offset_bc[None],
    )
    state = incoming_state(local, decay[:, 0])
    skip = jnp.repeat(skip_gain, HEADDIM)[None]
    inner = inside(x, bc, *later[:2], prior, skip)

    head = lax.axis_index("head")
    size = lax.axis_size("head")

    def run(which, squares_in):
        order = jnp.stack([(head + k) & (size - 1) for k in which]).astype(jnp.int32)
        return tail(
            order, read, later[2], inner, gate, state, norm_weight[None], out_weight,
            squares_in,
        )

    def moved(value, distance):
        return ring(value, "head", distance)

    far_left, far_right = run((2,), {(0, 0), (0, 1)})
    relay_up = moved(far_left, 1)
    relay_down = moved(far_right, -1)
    next_left, next_right, last_left, last_right = run((1, 3), {(0, 0), (1, 1)})
    direct_up = moved(next_right, 1)
    direct_down = moved(last_left, -1)
    own_left, own_right, own_squares = run((0,), set())
    up = merge(next_left, relay_up, True)
    up = moved(up, 1)
    down = merge(last_right, relay_down, False)
    down = moved(down, -1)
    return final(own_left, own_right, own_squares, up, down, direct_down, direct_up)


def solution(mesh):
    torus = Mesh(
        mesh.devices.reshape(4, 4, 2, mesh.shape["head"]), ("seq_0", "seq_1", "seq_2", "head")
    )
    return jax.shard_map(
        per_device,
        mesh=torus,
        in_specs=(
            P(SEQ, None),
            P(None, "head"),
            P(None, "head"),
            P(),
            P(None, "head"),
            P(None, "head"),
            P(),
            P("head"),
            P(),
            P("head"),
            P("head"),
            P("head"),
            P("head"),
            P("head", None),
        ),
        out_specs=P(SEQ_HEAD, None),
        check_vma=False,
    )
```

```python
import functools

import jax
import jax.numpy as jnp
from jax import lax
from jax.experimental import pallas as pl
from jax.experimental.pallas import tpu as pltpu
from jax.sharding import Mesh
from jax.sharding import PartitionSpec as P


HEADS = 80
HEADDIM = 64
STATE = 128
KERNEL = 4
SPAN = 128
LANES = 128
EDGE = 8
BLOCK = 256
SEQ = ("seq_0", "seq_1", "seq_2")
SEQ_HEAD = ("seq_0", "seq_1", "seq_2", "head")

MIB = 2**20
RAW_LIMIT = 24 * MIB
FRONT_LIMIT = 24 * MIB
INSIDE_LIMIT = 12 * MIB
TAIL_LIMIT = 16 * MIB
SMALL_LIMIT = 8 * MIB


F32 = jnp.float32
BF16 = jnp.bfloat16


def in_hbm(*arrays):
    return [pltpu.with_memory_space_constraint(a, pltpu.HBM) for a in arrays]


def dot(a, b):
    return jnp.dot(a, b, preferred_element_type=F32)


def silu(v):
    return v * (0.5 + 0.5 * jnp.tanh(0.5 * v))


def lane_pair(first, second):
    lane = lax.broadcasted_iota(jnp.int32, (first.shape[0], LANES), 1)
    return jnp.where(lane < HEADDIM, first, second)


def raw_kernel(
    tok_hbm, bc_hbm, step_hbm, in_hbm, gate_hbm,
    in_out, bc_out, step_out, edge_out, gate_out,
    tok, w_bc, w_step, w_in, w_gate, inner, gate, sems,
):
    rows = tok.shape[0]
    heads = w_step.shape[0]
    first = [
        pltpu.make_async_copy(tok_hbm, tok, sems.at[0]),
        pltpu.make_async_copy(bc_hbm, w_bc, sems.at[1]),
        pltpu.make_async_copy(step_hbm, w_step, sems.at[2]),
    ]
    inner_copy = pltpu.make_async_copy(in_hbm, w_in, sems.at[3])
    gate_copy = pltpu.make_async_copy(gate_hbm, w_gate, sems.at[4])
    for copy in first:
        copy.start()
    for copy in first:
        copy.wait()
    inner_copy.start()
    bc = dot(tok[...], w_bc[...]).astype(BF16)
    bc_out[...] = bc
    edge_out[:, :BLOCK] = bc[rows - EDGE :]
    step_out[:, :heads] = lax.dot_general(
        tok[...], w_step[...], (((1,), (1,)), ((), ())), preferred_element_type=F32
    )
    inner_copy.wait()
    gate_copy.start()
    raw = dot(tok[...], w_in[...]).astype(BF16)
    inner[...] = raw
    edge_out[:, BLOCK:] = raw[rows - EDGE :]
    stored = [pltpu.make_async_copy(inner, in_out, sems.at[7])]
    stored[0].start()
    gate_copy.wait()
    half = rows // 2
    for k in range(2):
        at = slice(k * half, (k + 1) * half)
        gate[at, :] = dot(tok[at, :], w_gate[...]).astype(BF16)
        stored.append(pltpu.make_async_copy(gate.at[at, :], gate_out.at[at, :], sems.at[5 + k]))
        stored[-1].start()
    for copy in stored:
        copy.wait()


def raw_projections(tokens, w_bc, w_step, w_in, w_gate):
    rows, width = tokens.shape
    channels = w_in.shape[1]
    vmem = pl.BlockSpec(memory_space=pltpu.VMEM)
    hbm = pl.BlockSpec(memory_space=pltpu.HBM)
    return pl.pallas_call(
        raw_kernel,
        in_specs=[hbm] * 5,
        out_specs=[hbm] + [vmem] * 3 + [hbm],
        out_shape=[
            pltpu.HBM((rows, channels), BF16),
            jax.ShapeDtypeStruct((rows, BLOCK), BF16),
            jax.ShapeDtypeStruct((rows, LANES), F32),
            jax.ShapeDtypeStruct((EDGE, channels + BLOCK), BF16),
            pltpu.HBM((rows, channels), BF16),
        ],
        scratch_shapes=[
            pltpu.VMEM(tokens.shape, BF16),
            pltpu.VMEM(w_bc.shape, BF16),
            pltpu.VMEM(w_step.shape, BF16),
            pltpu.VMEM((width, channels), BF16),
            pltpu.VMEM((width, channels), BF16),
            pltpu.VMEM((rows, channels), BF16),
            pltpu.VMEM((rows, channels), BF16),
            pltpu.SemaphoreType.DMA((8,)),
        ],
        compiler_params=pltpu.CompilerParams(vmem_limit_bytes=RAW_LIMIT),
        cost_estimate=pl.CostEstimate(
            flops=2 * rows * width * (2 * channels + BLOCK + LANES),
            bytes_accessed=2 * width * (rows + 2 * channels + BLOCK),
            transcendentals=0,
        ),
        name="raw",
    )(*in_hbm(tokens, w_bc, w_step, w_in, w_gate))


def steps_kernel(raw_step, step_bias, decay_log, cum_out, dt_out, lead_out, *later):
    rows = raw_step.shape[0]
    heads = step_bias.shape[1]
    v = raw_step[:, :heads] + step_bias[...]
    dt = jnp.maximum(v, 0.0) + jnp.log1p(jnp.exp(-jnp.abs(v)))
    log_decay = -jnp.exp(decay_log[...]) * dt
    cum_out[...] = jnp.zeros_like(cum_out)
    dt_out[...] = jnp.zeros_like(dt_out)
    lead_out[...] = jnp.zeros_like(lead_out)
    dt_out[:, :heads] = dt
    row = lax.broadcasted_iota(jnp.int32, (SPAN, SPAN), 0)
    col = lax.broadcasted_iota(jnp.int32, (SPAN, SPAN), 1)
    lower = (row >= col).astype(F32)
    lead = jnp.zeros((1, heads), F32)
    for s in range(rows // SPAN):
        at = slice(s * SPAN, (s + 1) * SPAN)
        cum = jnp.dot(
            lower, log_decay[at], preferred_element_type=F32, precision=lax.Precision.HIGHEST
        )
        cum_out[at, :heads] = cum
        lead_out[at, :heads] = jnp.exp(cum + lead)
        lead = lead + cum[SPAN - 1 :, :]
    for out, value in zip(later, (cum_out, dt_out, lead_out)):
        out[...] = value[...]


def steps(raw_step, step_bias, decay_log):
    vmem = pl.BlockSpec(memory_space=pltpu.VMEM)
    return pl.pallas_call(
        steps_kernel,
        in_specs=[vmem] * 3,
        out_specs=[vmem] * 6,
        out_shape=[jax.ShapeDtypeStruct(raw_step.shape, F32)] * 3
        + [pltpu.HBM(raw_step.shape, F32)] * 3,
        compiler_params=pltpu.CompilerParams(vmem_limit_bytes=SMALL_LIMIT),
        cost_estimate=pl.CostEstimate(flops=10**9, bytes_accessed=10**6, transcendentals=0),
        name="steps",
    )(raw_step, step_bias, decay_log)


def front_kernel(
    raw_in, raw_bc, edge, cum_ref, dt_ref, lead_ref, taps, offset, taps_bc, offset_bc,
    x_out, bc_out, read_out, local_out, prior_out, decay_out,
    padded, end_w, span_d, write_t,
):
    step = pl.program_id(0)
    rows = raw_in.shape[0]
    spans = rows // SPAN
    per = BLOCK // HEADDIM
    groups = end_w.shape[0]

    def conv(raw, tap, off):
        padded[EDGE:, :] = raw[...].astype(F32)
        padded[:EDGE, :] = edge[...].astype(F32)
        total = off + tap[0:1, :] * padded[EDGE - 3 : EDGE - 3 + rows, :]
        for k in range(1, KERNEL):
            total = total + tap[k : k + 1, :] * padded[EDGE - 3 + k : EDGE - 3 + k + rows, :]
        return silu(total).astype(BF16)

    @pl.when(step == 0)
    def _():
        bc = conv(raw_bc, taps_bc, offset_bc[...])
        bc_out[...] = bc
        read_out[...] = bc[:, STATE:]
        for s in range(spans):
            block = bc[s * SPAN : (s + 1) * SPAN, :STATE].astype(F32)
            write_t[s] = jnp.transpose(block).astype(BF16)
        for s in range(spans):
            at = slice(s * SPAN, (s + 1) * SPAN)
            cum = cum_ref[at, :]
            last = cum[SPAN - 1 :, :]
            ends = jnp.exp(last - cum) * dt_ref[at, :]
            gone = jnp.exp(last)
            for g in range(groups):
                end_w[g, at, :per] = ends[:, g * per : (g + 1) * per]
                span_d[g, s : s + 1, :per] = gone[:, g * per : (g + 1) * per]
        for g in range(groups):
            span_d[g, spans : spans + 1, :per] = lead_ref[rows - 1 :, g * per : (g + 1) * per]

    @pl.when(step > 0)
    def _():
        g = step - 1
        x = conv(raw_in, taps, offset[...])
        x_out[...] = x
        ends = end_w[g]
        gone = span_d[g]
        wide = jnp.concatenate(
            [lane_pair(ends[:, t : t + 1], ends[:, t + 1 : t + 2]) for t in range(0, per, 2)], axis=1
        )
        gone_wide = jnp.concatenate(
            [lane_pair(gone[:, t : t + 1], gone[:, t + 1 : t + 2]) for t in range(0, per, 2)], axis=1
        )
        weighted = (x.astype(F32) * wide).astype(BF16)
        running = jnp.zeros((STATE, BLOCK), F32)
        tiles = BLOCK // LANES
        for s in range(spans):
            if s > 0:
                for t in range(tiles):
                    prior_out[s - 1, t] = running[:, t * LANES : (t + 1) * LANES].astype(BF16)
            local = dot(write_t[s], weighted[s * SPAN : (s + 1) * SPAN])
            running = gone_wide[s : s + 1] * running + local
        for t in range(tiles):
            local_out[t] = running[:, t * LANES : (t + 1) * LANES].astype(BF16)
            decay_out[t] = jnp.broadcast_to(
                gone_wide[spans : spans + 1, t * LANES : (t + 1) * LANES], (8, LANES)
            )


def front(raw_in, raw_bc, edge, cum, dt, lead, taps, offset, taps_bc, offset_bc):
    rows, channels = raw_in.shape
    groups = channels // BLOCK
    spans = rows // SPAN
    tiles = channels // LANES
    per_block = BLOCK // LANES

    def whole(a):
        return pl.BlockSpec(a.shape, lambda i: (0,) * a.ndim)

    def late(shape, dim):
        return pl.BlockSpec(
            shape,
            lambda i: tuple(jnp.maximum(i - 1, 0) if d == dim else 0 for d in range(len(shape))),
        )

    return pl.pallas_call(
        front_kernel,
        grid=(groups + 1,),
        in_specs=[
            late((rows, BLOCK), 1), whole(raw_bc),
            pl.BlockSpec((EDGE, BLOCK), lambda i: (0, i)),
            whole(cum), whole(dt), whole(lead),
            late((KERNEL, BLOCK), 1), late((1, BLOCK), 1),
            whole(taps_bc), whole(offset_bc),
        ],
        out_specs=[
            late((rows, BLOCK), 1),
            pl.BlockSpec((rows, 2 * STATE), lambda i: (0, 0)),
            pl.BlockSpec((rows, STATE), lambda i: (0, 0)),
            late((per_block, STATE, LANES), 0),
            late((spans - 1, per_block, STATE, LANES), 1),
            late((per_block, 8, LANES), 0),
        ],
        out_shape=[
            pltpu.HBM((rows, channels), BF16),
            pltpu.HBM((rows, 2 * STATE), BF16),
            pltpu.HBM((rows, STATE), BF16),
            jax.ShapeDtypeStruct((tiles, STATE, LANES), BF16),
            pltpu.HBM((spans - 1, tiles, STATE, LANES), BF16),
            jax.ShapeDtypeStruct((tiles, 8, LANES), F32),
        ],
        scratch_shapes=[
            pltpu.VMEM((rows + EDGE, BLOCK), F32),
            pltpu.VMEM((groups, rows, LANES), F32),
            pltpu.VMEM((groups, 8, LANES), F32),
            pltpu.VMEM((spans, STATE, SPAN), BF16),
        ],
        compiler_params=pltpu.CompilerParams(vmem_limit_bytes=FRONT_LIMIT),
        cost_estimate=pl.CostEstimate(
            flops=2 * rows * 2560 * channels,
            bytes_accessed=4 * rows * channels,
            transcendentals=rows * channels,
        ),
        name="front",
    )(*in_hbm(raw_in), raw_bc, edge, cum, dt, lead, taps, offset, taps_bc, offset_bc)


def inside_kernel(first, x_ref, bc_ref, cum_ref, dt_ref, prior_ref, skip_ref, out_ref):
    tiles = x_ref.shape[1] // LANES
    row = lax.broadcasted_iota(jnp.int32, (SPAN, SPAN), 0)
    col = lax.broadcasted_iota(jnp.int32, (SPAN, SPAN), 1)
    lane = lax.broadcasted_iota(jnp.int32, (SPAN, LANES), 1)
    write = bc_ref[:, :STATE]
    read = bc_ref[:, STATE:]
    scores = lax.dot_general(read, write, (((1,), (1,)), ((), ())), preferred_element_type=F32)
    scores = jnp.where(row >= col, scores, 0.0)
    cum = cum_ref[...]
    cum_t = jnp.transpose(cum)
    dt_t = jnp.transpose(dt_ref[...])
    grown = jnp.where(pl.program_id(0) + first > 0, jnp.exp(cum), 0.0)
    for t in range(tiles):
        at = slice(t * LANES, (t + 1) * LANES)
        x = x_ref[:, at]
        both = []
        for h in (2 * t, 2 * t + 1):
            gap = jnp.minimum(cum[:, h : h + 1] - cum_t[h : h + 1, :], 0.0)
            both.append((scores * jnp.exp(gap) * dt_t[h : h + 1, :]).astype(BF16))
        zero = jnp.zeros_like(x)
        stacked = jnp.concatenate(
            [jnp.where(lane < HEADDIM, x, zero), jnp.where(lane < HEADDIM, zero, x)], axis=0
        )
        total = dot(jnp.concatenate(both, axis=1), stacked)
        total = total + skip_ref[:, at] * x.astype(F32)
        scale = jnp.where(
            lane < HEADDIM, grown[:, 2 * t : 2 * t + 1], grown[:, 2 * t + 1 : 2 * t + 2]
        )
        out_ref[:, at] = total + scale * dot(read, prior_ref[0, t])


def inside(first, count, x, bc, cum, dt, prior, skip):
    channels = x.shape[1]
    tiles = channels // LANES
    at = lambda s: (s + first, 0)
    return pl.pallas_call(
        functools.partial(inside_kernel, first),
        grid=(count,),
        in_specs=[
            pl.BlockSpec((SPAN, channels), at),
            pl.BlockSpec((SPAN, 2 * STATE), at),
            pl.BlockSpec((SPAN, LANES), at),
            pl.BlockSpec((SPAN, LANES), at),
            pl.BlockSpec((1, tiles, STATE, LANES), lambda s: (jnp.maximum(s + first - 1, 0), 0, 0, 0)),
            pl.BlockSpec((1, channels), lambda s: (0, 0)),
        ],
        out_specs=pl.BlockSpec((SPAN, channels), lambda s: (s, 0)),
        out_shape=pltpu.HBM((count * SPAN, channels), F32),
        compiler_params=pltpu.CompilerParams(vmem_limit_bytes=INSIDE_LIMIT),
        cost_estimate=pl.CostEstimate(
            flops=1_000_000, bytes_accessed=1_000_000, transcendentals=0
        ),
        name="inside",
    )(*in_hbm(x, bc, cum, dt, prior), skip)


def split3(v):
    high = v.astype(BF16)
    rest = v - high.astype(F32)
    mid = rest.astype(BF16)
    return high, mid, (rest - mid.astype(F32)).astype(BF16)


def joined(message, rows):
    return (
        message[rows : rows + 1].astype(F32)
        + message[rows + 1 : rows + 2].astype(F32)
        + message[rows + 2 : rows + 3].astype(F32)
    )


def squares_rows(total):
    index = lax.broadcasted_iota(jnp.int32, (16, LANES), 0)
    high, mid, low = (p.astype(F32) for p in split3(total))
    out = jnp.where(index == 0, high, jnp.where(index == 1, mid, jnp.where(index == 2, low, 0.0)))
    return out.astype(BF16)


def ready_kernel(
    which, read_hbm, lead_hbm, low_hbm, high_hbm, gate_hbm, w_hbm,
    read_ref, lead_ref, local_ref, gate_ref, w_ref, sems,
):
    copies = rows_copies(
        which[0], (read_hbm, lead_hbm, gate_hbm), (read_ref, lead_ref, gate_ref), 0, sems
    )
    local = local_copies(which[0], low_hbm, high_hbm, local_ref, 0, sems.at[3])
    weights = pltpu.make_async_copy(w_hbm, w_ref, sems.at[4])
    weights.start()
    for copy in copies:
        copy.start()
    start_local(which[0], local)
    for copy in copies:
        copy.wait()
    local[0].wait()
    weights.wait()


def rows_copies(span, sources, targets, place, sems):
    at = pl.ds(pl.multiple_of(span * SPAN, SPAN), SPAN)
    return [
        pltpu.make_async_copy(
            source.at[at, :], target.at[pl.ds(place * SPAN, SPAN), :], sems.at[k]
        )
        for k, (source, target) in enumerate(zip(sources, targets))
    ]


def local_copies(span, low, high, target, place, sem):
    half = low.shape[0] // SPAN
    to = target.at[pl.ds(place * SPAN, SPAN), :]
    out = []
    for source, start in ((low, 0), (high, half)):
        row = pl.multiple_of(jnp.clip(span - start, 0, half - 1) * SPAN, SPAN)
        out.append(pltpu.make_async_copy(source.at[pl.ds(row, SPAN), :], to, sem))
    return out + [half]


def start_local(span, local):
    low, high, half = local
    pl.when(span < half)(low.start)
    pl.when(span >= half)(high.start)


def ready(which, read, lead, low, high, gate, weight):
    channels = gate.shape[1]
    vmem = pl.BlockSpec(memory_space=pltpu.VMEM)
    hbm = pl.BlockSpec(memory_space=pltpu.HBM)
    return pl.pallas_call(
        ready_kernel,
        in_specs=[pl.BlockSpec(memory_space=pltpu.SMEM)] + [hbm] * 6,
        out_specs=[vmem] * 5,
        out_shape=[
            jax.ShapeDtypeStruct((SPAN, STATE), BF16),
            jax.ShapeDtypeStruct((SPAN, LANES), F32),
            jax.ShapeDtypeStruct((SPAN, channels), F32),
            jax.ShapeDtypeStruct((SPAN, channels), BF16),
            jax.ShapeDtypeStruct(weight.shape, BF16),
        ],
        scratch_shapes=[pltpu.SemaphoreType.DMA((5,))],
        compiler_params=pltpu.CompilerParams(vmem_limit_bytes=SMALL_LIMIT),
        cost_estimate=pl.CostEstimate(flops=1000000, bytes_accessed=10**6, transcendentals=0),
        name="ready",
    )(which, *in_hbm(read, lead, low, high, gate, weight))


def tail_kernel(inner_total, has_rows, count, *refs):
    if has_rows:
        read_ref, lead_ref, local_ref, gate_ref, state_ref, norm_ref, w_ref, *outs, gated = refs
    else:
        (which, read_hbm, lead_hbm, low_hbm, high_hbm, gate_hbm, state_ref, norm_ref, w_hbm,
         *outs, read_ref, lead_ref, local_ref, gate_ref, gated, w_ref, sems, w_sems) = refs
        waits = []
        for i in range(count):
            copies = rows_copies(
                which[i], (read_hbm, lead_hbm, gate_hbm), (read_ref, lead_ref, gate_ref), i,
                sems.at[i],
            )
            local = local_copies(which[i], low_hbm, high_hbm, local_ref, i, sems.at[i, 3])
            for copy in copies:
                copy.start()
            start_local(which[i], local)
            waits.append(copies + local[:1])
        weights = []
        for side in range(2):
            at = slice(side * w_hbm.shape[1] // 2, (side + 1) * w_hbm.shape[1] // 2)
            weights.append(
                pltpu.make_async_copy(w_hbm.at[:, at], w_ref.at[:, at], w_sems.at[side])
            )
        weights[0].start()
    channels = local_ref.shape[1]
    tiles = channels // LANES
    width = w_ref.shape[1]
    side_tiles = width // 2 // LANES
    side_rows = side_tiles * SPAN
    sums = []
    for i in range(count):
        if not has_rows:
            for copy in waits[i]:
                copy.wait()
            if i == count - 1:
                weights[1].start()
        rows = slice(i * SPAN, (i + 1) * SPAN)
        read = read_ref[rows, :]
        lead = lead_ref[rows, :]
        squares = jnp.zeros((SPAN, LANES), F32)
        for t in range(tiles):
            at = slice(t * LANES, (t + 1) * LANES)
            scale = lane_pair(lead[:, 2 * t : 2 * t + 1], lead[:, 2 * t + 1 : 2 * t + 2])
            mixed = local_ref[rows, at] + scale * dot(read, state_ref[t])
            pre = mixed * silu(gate_ref[rows, at].astype(F32))
            squares = squares + pre * pre
            gated[rows, at] = (pre * norm_ref[:, at]).astype(BF16)
        total = jnp.sum(squares, axis=1, keepdims=True) * (1.0 / inner_total)
        sums.append(jnp.transpose(jnp.broadcast_to(total, (SPAN, LANES)))[:1])
    for j in range(width // BLOCK):
        if not has_rows and j * BLOCK % (width // 2) == 0:
            weights[j * BLOCK // (width // 2)].wait()
        part = dot(gated[...], w_ref[:, j * BLOCK : (j + 1) * BLOCK]).astype(outs[0].dtype)
        for u in range(BLOCK // LANES):
            side, tile = divmod(j * (BLOCK // LANES) + u, side_tiles)
            for i in range(count):
                outs[2 * i + side][tile * SPAN : (tile + 1) * SPAN, :] = part[
                    i * SPAN : (i + 1) * SPAN, u * LANES : (u + 1) * LANES
                ]
    for i in range(count):
        for side in range(2):
            out = outs[2 * i + side]
            if out.shape[0] == side_rows + 16:
                out[side_rows:, :] = squares_rows(sums[i])
    if len(outs) > 2 * count:
        outs[2 * count][...] = jnp.broadcast_to(sums[0], (8, LANES))


def tail(which, rows_in, state, norm, weight, squares_in):
    count = 1 if which is None else which.shape[0]
    channels, width = weight.shape
    side_rows = width // 2 // LANES * SPAN
    vmem = pl.BlockSpec(memory_space=pltpu.VMEM)
    hbm = pl.BlockSpec(memory_space=pltpu.HBM)
    shapes = []
    for i in range(count):
        for side in range(2):
            extra = 16 if (i, side) in squares_in else 0
            shapes.append(jax.ShapeDtypeStruct((side_rows + extra, LANES), BF16))
    if not squares_in:
        shapes.append(jax.ShapeDtypeStruct((8, LANES), F32))
    rows = count * SPAN
    gated = pltpu.VMEM((rows, channels), BF16)
    if which is None:
        in_specs, args, scratch = [vmem] * 4, list(rows_in), [gated]
    else:
        in_specs = [pl.BlockSpec(memory_space=pltpu.SMEM)] + [hbm] * 5
        args = [which, *in_hbm(*rows_in)]
        scratch = [
            pltpu.VMEM((rows, STATE), BF16),
            pltpu.VMEM((rows, LANES), F32),
            pltpu.VMEM((rows, channels), F32),
            pltpu.VMEM((rows, channels), BF16),
            gated,
            pltpu.VMEM(weight.shape, BF16),
            pltpu.SemaphoreType.DMA((count, 4)),
            pltpu.SemaphoreType.DMA((2,)),
        ]
    return pl.pallas_call(
        functools.partial(tail_kernel, HEADS * HEADDIM, which is None, count),
        in_specs=in_specs + [vmem] * 2 + [vmem if which is None else hbm],
        out_specs=[vmem] * len(shapes),
        out_shape=shapes,
        scratch_shapes=scratch,
        compiler_params=pltpu.CompilerParams(vmem_limit_bytes=TAIL_LIMIT),
        cost_estimate=pl.CostEstimate(flops=1000000, bytes_accessed=10**6, transcendentals=0),
    )(*args, state, norm, *([weight] if which is None else in_hbm(weight)))


def merge_kernel(a_ref, b_ref, b_squares, out_ref):
    rows = a_ref.shape[0] - 16
    out_ref[:rows, :] = (a_ref[:rows, :].astype(F32) + b_ref[:rows, :].astype(F32)).astype(BF16)
    total = joined(a_ref, rows)
    if b_squares:
        total = total + joined(b_ref, rows)
    out_ref[rows:, :] = squares_rows(total)


def merge(near, relayed, with_squares):
    vmem = pl.BlockSpec(memory_space=pltpu.VMEM)

    def body(a_ref, b_ref, out_ref):
        merge_kernel(a_ref, b_ref, with_squares, out_ref)

    return pl.pallas_call(
        body,
        in_specs=[vmem] * 2,
        out_specs=vmem,
        out_shape=jax.ShapeDtypeStruct(near.shape, BF16),
        compiler_params=pltpu.CompilerParams(vmem_limit_bytes=SMALL_LIMIT),
        cost_estimate=pl.CostEstimate(flops=1000000, bytes_accessed=10**6, transcendentals=0),
    )(near, relayed)


def final_kernel(own_l, own_r, own_sq, up, down, direct_l, direct_r, out_ref):
    rows = own_l.shape[0]
    tiles = rows // SPAN
    total = own_sq[0:1, :] + joined(up, rows) + joined(down, rows)
    scale = lax.rsqrt(total + 0.25)
    column = jnp.transpose(jnp.broadcast_to(scale, (LANES, SPAN)))
    for side, parts in enumerate(((own_l, up, direct_l), (own_r, direct_r, down))):
        for t in range(tiles):
            at = slice(t * SPAN, (t + 1) * SPAN)
            added = sum(p[at, :].astype(F32) for p in parts)
            to = slice((side * tiles + t) * LANES, (side * tiles + t + 1) * LANES)
            out_ref[:, to] = (added * column).astype(BF16)


def final(*parts):
    vmem = pl.BlockSpec(memory_space=pltpu.VMEM)
    tiles = parts[0].shape[0] // SPAN
    return pl.pallas_call(
        final_kernel,
        in_specs=[vmem] * len(parts),
        out_specs=vmem,
        out_shape=jax.ShapeDtypeStruct((SPAN, 2 * tiles * LANES), BF16),
        compiler_params=pltpu.CompilerParams(vmem_limit_bytes=SMALL_LIMIT),
        cost_estimate=pl.CostEstimate(flops=1000000, bytes_accessed=10**6, transcendentals=0),
        name="final",
    )(*parts)


def ring(value, axis, distance):
    size = lax.axis_size(axis)
    return lax.ppermute(value, axis, [(i, (i + distance) % size) for i in range(size)])


def pick(values, index):
    out = values[0]
    for k in range(1, len(values)):
        out = jnp.where(index == k, values[k], out)
    return out


def packed(state, decay):
    tiles = state.shape[0]
    high = decay.astype(BF16)
    low = (decay - high.astype(F32)).astype(BF16)
    spare = jnp.zeros((16 - 2 * tiles, LANES), BF16)
    return jnp.concatenate([state.astype(BF16).reshape(-1, LANES), high, low, spare], 0)


def unpacked(message, tiles):
    rows = message.shape[0] - 16
    state = message[:rows].reshape(tiles, rows // tiles, LANES).astype(F32)
    high = message[rows : rows + tiles].astype(F32)
    low = message[rows + tiles : rows + 2 * tiles].astype(F32)
    return state, (high + low)[:, None, :]


def incoming_state(local, decay):
    z_axis, y_axis, c_axis = SEQ
    z, y, c = (lax.axis_index(a) for a in SEQ)
    ys, zs = lax.axis_size(y_axis), lax.axis_size(z_axis)
    tiles = local.shape[0] // 2
    first = c == 0
    here = jnp.where(first, local[:tiles], local[tiles:])
    there = jnp.where(first, local[tiles:], local[:tiles])
    here_d = jnp.where(first, decay[:tiles], decay[tiles:])
    there_d = jnp.where(first, decay[tiles:], decay[:tiles])

    got = ring(packed(there, there_d), c_axis, 1)
    other, other_d = unpacked(got, tiles)
    here, here_d = here.astype(F32), here_d[:, None, :]
    s0, d0 = jnp.where(first, here, other), jnp.where(first, here_d, other_d)
    s1, d1 = jnp.where(first, other, here), jnp.where(first, other_d, here_d)
    chip, chip_d = d1 * s0 + s1, d0 * d1

    part = STATE // ys
    quarters = [chip[:, q * part : (q + 1) * part] for q in range(ys)]
    sent = [pick(quarters, (y + k) % ys) for k in range(ys)]
    messages = [packed(sent[k], chip_d[:, 0]) for k in range(1, ys)]
    got = [ring(message, y_axis, k + 1) for k, message in enumerate(messages)]
    got = [unpacked(message, tiles) for message in got]
    by_shift = [(sent[0], chip_d)] + got
    states = [pick([g[0] for g in by_shift], (y - q) % ys) for q in range(ys)]
    decays = [pick([g[1] for g in by_shift], (y - q) % ys) for q in range(ys)]
    plane, plane_d = states[0], decays[0]
    for q in range(1, ys):
        plane, plane_d = decays[q] * plane + states[q], decays[q] * plane_d

    message = packed(plane, plane_d[:, 0])
    got = [ring(message, z_axis, k) for k in range(1, zs)]
    got = [unpacked(message, tiles) for message in got]
    before = jnp.zeros_like(plane)
    for q in range(zs - 1):
        s = pick([g[0] for g in got], z - q - 1)
        d = pick([g[1] for g in got], z - q - 1)
        before = jnp.where(q < z, d * before + s, before)

    prefix = [before]
    for q in range(ys - 1):
        prefix.append(decays[q] * prefix[-1] + states[q])
    sent = [pick(prefix, (y + k) % ys).astype(BF16) for k in range(ys)]
    got = [sent[0]] + [ring(sent[k], y_axis, k) for k in range(1, ys)]
    chip_in = jnp.concatenate([pick(got, (y - q) % ys) for q in range(ys)], axis=1)
    second_in = (d0 * chip_in.astype(F32) + s0).astype(BF16)
    mine = jnp.where(first, chip_in, second_in)
    message = jnp.where(first, second_in, chip_in)
    got = ring(message, c_axis, 1)
    return jnp.concatenate([jnp.where(first, mine, got), jnp.where(first, got, mine)], axis=0)


def per_device(
    tokens,
    proj_inner,
    proj_gate,
    proj_bc,
    proj_step,
    conv_inner,
    conv_bc,
    offset_inner,
    offset_bc,
    step_bias,
    decay_log,
    skip_gain,
    norm_weight,
    out_weight,
):
    rows = tokens.shape[0]
    spans = rows // SPAN
    devices = lax.axis_size(SEQ)
    raw_in, raw_bc, raw_step, edge, gate = raw_projections(
        tokens, proj_bc, proj_step.T, proj_inner, proj_gate
    )
    edge = lax.ppermute(edge, SEQ, [(i, i + 1) for i in range(devices - 1)])
    cum, dt, lead, *later = steps(raw_step, step_bias[None], decay_log[None])
    x, bc, read, local, prior, decay = front(
        raw_in, raw_bc, edge, cum, dt, lead, conv_inner, offset_inner[None],
        conv_bc, offset_bc[None],
    )
    state = incoming_state(local, decay[:, 0])
    skip = jnp.repeat(skip_gain, HEADDIM)[None]
    inner = []
    for part in range(2):
        half = spans // 2
        inner.append(inside(part * half, half, x, bc, *later[:2], prior, skip))

    head = lax.axis_index("head")
    size = lax.axis_size("head")

    def order(*which):
        return jnp.stack([(head + k) & (size - 1) for k in which]).astype(jnp.int32)

    norm = norm_weight[None]
    sources = (read, later[2], *inner, gate)
    *far_rows, far_weight = ready(order(2), *sources, out_weight)

    def moved(value, distance):
        return ring(value, "head", distance)

    far_left, far_right = tail(None, far_rows, state, norm, far_weight, {(0, 0), (0, 1)})
    relay_up = moved(far_left, 1)
    relay_down = moved(far_right, -1)
    next_left, next_right, last_left, last_right = tail(
        order(1, 3), sources, state, norm, out_weight, {(0, 0), (1, 1)}
    )
    direct_up = moved(next_right, 1)
    direct_down = moved(last_left, -1)
    own_left, own_right, own_squares = tail(order(0), sources, state, norm, out_weight, set())
    up = merge(next_left, relay_up, True)
    up = moved(up, 1)
    down = merge(last_right, relay_down, False)
    down = moved(down, -1)
    return final(own_left, own_right, own_squares, up, down, direct_down, direct_up)


def solution(mesh):
    torus = Mesh(
        mesh.devices.reshape(4, 4, 2, mesh.shape["head"]), ("seq_0", "seq_1", "seq_2", "head")
    )
    return jax.shard_map(
        per_device,
        mesh=torus,
        in_specs=(
            P(SEQ, None),
            P(None, "head"),
            P(None, "head"),
            P(),
            P(None, "head"),
            P(None, "head"),
            P(),
            P("head"),
            P(),
            P("head"),
            P("head"),
            P("head"),
            P("head"),
            P("head", None),
        ),
        out_specs=P(SEQ_HEAD, None),
        check_vma=False,
    )
```

```python
import functools

import jax
import jax.numpy as jnp
from jax import lax
from jax.experimental import pallas as pl
from jax.experimental.pallas import tpu as pltpu
from jax.sharding import Mesh
from jax.sharding import PartitionSpec as P


HEADS = 80
HEADDIM = 64
STATE = 128
KERNEL = 4
SPAN = 128
LANES = 128
EDGE = 16
BLOCK = 256
SEQ = ("seq_0", "seq_1", "seq_2")
SEQ_HEAD = ("seq_0", "seq_1", "seq_2", "head")

MIB = 2**20
FIRST_LIMIT = 48 * MIB
INSIDE_LIMIT = 12 * MIB
TAIL_LIMIT = 16 * MIB
SMALL_LIMIT = 8 * MIB


F32 = jnp.float32
BF16 = jnp.bfloat16


def in_hbm(*arrays):
    return [pltpu.with_memory_space_constraint(a, pltpu.HBM) for a in arrays]


def dot(a, b):
    return jnp.dot(a, b, preferred_element_type=F32)


def silu(v):
    return v * (0.5 + 0.5 * jnp.tanh(0.5 * v))


def lane_pair(first, second):
    lane = lax.broadcasted_iota(jnp.int32, (first.shape[0], LANES), 1)
    return jnp.where(lane < HEADDIM, first, second)


def first_kernel(
    edge, tok_hbm, bc_hbm, step_hbm, in_hbm, gate_hbm, s0, s1, s2, s3, s4, s5,
    x_hbm, maps_hbm, read_hbm, cum_hbm, dt_hbm, lead_hbm, prior_hbm, gate_out, local_out, decay_out,
    tok, w_bc, w_step, w_in, w_gate, padded, padded_bc,
    x_ref, maps_ref, read_ref, cum_ref, dt_ref, lead_ref, prior_ref, gate_ref,
    taps, offset, taps_bc, offset_bc, step_bias, decay_log, sems,
):
    rows = x_ref.shape[0]
    above = edge.shape[0]
    channels = x_ref.shape[1]
    heads = step_bias.shape[1]
    spans = rows // SPAN
    per = BLOCK // HEADDIM
    tiles = BLOCK // LANES

    first = [
        pltpu.make_async_copy(tok_hbm, tok.at[pl.ds(above, rows), :], sems.at[0]),
        pltpu.make_async_copy(bc_hbm, w_bc, sems.at[1]),
        pltpu.make_async_copy(step_hbm, w_step, sems.at[2]),
    ]
    inner_copy = pltpu.make_async_copy(in_hbm, w_in, sems.at[3])
    gate_copy = pltpu.make_async_copy(gate_hbm, w_gate, sems.at[4])
    small = (taps, offset, taps_bc, offset_bc, step_bias, decay_log)
    for k, (source, target) in enumerate(zip((s0, s1, s2, s3, s4, s5), small)):
        first.append(pltpu.make_async_copy(source, target, sems.at[14 + k]))
    for copy in first:
        copy.start()
    tok[:above, :] = edge[...]
    for copy in first:
        copy.wait()
    inner_copy.start()

    def conv(source, at, tap, off):
        total = off
        for k in range(KERNEL):
            begin = above - (KERNEL - 1) + k
            total = total + tap[k : k + 1, at] * source[begin : begin + rows, at]
        return silu(total).astype(BF16)

    padded_bc[...] = dot(tok[...], w_bc[...]).astype(BF16).astype(F32)
    steps = lax.dot_general(
        tok[above:, :], w_step[...], (((1,), (1,)), ((), ())), preferred_element_type=F32
    )
    inner_copy.wait()
    gate_copy.start()
    padded[...] = dot(tok[...], w_in[...]).astype(BF16).astype(F32)

    maps = conv(padded_bc, slice(0, 2 * STATE), taps_bc, offset_bc[...])
    maps_ref[...] = maps
    read_ref[...] = maps[:, STATE:]
    v = steps + step_bias[...]
    dt = jnp.maximum(v, 0.0) + jnp.log1p(jnp.exp(-jnp.abs(v)))
    log_decay = -jnp.exp(decay_log[...]) * dt
    cum_ref[...] = jnp.zeros_like(cum_ref)
    dt_ref[...] = jnp.zeros_like(dt_ref)
    lead_ref[...] = jnp.zeros_like(lead_ref)
    dt_ref[:, :heads] = dt
    row = lax.broadcasted_iota(jnp.int32, (SPAN, SPAN), 0)
    col = lax.broadcasted_iota(jnp.int32, (SPAN, SPAN), 1)
    lower = (row >= col).astype(F32)
    lead = jnp.zeros((1, heads), F32)
    ends, gone, write_t = [], [], []
    for s in range(spans):
        at = slice(s * SPAN, (s + 1) * SPAN)
        write_t.append(jnp.transpose(maps[at, :STATE].astype(F32)).astype(BF16))
        cum = jnp.dot(
            lower, log_decay[at], preferred_element_type=F32, precision=lax.Precision.HIGHEST
        )
        cum_ref[at, :heads] = cum
        lead_ref[at, :heads] = jnp.exp(cum + lead)
        last = cum[SPAN - 1 :, :]
        lead = lead + last
        ends.append(jnp.exp(last - cum) * dt[at])
        gone.append(jnp.exp(last))
    gone.append(jnp.exp(lead))

    gate_copy.wait()
    early = [
        pltpu.make_async_copy(source, target, sems.at[5 + k])
        for k, (source, target) in enumerate(
            (
                (maps_ref, maps_hbm), (read_ref, read_hbm), (cum_ref, cum_hbm), (dt_ref, dt_hbm),
                (lead_ref, lead_hbm),
            )
        )
    ]
    for copy in early:
        copy.start()
    half = rows // 2
    gate_ref[:half, :] = dot(tok[above : above + half, :], w_gate[...]).astype(BF16)
    for g in range(channels // BLOCK):
        at = slice(g * BLOCK, (g + 1) * BLOCK)
        x = conv(padded, at, taps, offset[:, at])
        x_ref[:, at] = x
        running = jnp.zeros((STATE, BLOCK), F32)
        for s in range(spans):
            if s > 0:
                for t in range(tiles):
                    prior_ref[s - 1, g * tiles + t] = running[
                        :, t * LANES : (t + 1) * LANES
                    ].astype(BF16)

            def wide(value):
                return jnp.concatenate(
                    [
                        lane_pair(value[:, h : h + 1], value[:, h + 1 : h + 2])
                        for h in range(g * per, (g + 1) * per, 2)
                    ],
                    axis=1,
                )

            here = x[s * SPAN : (s + 1) * SPAN].astype(F32)
            local = dot(write_t[s], (here * wide(ends[s])).astype(BF16))
            running = wide(gone[s]) * running + local
        for t in range(tiles):
            to = g * tiles + t
            local_out[to] = running[:, t * LANES : (t + 1) * LANES].astype(BF16)
            h = g * per + 2 * t
            decay_out[to] = jnp.broadcast_to(
                lane_pair(gone[spans][:, h : h + 1], gone[spans][:, h + 1 : h + 2]), (8, LANES)
            )
    late = [
        pltpu.make_async_copy(x_ref, x_hbm, sems.at[10]),
        pltpu.make_async_copy(prior_ref, prior_hbm, sems.at[11]),
    ]
    for k in range(2):
        at = slice(k * half, (k + 1) * half)
        late.append(
            pltpu.make_async_copy(gate_ref.at[at, :], gate_out.at[at, :], sems.at[12 + k])
        )
    for copy in late[:3]:
        copy.start()
    gate_ref[half:, :] = dot(tok[above + half :, :], w_gate[...]).astype(BF16)
    late[3].start()
    for copy in early + late:
        copy.wait()


def first_part(edge, tokens, w_bc, w_step, w_in, w_gate, *small):
    rows, width = tokens.shape
    above = edge.shape[0]
    channels = w_in.shape[1]
    spans = rows // SPAN
    tiles = channels // LANES
    vmem = pl.BlockSpec(memory_space=pltpu.VMEM)
    hbm = pl.BlockSpec(memory_space=pltpu.HBM)
    kept = [
        ((rows, channels), BF16),
        ((rows, 2 * STATE), BF16),
        ((rows, STATE), BF16),
        ((rows, LANES), F32),
        ((rows, LANES), F32),
        ((rows, LANES), F32),
        ((spans - 1, tiles, STATE, LANES), BF16),
        ((rows, channels), BF16),
    ]
    return pl.pallas_call(
        first_kernel,
        in_specs=[vmem] + [hbm] * (5 + len(small)),
        out_specs=[hbm] * len(kept) + [vmem] * 2,
        out_shape=[pltpu.HBM(*a) for a in kept]
        + [
            jax.ShapeDtypeStruct((tiles, STATE, LANES), BF16),
            jax.ShapeDtypeStruct((tiles, 8, LANES), F32),
        ],
        scratch_shapes=[
            pltpu.VMEM((above + rows, width), BF16),
            pltpu.VMEM(w_bc.shape, BF16),
            pltpu.VMEM(w_step.shape, BF16),
            pltpu.VMEM(w_in.shape, BF16),
            pltpu.VMEM(w_gate.shape, BF16),
            pltpu.VMEM((above + rows, channels), F32),
            pltpu.VMEM((above + rows, 2 * STATE), F32),
            *[pltpu.VMEM(*a) for a in kept],
            *[pltpu.VMEM(a.shape, F32) for a in small],
            pltpu.SemaphoreType.DMA((20,)),
        ],
        compiler_params=pltpu.CompilerParams(vmem_limit_bytes=FIRST_LIMIT),
        cost_estimate=pl.CostEstimate(
            flops=2 * rows * width * (2 * channels + BLOCK + LANES),
            bytes_accessed=2 * width * (rows + 2 * channels + BLOCK),
            transcendentals=0,
        ),
        name="first",
    )(edge, *in_hbm(tokens, w_bc, w_step, w_in, w_gate, *small))


def inside_kernel(first, x_ref, bc_ref, cum_ref, dt_ref, prior_ref, skip_ref, out_ref):
    tiles = x_ref.shape[1] // LANES
    row = lax.broadcasted_iota(jnp.int32, (SPAN, SPAN), 0)
    col = lax.broadcasted_iota(jnp.int32, (SPAN, SPAN), 1)
    lane = lax.broadcasted_iota(jnp.int32, (SPAN, LANES), 1)
    write = bc_ref[:, :STATE]
    read = bc_ref[:, STATE:]
    scores = lax.dot_general(read, write, (((1,), (1,)), ((), ())), preferred_element_type=F32)
    scores = jnp.where(row >= col, scores, 0.0)
    cum = cum_ref[...]
    cum_t = jnp.transpose(cum)
    dt_t = jnp.transpose(dt_ref[...])
    grown = jnp.where(pl.program_id(0) + first > 0, jnp.exp(cum), 0.0)
    for t in range(tiles):
        at = slice(t * LANES, (t + 1) * LANES)
        x = x_ref[:, at]
        both = []
        for h in (2 * t, 2 * t + 1):
            gap = jnp.minimum(cum[:, h : h + 1] - cum_t[h : h + 1, :], 0.0)
            both.append((scores * jnp.exp(gap) * dt_t[h : h + 1, :]).astype(BF16))
        zero = jnp.zeros_like(x)
        stacked = jnp.concatenate(
            [jnp.where(lane < HEADDIM, x, zero), jnp.where(lane < HEADDIM, zero, x)], axis=0
        )
        total = dot(jnp.concatenate(both, axis=1), stacked)
        total = total + skip_ref[:, at] * x.astype(F32)
        scale = jnp.where(
            lane < HEADDIM, grown[:, 2 * t : 2 * t + 1], grown[:, 2 * t + 1 : 2 * t + 2]
        )
        out_ref[:, at] = total + scale * dot(read, prior_ref[0, t])


def inside(first, count, x, bc, cum, dt, prior, skip):
    channels = x.shape[1]
    tiles = channels // LANES
    at = lambda s: (s + first, 0)
    return pl.pallas_call(
        functools.partial(inside_kernel, first),
        grid=(count,),
        in_specs=[
            pl.BlockSpec((SPAN, channels), at),
            pl.BlockSpec((SPAN, 2 * STATE), at),
            pl.BlockSpec((SPAN, LANES), at),
            pl.BlockSpec((SPAN, LANES), at),
            pl.BlockSpec((1, tiles, STATE, LANES), lambda s: (jnp.maximum(s + first - 1, 0), 0, 0, 0)),
            pl.BlockSpec((1, channels), lambda s: (0, 0)),
        ],
        out_specs=pl.BlockSpec((SPAN, channels), lambda s: (s, 0)),
        out_shape=pltpu.HBM((count * SPAN, channels), F32),
        compiler_params=pltpu.CompilerParams(vmem_limit_bytes=INSIDE_LIMIT),
        cost_estimate=pl.CostEstimate(
            flops=1_000_000, bytes_accessed=1_000_000, transcendentals=0
        ),
        name="inside",
    )(*in_hbm(x, bc, cum, dt, prior), skip)


def split3(v):
    high = v.astype(BF16)
    rest = v - high.astype(F32)
    mid = rest.astype(BF16)
    return high, mid, (rest - mid.astype(F32)).astype(BF16)


def joined(message, rows):
    return (
        message[rows : rows + 1].astype(F32)
        + message[rows + 1 : rows + 2].astype(F32)
        + message[rows + 2 : rows + 3].astype(F32)
    )


def squares_rows(total):
    index = lax.broadcasted_iota(jnp.int32, (16, LANES), 0)
    high, mid, low = (p.astype(F32) for p in split3(total))
    out = jnp.where(index == 0, high, jnp.where(index == 1, mid, jnp.where(index == 2, low, 0.0)))
    return out.astype(BF16)


def ready_kernel(
    which, read_hbm, lead_hbm, low_hbm, high_hbm, gate_hbm, w_hbm,
    read_ref, lead_ref, local_ref, gate_ref, w_ref, sems,
):
    copies = rows_copies(
        which[0], (read_hbm, lead_hbm, gate_hbm), (read_ref, lead_ref, gate_ref), 0, sems
    )
    local = local_copies(which[0], low_hbm, high_hbm, local_ref, 0, sems.at[3])
    weights = pltpu.make_async_copy(w_hbm, w_ref, sems.at[4])
    weights.start()
    for copy in copies:
        copy.start()
    start_local(which[0], local)
    for copy in copies:
        copy.wait()
    local[0].wait()
    weights.wait()


def rows_copies(span, sources, targets, place, sems):
    at = pl.ds(pl.multiple_of(span * SPAN, SPAN), SPAN)
    return [
        pltpu.make_async_copy(
            source.at[at, :], target.at[pl.ds(place * SPAN, SPAN), :], sems.at[k]
        )
        for k, (source, target) in enumerate(zip(sources, targets))
    ]


def local_copies(span, low, high, target, place, sem):
    half = low.shape[0] // SPAN
    to = target.at[pl.ds(place * SPAN, SPAN), :]
    out = []
    for source, start in ((low, 0), (high, half)):
        row = pl.multiple_of(jnp.clip(span - start, 0, half - 1) * SPAN, SPAN)
        out.append(pltpu.make_async_copy(source.at[pl.ds(row, SPAN), :], to, sem))
    return out + [half]


def start_local(span, local):
    low, high, half = local
    pl.when(span < half)(low.start)
    pl.when(span >= half)(high.start)


def ready(which, read, lead, low, high, gate, weight):
    channels = gate.shape[1]
    vmem = pl.BlockSpec(memory_space=pltpu.VMEM)
    hbm = pl.BlockSpec(memory_space=pltpu.HBM)
    return pl.pallas_call(
        ready_kernel,
        in_specs=[pl.BlockSpec(memory_space=pltpu.SMEM)] + [hbm] * 6,
        out_specs=[vmem] * 5,
        out_shape=[
            jax.ShapeDtypeStruct((SPAN, STATE), BF16),
            jax.ShapeDtypeStruct((SPAN, LANES), F32),
            jax.ShapeDtypeStruct((SPAN, channels), F32),
            jax.ShapeDtypeStruct((SPAN, channels), BF16),
            jax.ShapeDtypeStruct(weight.shape, BF16),
        ],
        scratch_shapes=[pltpu.SemaphoreType.DMA((5,))],
        compiler_params=pltpu.CompilerParams(vmem_limit_bytes=SMALL_LIMIT),
        cost_estimate=pl.CostEstimate(flops=1000000, bytes_accessed=10**6, transcendentals=0),
        name="ready",
    )(which, *in_hbm(read, lead, low, high, gate, weight))


def tail_kernel(inner_total, has_rows, count, *refs):
    if has_rows:
        read_ref, lead_ref, local_ref, gate_ref, state_ref, norm_ref, w_ref, *outs, gated = refs
    else:
        (which, read_hbm, lead_hbm, low_hbm, high_hbm, gate_hbm, state_ref, norm_ref, w_hbm,
         *outs, read_ref, lead_ref, local_ref, gate_ref, gated, w_ref, sems, w_sems) = refs
        waits = []
        for i in range(count):
            copies = rows_copies(
                which[i], (read_hbm, lead_hbm, gate_hbm), (read_ref, lead_ref, gate_ref), i,
                sems.at[i],
            )
            local = local_copies(which[i], low_hbm, high_hbm, local_ref, i, sems.at[i, 3])
            for copy in copies:
                copy.start()
            start_local(which[i], local)
            waits.append(copies + local[:1])
        weights = []
        for side in range(2):
            at = slice(side * w_hbm.shape[1] // 2, (side + 1) * w_hbm.shape[1] // 2)
            weights.append(
                pltpu.make_async_copy(w_hbm.at[:, at], w_ref.at[:, at], w_sems.at[side])
            )
        weights[0].start()
    channels = local_ref.shape[1]
    tiles = channels // LANES
    width = w_ref.shape[1]
    side_tiles = width // 2 // LANES
    side_rows = side_tiles * SPAN
    sums = []
    for i in range(count):
        if not has_rows:
            for copy in waits[i]:
                copy.wait()
            if i == count - 1:
                weights[1].start()
        rows = slice(i * SPAN, (i + 1) * SPAN)
        read = read_ref[rows, :]
        lead = lead_ref[rows, :]
        squares = jnp.zeros((SPAN, LANES), F32)
        for t in range(tiles):
            at = slice(t * LANES, (t + 1) * LANES)
            scale = lane_pair(lead[:, 2 * t : 2 * t + 1], lead[:, 2 * t + 1 : 2 * t + 2])
            mixed = local_ref[rows, at] + scale * dot(read, state_ref[t])
            pre = mixed * silu(gate_ref[rows, at].astype(F32))
            squares = squares + pre * pre
            gated[rows, at] = (pre * norm_ref[:, at]).astype(BF16)
        total = jnp.sum(squares, axis=1, keepdims=True) * (1.0 / inner_total)
        sums.append(jnp.transpose(jnp.broadcast_to(total, (SPAN, LANES)))[:1])
    for j in range(width // BLOCK):
        if not has_rows and j * BLOCK % (width // 2) == 0:
            weights[j * BLOCK // (width // 2)].wait()
        part = dot(gated[...], w_ref[:, j * BLOCK : (j + 1) * BLOCK]).astype(outs[0].dtype)
        for u in range(BLOCK // LANES):
            side, tile = divmod(j * (BLOCK // LANES) + u, side_tiles)
            for i in range(count):
                outs[2 * i + side][tile * SPAN : (tile + 1) * SPAN, :] = part[
                    i * SPAN : (i + 1) * SPAN, u * LANES : (u + 1) * LANES
                ]
    for i in range(count):
        for side in range(2):
            out = outs[2 * i + side]
            if out.shape[0] == side_rows + 16:
                out[side_rows:, :] = squares_rows(sums[i])
    if len(outs) > 2 * count:
        outs[2 * count][...] = jnp.broadcast_to(sums[0], (8, LANES))


def tail(which, rows_in, state, norm, weight, squares_in):
    count = 1 if which is None else which.shape[0]
    channels, width = weight.shape
    side_rows = width // 2 // LANES * SPAN
    vmem = pl.BlockSpec(memory_space=pltpu.VMEM)
    hbm = pl.BlockSpec(memory_space=pltpu.HBM)
    shapes = []
    for i in range(count):
        for side in range(2):
            extra = 16 if (i, side) in squares_in else 0
            shapes.append(jax.ShapeDtypeStruct((side_rows + extra, LANES), BF16))
    if not squares_in:
        shapes.append(jax.ShapeDtypeStruct((8, LANES), F32))
    rows = count * SPAN
    gated = pltpu.VMEM((rows, channels), BF16)
    if which is None:
        in_specs, args, scratch = [vmem] * 4, list(rows_in), [gated]
    else:
        in_specs = [pl.BlockSpec(memory_space=pltpu.SMEM)] + [hbm] * 5
        args = [which, *in_hbm(*rows_in)]
        scratch = [
            pltpu.VMEM((rows, STATE), BF16),
            pltpu.VMEM((rows, LANES), F32),
            pltpu.VMEM((rows, channels), F32),
            pltpu.VMEM((rows, channels), BF16),
            gated,
            pltpu.VMEM(weight.shape, BF16),
            pltpu.SemaphoreType.DMA((count, 4)),
            pltpu.SemaphoreType.DMA((2,)),
        ]
    return pl.pallas_call(
        functools.partial(tail_kernel, HEADS * HEADDIM, which is None, count),
        in_specs=in_specs + [vmem] * 2 + [vmem if which is None else hbm],
        out_specs=[vmem] * len(shapes),
        out_shape=shapes,
        scratch_shapes=scratch,
        compiler_params=pltpu.CompilerParams(vmem_limit_bytes=TAIL_LIMIT),
        cost_estimate=pl.CostEstimate(flops=1000000, bytes_accessed=10**6, transcendentals=0),
    )(*args, state, norm, *([weight] if which is None else in_hbm(weight)))


def merge_kernel(a_ref, b_ref, b_squares, out_ref):
    rows = a_ref.shape[0] - 16
    out_ref[:rows, :] = (a_ref[:rows, :].astype(F32) + b_ref[:rows, :].astype(F32)).astype(BF16)
    total = joined(a_ref, rows)
    if b_squares:
        total = total + joined(b_ref, rows)
    out_ref[rows:, :] = squares_rows(total)


def merge(near, relayed, with_squares):
    vmem = pl.BlockSpec(memory_space=pltpu.VMEM)

    def body(a_ref, b_ref, out_ref):
        merge_kernel(a_ref, b_ref, with_squares, out_ref)

    return pl.pallas_call(
        body,
        in_specs=[vmem] * 2,
        out_specs=vmem,
        out_shape=jax.ShapeDtypeStruct(near.shape, BF16),
        compiler_params=pltpu.CompilerParams(vmem_limit_bytes=SMALL_LIMIT),
        cost_estimate=pl.CostEstimate(flops=1000000, bytes_accessed=10**6, transcendentals=0),
    )(near, relayed)


def final_kernel(own_l, own_r, own_sq, up, down, direct_l, direct_r, out_ref):
    rows = own_l.shape[0]
    tiles = rows // SPAN
    total = own_sq[0:1, :] + joined(up, rows) + joined(down, rows)
    scale = lax.rsqrt(total + 0.25)
    column = jnp.transpose(jnp.broadcast_to(scale, (LANES, SPAN)))
    for side, parts in enumerate(((own_l, up, direct_l), (own_r, direct_r, down))):
        for t in range(tiles):
            at = slice(t * SPAN, (t + 1) * SPAN)
            added = sum(p[at, :].astype(F32) for p in parts)
            to = slice((side * tiles + t) * LANES, (side * tiles + t + 1) * LANES)
            out_ref[:, to] = (added * column).astype(BF16)


def final(*parts):
    vmem = pl.BlockSpec(memory_space=pltpu.VMEM)
    tiles = parts[0].shape[0] // SPAN
    return pl.pallas_call(
        final_kernel,
        in_specs=[vmem] * len(parts),
        out_specs=vmem,
        out_shape=jax.ShapeDtypeStruct((SPAN, 2 * tiles * LANES), BF16),
        compiler_params=pltpu.CompilerParams(vmem_limit_bytes=SMALL_LIMIT),
        cost_estimate=pl.CostEstimate(flops=1000000, bytes_accessed=10**6, transcendentals=0),
        name="final",
    )(*parts)


def ring(value, axis, distance):
    size = lax.axis_size(axis)
    return lax.ppermute(value, axis, [(i, (i + distance) % size) for i in range(size)])


def pick(values, index):
    out = values[0]
    for k in range(1, len(values)):
        out = jnp.where(index == k, values[k], out)
    return out


def packed(state, decay):
    tiles = state.shape[0]
    high = decay.astype(BF16)
    low = (decay - high.astype(F32)).astype(BF16)
    spare = jnp.zeros((16 - 2 * tiles, LANES), BF16)
    return jnp.concatenate([state.astype(BF16).reshape(-1, LANES), high, low, spare], 0)


def unpacked(message, tiles):
    rows = message.shape[0] - 16
    state = message[:rows].reshape(tiles, rows // tiles, LANES).astype(F32)
    high = message[rows : rows + tiles].astype(F32)
    low = message[rows + tiles : rows + 2 * tiles].astype(F32)
    return state, (high + low)[:, None, :]


def incoming_state(local, decay):
    z_axis, y_axis, c_axis = SEQ
    z, y, c = (lax.axis_index(a) for a in SEQ)
    ys, zs = lax.axis_size(y_axis), lax.axis_size(z_axis)
    tiles = local.shape[0] // 2
    first = c == 0
    here = jnp.where(first, local[:tiles], local[tiles:])
    there = jnp.where(first, local[tiles:], local[:tiles])
    here_d = jnp.where(first, decay[:tiles], decay[tiles:])
    there_d = jnp.where(first, decay[tiles:], decay[:tiles])

    got = ring(packed(there, there_d), c_axis, 1)
    other, other_d = unpacked(got, tiles)
    here, here_d = here.astype(F32), here_d[:, None, :]
    s0, d0 = jnp.where(first, here, other), jnp.where(first, here_d, other_d)
    s1, d1 = jnp.where(first, other, here), jnp.where(first, other_d, here_d)
    chip, chip_d = d1 * s0 + s1, d0 * d1

    part = STATE // ys
    quarters = [chip[:, q * part : (q + 1) * part] for q in range(ys)]
    sent = [pick(quarters, (y + k) % ys) for k in range(ys)]
    messages = [packed(sent[k], chip_d[:, 0]) for k in range(1, ys)]
    got = [ring(message, y_axis, k + 1) for k, message in enumerate(messages)]
    got = [unpacked(message, tiles) for message in got]
    by_shift = [(sent[0], chip_d)] + got
    states = [pick([g[0] for g in by_shift], (y - q) % ys) for q in range(ys)]
    decays = [pick([g[1] for g in by_shift], (y - q) % ys) for q in range(ys)]
    plane, plane_d = states[0], decays[0]
    for q in range(1, ys):
        plane, plane_d = decays[q] * plane + states[q], decays[q] * plane_d

    message = packed(plane, plane_d[:, 0])
    got = [ring(message, z_axis, k) for k in range(1, zs)]
    got = [unpacked(message, tiles) for message in got]
    before = jnp.zeros_like(plane)
    for q in range(zs - 1):
        s = pick([g[0] for g in got], z - q - 1)
        d = pick([g[1] for g in got], z - q - 1)
        before = jnp.where(q < z, d * before + s, before)

    prefix = [before]
    for q in range(ys - 1):
        prefix.append(decays[q] * prefix[-1] + states[q])
    sent = [pick(prefix, (y + k) % ys).astype(BF16) for k in range(ys)]
    got = [sent[0]] + [ring(sent[k], y_axis, k) for k in range(1, ys)]
    chip_in = jnp.concatenate([pick(got, (y - q) % ys) for q in range(ys)], axis=1)
    second_in = (d0 * chip_in.astype(F32) + s0).astype(BF16)
    mine = jnp.where(first, chip_in, second_in)
    message = jnp.where(first, second_in, chip_in)
    got = ring(message, c_axis, 1)
    return jnp.concatenate([jnp.where(first, mine, got), jnp.where(first, got, mine)], axis=0)


def per_device(
    tokens,
    proj_inner,
    proj_gate,
    proj_bc,
    proj_step,
    conv_inner,
    conv_bc,
    offset_inner,
    offset_bc,
    step_bias,
    decay_log,
    skip_gain,
    norm_weight,
    out_weight,
):
    rows = tokens.shape[0]
    spans = rows // SPAN
    devices = lax.axis_size(SEQ)
    edge = lax.ppermute(tokens[rows - EDGE :], SEQ, [(i, i + 1) for i in range(devices - 1)])
    x, bc, read, cum, dt, lead, prior, gate, local, decay = first_part(
        edge, tokens, proj_bc, proj_step.T, proj_inner, proj_gate, conv_inner, offset_inner[None],
        conv_bc, offset_bc[None], step_bias[None], decay_log[None],
    )
    state = incoming_state(local, decay[:, 0])
    skip = jnp.repeat(skip_gain, HEADDIM)[None]
    inner = []
    for part in range(2):
        half = spans // 2
        inner.append(inside(part * half, half, x, bc, cum, dt, prior, skip))

    head = lax.axis_index("head")
    size = lax.axis_size("head")

    def order(*which):
        return jnp.stack([(head + k) & (size - 1) for k in which]).astype(jnp.int32)

    norm = norm_weight[None]
    sources = (read, lead, *inner, gate)
    *far_rows, far_weight = ready(order(2), *sources, out_weight)

    def moved(value, distance):
        return ring(value, "head", distance)

    far_left, far_right = tail(None, far_rows, state, norm, far_weight, {(0, 0), (0, 1)})
    relay_up = moved(far_left, 1)
    relay_down = moved(far_right, -1)
    next_left, next_right, last_left, last_right = tail(
        order(1, 3), sources, state, norm, out_weight, {(0, 0), (1, 1)}
    )
    direct_up = moved(next_right, 1)
    direct_down = moved(last_left, -1)
    own_left, own_right, own_squares = tail(order(0), sources, state, norm, out_weight, set())
    up = merge(next_left, relay_up, True)
    up = moved(up, 1)
    down = merge(last_right, relay_down, False)
    down = moved(down, -1)
    return final(own_left, own_right, own_squares, up, down, direct_down, direct_up)


def solution(mesh):
    torus = Mesh(
        mesh.devices.reshape(4, 4, 2, mesh.shape["head"]), ("seq_0", "seq_1", "seq_2", "head")
    )
    return jax.shard_map(
        per_device,
        mesh=torus,
        in_specs=(
            P(SEQ, None),
            P(None, "head"),
            P(None, "head"),
            P(),
            P(None, "head"),
            P(None, "head"),
            P(),
            P("head"),
            P(),
            P("head"),
            P("head"),
            P("head"),
            P("head"),
            P("head", None),
        ),
        out_specs=P(SEQ_HEAD, None),
        check_vma=False,
    )
```

```python
import functools

import jax
import jax.numpy as jnp
from jax import lax
from jax.experimental import pallas as pl
from jax.experimental.pallas import tpu as pltpu
from jax.sharding import Mesh
from jax.sharding import PartitionSpec as P


HEADS = 80
HEADDIM = 64
STATE = 128
KERNEL = 4
SPAN = 128
LANES = 128
EDGE = 16
CHUNKS = 4
PIECES = 4
BLOCK = 256
SEQ = ("seq_0", "seq_1", "seq_2")
SEQ_HEAD = ("seq_0", "seq_1", "seq_2", "head")

MIB = 2**20
FIRST_LIMIT = 48 * MIB
INSIDE_LIMIT = 12 * MIB
TAIL_LIMIT = 16 * MIB
SMALL_LIMIT = 8 * MIB


F32 = jnp.float32
BF16 = jnp.bfloat16


def in_hbm(*arrays):
    return [pltpu.with_memory_space_constraint(a, pltpu.HBM) for a in arrays]


def dot(a, b):
    return jnp.dot(a, b, preferred_element_type=F32)


def silu(v):
    return v * (0.5 + 0.5 * jnp.tanh(0.5 * v))


def lane_pair(first, second):
    lane = lax.broadcasted_iota(jnp.int32, (first.shape[0], LANES), 1)
    return jnp.where(lane < HEADDIM, first, second)


def first_kernel(
    edge, tok_hbm, bc_hbm, step_hbm, in_hbm, gate_hbm, s0, s1, s2, s3, s4, s5,
    x_hbm, maps_hbm, read_hbm, cum_hbm, dt_hbm, lead_hbm, prior_hbm, gate_out, local_out, decay_out,
    tok, w_bc, w_step, w_in, w_gate, padded, padded_bc,
    x_ref, maps_ref, read_ref, cum_ref, dt_ref, lead_ref, prior_ref, gate_ref,
    taps, taps_bc, offset_bc, step_bias, decay_log, sems,
):
    rows = x_ref.shape[0]
    above = edge.shape[0]
    channels = x_ref.shape[1]
    heads = step_bias.shape[1]
    spans = rows // SPAN
    per = BLOCK // HEADDIM
    tiles = BLOCK // LANES

    width = tok.shape[1]
    chunk = width // CHUNKS
    pairs = []
    for k in range(CHUNKS):
        at = slice(k * chunk, (k + 1) * chunk)
        pairs.append(
            [
                pltpu.make_async_copy(
                    tok_hbm.at[:, at], tok.at[pl.ds(above, rows), at], sems.at[20 + 2 * k]
                ),
                pltpu.make_async_copy(in_hbm.at[at, :], w_in.at[at, :], sems.at[21 + 2 * k]),
            ]
        )
    offset = s1
    small = (taps, offset, taps_bc, offset_bc, step_bias, decay_log)
    first = [
        pltpu.make_async_copy(bc_hbm, w_bc, sems.at[1]),
        pltpu.make_async_copy(step_hbm, w_step, sems.at[2]),
    ]
    for k, (source, target) in enumerate(zip((s0, s1, s2, s3, s4, s5), small)):
        if k != 1:
            first.append(pltpu.make_async_copy(source, target, sems.at[14 + k]))
    gate_copy = pltpu.make_async_copy(gate_hbm, w_gate, sems.at[4])
    for k in range(2):
        for copy in pairs[k]:
            copy.start()
    tok[:above, :] = edge[...]
    for k in range(CHUNKS):
        for copy in pairs[k]:
            copy.wait()
        for copy in pairs[k + 2] if k + 2 < CHUNKS else first if k + 2 == CHUNKS else [gate_copy]:
            copy.start()
        at = slice(k * chunk, (k + 1) * chunk)
        part = dot(tok[:, at], w_in[at, :])
        if k > 0:
            part = padded[...] + part
        padded[...] = part if k + 1 < CHUNKS else part.astype(BF16).astype(F32)
    for copy in first:
        copy.wait()

    def conv(source, at, tap, off):
        total = off
        for k in range(KERNEL):
            begin = above - (KERNEL - 1) + k
            total = total + tap[k : k + 1, at] * source[begin : begin + rows, at]
        return silu(total).astype(BF16)

    padded_bc[...] = dot(tok[...], w_bc[...]).astype(BF16).astype(F32)
    steps = lax.dot_general(
        tok[above:, :], w_step[...], (((1,), (1,)), ((), ())), preferred_element_type=F32
    )

    maps = conv(padded_bc, slice(0, 2 * STATE), taps_bc, offset_bc[...])
    maps_ref[...] = maps
    read_ref[...] = maps[:, STATE:]
    v = steps + step_bias[...]
    dt = jnp.maximum(v, 0.0) + jnp.log1p(jnp.exp(-jnp.abs(v)))
    log_decay = -jnp.exp(decay_log[...]) * dt
    cum_ref[...] = jnp.zeros_like(cum_ref)
    dt_ref[...] = jnp.zeros_like(dt_ref)
    lead_ref[...] = jnp.zeros_like(lead_ref)
    dt_ref[:, :heads] = dt
    row = lax.broadcasted_iota(jnp.int32, (SPAN, SPAN), 0)
    col = lax.broadcasted_iota(jnp.int32, (SPAN, SPAN), 1)
    lower = (row >= col).astype(F32)
    lead = jnp.zeros((1, heads), F32)
    ends, gone, write_t = [], [], []
    for s in range(spans):
        at = slice(s * SPAN, (s + 1) * SPAN)
        write_t.append(jnp.transpose(maps[at, :STATE].astype(F32)).astype(BF16))
        cum = jnp.dot(
            lower, log_decay[at], preferred_element_type=F32, precision=lax.Precision.HIGHEST
        )
        cum_ref[at, :heads] = cum
        lead_ref[at, :heads] = jnp.exp(cum + lead)
        last = cum[SPAN - 1 :, :]
        lead = lead + last
        ends.append(jnp.exp(last - cum) * dt[at])
        gone.append(jnp.exp(last))
    gone.append(jnp.exp(lead))

    gate_copy.wait()
    early = [
        pltpu.make_async_copy(source, target, sems.at[5 + k])
        for k, (source, target) in enumerate(
            (
                (maps_ref, maps_hbm), (read_ref, read_hbm), (cum_ref, cum_hbm), (dt_ref, dt_hbm),
                (lead_ref, lead_hbm),
            )
        )
    ]
    for copy in early:
        copy.start()
    half = rows // 2
    gate_ref[:half, :] = dot(tok[above : above + half, :], w_gate[...]).astype(BF16)
    for g in range(channels // BLOCK):
        at = slice(g * BLOCK, (g + 1) * BLOCK)
        x = conv(padded, at, taps, offset[:, at])
        x_ref[:, at] = x
        running = jnp.zeros((STATE, BLOCK), F32)
        for s in range(spans):
            if s > 0:
                for t in range(tiles):
                    prior_ref[s - 1, g * tiles + t] = running[
                        :, t * LANES : (t + 1) * LANES
                    ].astype(BF16)

            def wide(value):
                return jnp.concatenate(
                    [
                        lane_pair(value[:, h : h + 1], value[:, h + 1 : h + 2])
                        for h in range(g * per, (g + 1) * per, 2)
                    ],
                    axis=1,
                )

            here = x[s * SPAN : (s + 1) * SPAN].astype(F32)
            local = dot(write_t[s], (here * wide(ends[s])).astype(BF16))
            running = wide(gone[s]) * running + local
        for t in range(tiles):
            to = g * tiles + t
            local_out[to] = running[:, t * LANES : (t + 1) * LANES].astype(BF16)
            h = g * per + 2 * t
            decay_out[to] = jnp.broadcast_to(
                lane_pair(gone[spans][:, h : h + 1], gone[spans][:, h + 1 : h + 2]), (8, LANES)
            )
    late = [
        pltpu.make_async_copy(x_ref, x_hbm, sems.at[10]),
        pltpu.make_async_copy(prior_ref, prior_hbm, sems.at[11]),
    ]
    for k in range(2):
        at = slice(k * half, (k + 1) * half)
        late.append(
            pltpu.make_async_copy(gate_ref.at[at, :], gate_out.at[at, :], sems.at[12 + k])
        )
    for copy in late[:3]:
        copy.start()
    gate_ref[half:, :] = dot(tok[above + half :, :], w_gate[...]).astype(BF16)
    late[3].start()
    for copy in early + late:
        copy.wait()


def first_part(edge, tokens, w_bc, w_step, w_in, w_gate, *small):
    rows, width = tokens.shape
    above = edge.shape[0]
    channels = w_in.shape[1]
    spans = rows // SPAN
    tiles = channels // LANES
    vmem = pl.BlockSpec(memory_space=pltpu.VMEM)
    hbm = pl.BlockSpec(memory_space=pltpu.HBM)
    kept = [
        ((rows, channels), BF16),
        ((rows, 2 * STATE), BF16),
        ((rows, STATE), BF16),
        ((rows, LANES), F32),
        ((rows, LANES), F32),
        ((rows, LANES), F32),
        ((spans - 1, tiles, STATE, LANES), BF16),
        ((rows, channels), BF16),
    ]
    return pl.pallas_call(
        first_kernel,
        in_specs=[vmem] + [hbm] * 6 + [vmem] + [hbm] * 4,
        out_specs=[hbm] * len(kept) + [vmem] * 2,
        out_shape=[pltpu.HBM(*a) for a in kept]
        + [
            jax.ShapeDtypeStruct((tiles, STATE, LANES), BF16),
            jax.ShapeDtypeStruct((tiles, 8, LANES), F32),
        ],
        scratch_shapes=[
            pltpu.VMEM((above + rows, width), BF16),
            pltpu.VMEM(w_bc.shape, BF16),
            pltpu.VMEM(w_step.shape, BF16),
            pltpu.VMEM(w_in.shape, BF16),
            pltpu.VMEM(w_gate.shape, BF16),
            pltpu.VMEM((above + rows, channels), F32),
            pltpu.VMEM((above + rows, 2 * STATE), F32),
            *[pltpu.VMEM(*a) for a in kept],
            *[pltpu.VMEM(a.shape, F32) for k, a in enumerate(small) if k != 1],
            pltpu.SemaphoreType.DMA((20 + 2 * CHUNKS,)),
        ],
        compiler_params=pltpu.CompilerParams(vmem_limit_bytes=FIRST_LIMIT),
        cost_estimate=pl.CostEstimate(
            flops=2 * rows * width * (2 * channels + BLOCK + LANES),
            bytes_accessed=2 * width * (rows + 2 * channels + BLOCK),
            transcendentals=0,
        ),
        name="first",
    )(edge, *in_hbm(tokens, w_bc, w_step, w_in, w_gate, small[0]), small[1], *in_hbm(*small[2:]))


def inside_kernel(first, x_ref, bc_ref, cum_ref, dt_ref, prior_ref, skip_ref, out_ref):
    tiles = x_ref.shape[1] // LANES
    row = lax.broadcasted_iota(jnp.int32, (SPAN, SPAN), 0)
    col = lax.broadcasted_iota(jnp.int32, (SPAN, SPAN), 1)
    lane = lax.broadcasted_iota(jnp.int32, (SPAN, LANES), 1)
    write = bc_ref[:, :STATE]
    read = bc_ref[:, STATE:]
    scores = lax.dot_general(read, write, (((1,), (1,)), ((), ())), preferred_element_type=F32)
    scores = jnp.where(row >= col, scores, 0.0)
    cum = cum_ref[...]
    cum_t = jnp.transpose(cum)
    dt_t = jnp.transpose(dt_ref[...])
    grown = jnp.where(pl.program_id(0) + first > 0, jnp.exp(cum), 0.0)
    for t in range(tiles):
        at = slice(t * LANES, (t + 1) * LANES)
        x = x_ref[:, at]
        both = []
        for h in (2 * t, 2 * t + 1):
            gap = jnp.minimum(cum[:, h : h + 1] - cum_t[h : h + 1, :], 0.0)
            both.append((scores * jnp.exp(gap) * dt_t[h : h + 1, :]).astype(BF16))
        zero = jnp.zeros_like(x)
        stacked = jnp.concatenate(
            [jnp.where(lane < HEADDIM, x, zero), jnp.where(lane < HEADDIM, zero, x)], axis=0
        )
        total = dot(jnp.concatenate(both, axis=1), stacked)
        total = total + skip_ref[:, at] * x.astype(F32)
        scale = jnp.where(
            lane < HEADDIM, grown[:, 2 * t : 2 * t + 1], grown[:, 2 * t + 1 : 2 * t + 2]
        )
        out_ref[:, at] = total + scale * dot(read, prior_ref[0, t])


def inside(first, count, x, bc, cum, dt, prior, skip):
    channels = x.shape[1]
    tiles = channels // LANES
    at = lambda s: (s + first, 0)
    return pl.pallas_call(
        functools.partial(inside_kernel, first),
        grid=(count,),
        in_specs=[
            pl.BlockSpec((SPAN, channels), at),
            pl.BlockSpec((SPAN, 2 * STATE), at),
            pl.BlockSpec((SPAN, LANES), at),
            pl.BlockSpec((SPAN, LANES), at),
            pl.BlockSpec((1, tiles, STATE, LANES), lambda s: (jnp.maximum(s + first - 1, 0), 0, 0, 0)),
            pl.BlockSpec((1, channels), lambda s: (0, 0)),
        ],
        out_specs=pl.BlockSpec((SPAN, channels), lambda s: (s, 0)),
        out_shape=pltpu.HBM((count * SPAN, channels), F32),
        compiler_params=pltpu.CompilerParams(vmem_limit_bytes=INSIDE_LIMIT),
        cost_estimate=pl.CostEstimate(
            flops=1_000_000, bytes_accessed=1_000_000, transcendentals=0
        ),
        name="inside",
    )(*in_hbm(x, bc, cum, dt, prior), skip)


def split3(v):
    high = v.astype(BF16)
    rest = v - high.astype(F32)
    mid = rest.astype(BF16)
    return high, mid, (rest - mid.astype(F32)).astype(BF16)


def joined(message, rows):
    return (
        message[rows : rows + 1].astype(F32)
        + message[rows + 1 : rows + 2].astype(F32)
        + message[rows + 2 : rows + 3].astype(F32)
    )


def squares_rows(total):
    index = lax.broadcasted_iota(jnp.int32, (16, LANES), 0)
    high, mid, low = (p.astype(F32) for p in split3(total))
    out = jnp.where(index == 0, high, jnp.where(index == 1, mid, jnp.where(index == 2, low, 0.0)))
    return out.astype(BF16)


def ready_kernel(
    which, read_hbm, lead_hbm, low_hbm, high_hbm, gate_hbm, w_hbm,
    read_ref, lead_ref, local_ref, gate_ref, w_ref, sems,
):
    copies = rows_copies(
        which[0], (read_hbm, lead_hbm, gate_hbm), (read_ref, lead_ref, gate_ref), 0, sems
    )
    local = local_copies(which[0], low_hbm, high_hbm, local_ref, 0, sems.at[3])
    weights = pltpu.make_async_copy(w_hbm, w_ref, sems.at[4])
    weights.start()
    for copy in copies:
        copy.start()
    start_local(which[0], local)
    for copy in copies:
        copy.wait()
    local[0].wait()
    weights.wait()


def rows_copies(span, sources, targets, place, sems):
    at = pl.ds(pl.multiple_of(span * SPAN, SPAN), SPAN)
    return [
        pltpu.make_async_copy(
            source.at[at, :], target.at[pl.ds(place * SPAN, SPAN), :], sems.at[k]
        )
        for k, (source, target) in enumerate(zip(sources, targets))
    ]


def local_copies(span, low, high, target, place, sem):
    half = low.shape[0] // SPAN
    to = target.at[pl.ds(place * SPAN, SPAN), :]
    out = []
    for source, start in ((low, 0), (high, half)):
        row = pl.multiple_of(jnp.clip(span - start, 0, half - 1) * SPAN, SPAN)
        out.append(pltpu.make_async_copy(source.at[pl.ds(row, SPAN), :], to, sem))
    return out + [half]


def start_local(span, local):
    low, high, half = local
    pl.when(span < half)(low.start)
    pl.when(span >= half)(high.start)


def ready(which, read, lead, low, high, gate, weight):
    channels = gate.shape[1]
    vmem = pl.BlockSpec(memory_space=pltpu.VMEM)
    hbm = pl.BlockSpec(memory_space=pltpu.HBM)
    return pl.pallas_call(
        ready_kernel,
        in_specs=[pl.BlockSpec(memory_space=pltpu.SMEM)] + [hbm] * 6,
        out_specs=[vmem] * 5,
        out_shape=[
            jax.ShapeDtypeStruct((SPAN, STATE), BF16),
            jax.ShapeDtypeStruct((SPAN, LANES), F32),
            jax.ShapeDtypeStruct((SPAN, channels), F32),
            jax.ShapeDtypeStruct((SPAN, channels), BF16),
            jax.ShapeDtypeStruct(weight.shape, BF16),
        ],
        scratch_shapes=[pltpu.SemaphoreType.DMA((5,))],
        compiler_params=pltpu.CompilerParams(vmem_limit_bytes=SMALL_LIMIT),
        cost_estimate=pl.CostEstimate(flops=1000000, bytes_accessed=10**6, transcendentals=0),
        name="ready",
    )(which, *in_hbm(read, lead, low, high, gate, weight))


def tail_kernel(inner_total, has_rows, count, *refs):
    if has_rows:
        read_ref, lead_ref, local_ref, gate_ref, state_ref, norm_ref, w_ref, *outs, gated = refs
    else:
        (which, read_hbm, lead_hbm, low_hbm, high_hbm, gate_hbm, state_ref, norm_ref, w_hbm,
         *outs, read_ref, lead_ref, local_ref, gate_ref, gated, w_ref, sems, w_sems) = refs
        waits = []
        for i in range(count):
            copies = rows_copies(
                which[i], (read_hbm, lead_hbm, gate_hbm), (read_ref, lead_ref, gate_ref), i,
                sems.at[i],
            )
            local = local_copies(which[i], low_hbm, high_hbm, local_ref, i, sems.at[i, 3])
            for copy in copies:
                copy.start()
            start_local(which[i], local)
            waits.append(copies + local[:1])
        weights = []
        piece = w_hbm.shape[1] // PIECES
        for k in range(PIECES):
            at = slice(k * piece, (k + 1) * piece)
            weights.append(
                pltpu.make_async_copy(w_hbm.at[:, at], w_ref.at[:, at], w_sems.at[k])
            )
        weights[0].start()
    channels = local_ref.shape[1]
    tiles = channels // LANES
    width = w_ref.shape[1]
    side_tiles = width // 2 // LANES
    side_rows = side_tiles * SPAN
    sums = []
    for i in range(count):
        if not has_rows:
            for copy in waits[i]:
                copy.wait()
            if i == 0:
                weights[1].start()
            if i == count - 1:
                weights[2].start()
        rows = slice(i * SPAN, (i + 1) * SPAN)
        read = read_ref[rows, :]
        lead = lead_ref[rows, :]
        squares = jnp.zeros((SPAN, LANES), F32)
        for t in range(tiles):
            at = slice(t * LANES, (t + 1) * LANES)
            scale = lane_pair(lead[:, 2 * t : 2 * t + 1], lead[:, 2 * t + 1 : 2 * t + 2])
            mixed = local_ref[rows, at] + scale * dot(read, state_ref[t])
            pre = mixed * silu(gate_ref[rows, at].astype(F32))
            squares = squares + pre * pre
            gated[rows, at] = (pre * norm_ref[:, at]).astype(BF16)
        total = jnp.sum(squares, axis=1, keepdims=True) * (1.0 / inner_total)
        sums.append(jnp.transpose(jnp.broadcast_to(total, (SPAN, LANES)))[:1])
    arrived = 0
    for j in range(width // BLOCK):
        if not has_rows:
            needed = ((j + 1) * BLOCK - 1) // (width // PIECES)
            if needed == arrived:
                weights[arrived].wait()
                arrived += 1
                if arrived + 1 < PIECES and arrived > 1:
                    weights[arrived + 1].start()
        part = dot(gated[...], w_ref[:, j * BLOCK : (j + 1) * BLOCK]).astype(outs[0].dtype)
        for u in range(BLOCK // LANES):
            side, tile = divmod(j * (BLOCK // LANES) + u, side_tiles)
            for i in range(count):
                outs[2 * i + side][tile * SPAN : (tile + 1) * SPAN, :] = part[
                    i * SPAN : (i + 1) * SPAN, u * LANES : (u + 1) * LANES
                ]
    for i in range(count):
        for side in range(2):
            out = outs[2 * i + side]
            if out.shape[0] == side_rows + 16:
                out[side_rows:, :] = squares_rows(sums[i])
    if len(outs) > 2 * count:
        outs[2 * count][...] = jnp.broadcast_to(sums[0], (8, LANES))


def tail(which, rows_in, state, norm, weight, squares_in):
    count = 1 if which is None else which.shape[0]
    channels, width = weight.shape
    side_rows = width // 2 // LANES * SPAN
    vmem = pl.BlockSpec(memory_space=pltpu.VMEM)
    hbm = pl.BlockSpec(memory_space=pltpu.HBM)
    shapes = []
    for i in range(count):
        for side in range(2):
            extra = 16 if (i, side) in squares_in else 0
            shapes.append(jax.ShapeDtypeStruct((side_rows + extra, LANES), BF16))
    if not squares_in:
        shapes.append(jax.ShapeDtypeStruct((8, LANES), F32))
    rows = count * SPAN
    gated = pltpu.VMEM((rows, channels), BF16)
    if which is None:
        in_specs, args, scratch = [vmem] * 4, list(rows_in), [gated]
    else:
        in_specs = [pl.BlockSpec(memory_space=pltpu.SMEM)] + [hbm] * 5
        args = [which, *in_hbm(*rows_in)]
        scratch = [
            pltpu.VMEM((rows, STATE), BF16),
            pltpu.VMEM((rows, LANES), F32),
            pltpu.VMEM((rows, channels), F32),
            pltpu.VMEM((rows, channels), BF16),
            gated,
            pltpu.VMEM(weight.shape, BF16),
            pltpu.SemaphoreType.DMA((count, 4)),
            pltpu.SemaphoreType.DMA((PIECES,)),
        ]
    return pl.pallas_call(
        functools.partial(tail_kernel, HEADS * HEADDIM, which is None, count),
        in_specs=in_specs + [vmem] * 2 + [vmem if which is None else hbm],
        out_specs=[vmem] * len(shapes),
        out_shape=shapes,
        scratch_shapes=scratch,
        compiler_params=pltpu.CompilerParams(vmem_limit_bytes=TAIL_LIMIT),
        cost_estimate=pl.CostEstimate(flops=1000000, bytes_accessed=10**6, transcendentals=0),
    )(*args, state, norm, *([weight] if which is None else in_hbm(weight)))


def merge_kernel(a_ref, b_ref, b_squares, out_ref):
    rows = a_ref.shape[0] - 16
    out_ref[:rows, :] = (a_ref[:rows, :].astype(F32) + b_ref[:rows, :].astype(F32)).astype(BF16)
    total = joined(a_ref, rows)
    if b_squares:
        total = total + joined(b_ref, rows)
    out_ref[rows:, :] = squares_rows(total)


def merge(near, relayed, with_squares):
    vmem = pl.BlockSpec(memory_space=pltpu.VMEM)

    def body(a_ref, b_ref, out_ref):
        merge_kernel(a_ref, b_ref, with_squares, out_ref)

    return pl.pallas_call(
        body,
        in_specs=[vmem] * 2,
        out_specs=vmem,
        out_shape=jax.ShapeDtypeStruct(near.shape, BF16),
        compiler_params=pltpu.CompilerParams(vmem_limit_bytes=SMALL_LIMIT),
        cost_estimate=pl.CostEstimate(flops=1000000, bytes_accessed=10**6, transcendentals=0),
    )(near, relayed)


def final_kernel(own_l, own_r, own_sq, up, down, direct_l, direct_r, out_ref):
    rows = own_l.shape[0]
    tiles = rows // SPAN
    total = own_sq[0:1, :] + joined(up, rows) + joined(down, rows)
    scale = lax.rsqrt(total + 0.25)
    column = jnp.transpose(jnp.broadcast_to(scale, (LANES, SPAN)))
    for side, parts in enumerate(((own_l, up, direct_l), (own_r, direct_r, down))):
        for t in range(tiles):
            at = slice(t * SPAN, (t + 1) * SPAN)
            added = sum(p[at, :].astype(F32) for p in parts)
            to = slice((side * tiles + t) * LANES, (side * tiles + t + 1) * LANES)
            out_ref[:, to] = (added * column).astype(BF16)


def final(*parts):
    vmem = pl.BlockSpec(memory_space=pltpu.VMEM)
    tiles = parts[0].shape[0] // SPAN
    return pl.pallas_call(
        final_kernel,
        in_specs=[vmem] * len(parts),
        out_specs=vmem,
        out_shape=jax.ShapeDtypeStruct((SPAN, 2 * tiles * LANES), BF16),
        compiler_params=pltpu.CompilerParams(vmem_limit_bytes=SMALL_LIMIT),
        cost_estimate=pl.CostEstimate(flops=1000000, bytes_accessed=10**6, transcendentals=0),
        name="final",
    )(*parts)


def ring(value, axis, distance):
    size = lax.axis_size(axis)
    return lax.ppermute(value, axis, [(i, (i + distance) % size) for i in range(size)])


def pick(values, index):
    out = values[0]
    for k in range(1, len(values)):
        out = jnp.where(index == k, values[k], out)
    return out


def packed(state, decay):
    tiles = state.shape[0]
    high = decay.astype(BF16)
    low = (decay - high.astype(F32)).astype(BF16)
    spare = jnp.zeros((16 - 2 * tiles, LANES), BF16)
    return jnp.concatenate([state.astype(BF16).reshape(-1, LANES), high, low, spare], 0)


def unpacked(message, tiles):
    rows = message.shape[0] - 16
    state = message[:rows].reshape(tiles, rows // tiles, LANES).astype(F32)
    high = message[rows : rows + tiles].astype(F32)
    low = message[rows + tiles : rows + 2 * tiles].astype(F32)
    return state, (high + low)[:, None, :]


def incoming_state(local, decay):
    z_axis, y_axis, c_axis = SEQ
    z, y, c = (lax.axis_index(a) for a in SEQ)
    ys, zs = lax.axis_size(y_axis), lax.axis_size(z_axis)
    tiles = local.shape[0] // 2
    first = c == 0
    here = jnp.where(first, local[:tiles], local[tiles:])
    there = jnp.where(first, local[tiles:], local[:tiles])
    here_d = jnp.where(first, decay[:tiles], decay[tiles:])
    there_d = jnp.where(first, decay[tiles:], decay[:tiles])

    got = ring(packed(there, there_d), c_axis, 1)
    other, other_d = unpacked(got, tiles)
    here, here_d = here.astype(F32), here_d[:, None, :]
    s0, d0 = jnp.where(first, here, other), jnp.where(first, here_d, other_d)
    s1, d1 = jnp.where(first, other, here), jnp.where(first, other_d, here_d)
    chip, chip_d = d1 * s0 + s1, d0 * d1

    part = STATE // ys
    quarters = [chip[:, q * part : (q + 1) * part] for q in range(ys)]
    sent = [pick(quarters, (y + k) % ys) for k in range(ys)]
    messages = [packed(sent[k], chip_d[:, 0]) for k in range(1, ys)]
    got = [ring(message, y_axis, k + 1) for k, message in enumerate(messages)]
    got = [unpacked(message, tiles) for message in got]
    by_shift = [(sent[0], chip_d)] + got
    states = [pick([g[0] for g in by_shift], (y - q) % ys) for q in range(ys)]
    decays = [pick([g[1] for g in by_shift], (y - q) % ys) for q in range(ys)]
    plane, plane_d = states[0], decays[0]
    for q in range(1, ys):
        plane, plane_d = decays[q] * plane + states[q], decays[q] * plane_d

    message = packed(plane, plane_d[:, 0])
    got = [ring(message, z_axis, k) for k in range(1, zs)]
    got = [unpacked(message, tiles) for message in got]
    before = jnp.zeros_like(plane)
    for q in range(zs - 1):
        s = pick([g[0] for g in got], z - q - 1)
        d = pick([g[1] for g in got], z - q - 1)
        before = jnp.where(q < z, d * before + s, before)

    prefix = [before]
    for q in range(ys - 1):
        prefix.append(decays[q] * prefix[-1] + states[q])
    sent = [pick(prefix, (y + k) % ys).astype(BF16) for k in range(ys)]
    got = [sent[0]] + [ring(sent[k], y_axis, k) for k in range(1, ys)]
    chip_in = jnp.concatenate([pick(got, (y - q) % ys) for q in range(ys)], axis=1)
    second_in = (d0 * chip_in.astype(F32) + s0).astype(BF16)
    mine = jnp.where(first, chip_in, second_in)
    message = jnp.where(first, second_in, chip_in)
    got = ring(message, c_axis, 1)
    return jnp.concatenate([jnp.where(first, mine, got), jnp.where(first, got, mine)], axis=0)


def per_device(
    tokens,
    proj_inner,
    proj_gate,
    proj_bc,
    proj_step,
    conv_inner,
    conv_bc,
    offset_inner,
    offset_bc,
    step_bias,
    decay_log,
    skip_gain,
    norm_weight,
    out_weight,
):
    rows = tokens.shape[0]
    spans = rows // SPAN
    devices = lax.axis_size(SEQ)
    edge = lax.ppermute(tokens[rows - EDGE :], SEQ, [(i, i + 1) for i in range(devices - 1)])
    x, bc, read, cum, dt, lead, prior, gate, local, decay = first_part(
        edge, tokens, proj_bc, proj_step.T, proj_inner, proj_gate, conv_inner, offset_inner[None],
        conv_bc, offset_bc[None], step_bias[None], decay_log[None],
    )
    state = incoming_state(local, decay[:, 0])
    skip = jnp.repeat(skip_gain, HEADDIM)[None]
    inner = []
    for part in range(2):
        half = spans // 2
        inner.append(inside(part * half, half, x, bc, cum, dt, prior, skip))

    head = lax.axis_index("head")
    size = lax.axis_size("head")

    def order(*which):
        return jnp.stack([(head + k) & (size - 1) for k in which]).astype(jnp.int32)

    norm = norm_weight[None]
    sources = (read, lead, *inner, gate)
    *far_rows, far_weight = ready(order(2), *sources, out_weight)

    def moved(value, distance):
        return ring(value, "head", distance)

    far_left, far_right = tail(None, far_rows, state, norm, far_weight, {(0, 0), (0, 1)})
    relay_up = moved(far_left, 1)
    relay_down = moved(far_right, -1)
    next_left, next_right, last_left, last_right = tail(
        order(1, 3), sources, state, norm, out_weight, {(0, 0), (1, 1)}
    )
    direct_up = moved(next_right, 1)
    direct_down = moved(last_left, -1)
    own_left, own_right, own_squares = tail(order(0), sources, state, norm, out_weight, set())
    up = merge(next_left, relay_up, True)
    up = moved(up, 1)
    down = merge(last_right, relay_down, False)
    down = moved(down, -1)
    return final(own_left, own_right, own_squares, up, down, direct_down, direct_up)


def solution(mesh):
    torus = Mesh(
        mesh.devices.reshape(4, 4, 2, mesh.shape["head"]), ("seq_0", "seq_1", "seq_2", "head")
    )
    return jax.shard_map(
        per_device,
        mesh=torus,
        in_specs=(
            P(SEQ, None),
            P(None, "head"),
            P(None, "head"),
            P(),
            P(None, "head"),
            P(None, "head"),
            P(),
            P("head"),
            P(),
            P("head"),
            P("head"),
            P("head"),
            P("head"),
            P("head", None),
        ),
        out_specs=P(SEQ_HEAD, None),
        check_vma=False,
    )
```

```python
import functools

import jax
import jax.numpy as jnp
from jax import lax
from jax.experimental import pallas as pl
from jax.experimental.pallas import tpu as pltpu
from jax.sharding import Mesh
from jax.sharding import PartitionSpec as P


HEADS = 80
HEADDIM = 64
STATE = 128
KERNEL = 4
SPAN = 128
LANES = 128
EDGE = 16
BLOCK = 256
SEQ = ("seq_0", "seq_1", "seq_2")
SEQ_HEAD = ("seq_0", "seq_1", "seq_2", "head")

MIB = 2**20
FIRST_LIMIT = 48 * MIB
INSIDE_LIMIT = 12 * MIB
TAIL_LIMIT = 16 * MIB
SMALL_LIMIT = 8 * MIB


F32 = jnp.float32
BF16 = jnp.bfloat16


def in_hbm(*arrays):
    return [pltpu.with_memory_space_constraint(a, pltpu.HBM) for a in arrays]


def dot(a, b):
    return jnp.dot(a, b, preferred_element_type=F32)


def silu(v):
    return v * (0.5 + 0.5 * jnp.tanh(0.5 * v))


def lane_pair(first, second):
    lane = lax.broadcasted_iota(jnp.int32, (first.shape[0], LANES), 1)
    return jnp.where(lane < HEADDIM, first, second)


def first_kernel(
    edge, tok_hbm, bc_hbm, step_hbm, in_hbm, gate_hbm, s0, s1, s2, s3, s4, s5,
    x_hbm, maps_hbm, read_hbm, cum_hbm, dt_hbm, lead_hbm, prior_hbm, gate_out, local_out, decay_out,
    tok, w_bc, w_step, w_wide, padded, padded_bc, ends, gone, write_t,
    x_ref, maps_ref, read_ref, cum_ref, dt_ref, lead_ref, prior_ref, gate_ref,
    taps, offset, taps_bc, offset_bc, step_bias, decay_log, sems,
):
    rows = x_ref.shape[0]
    above = edge.shape[0]
    channels = x_ref.shape[1]
    heads = step_bias.shape[1]
    spans = rows // SPAN
    side = channels // 2
    first = [
        pltpu.make_async_copy(tok_hbm, tok.at[pl.ds(above, rows), :], sems.at[0]),
        pltpu.make_async_copy(bc_hbm, w_bc, sems.at[1]),
        pltpu.make_async_copy(step_hbm, w_step, sems.at[2]),
    ]
    small = (taps, offset, taps_bc, offset_bc, step_bias, decay_log)
    for k, (source, target) in enumerate(zip((s0, s1, s2, s3, s4, s5), small)):
        first.append(pltpu.make_async_copy(source, target, sems.at[14 + k]))
    weights = []
    for k in range(4):
        source = in_hbm if k < 2 else gate_hbm
        at = slice(k % 2 * side, (k % 2 + 1) * side)
        weights.append(pltpu.make_async_copy(source.at[:, at], w_wide.at[k], sems.at[20 + k]))
    for copy in first:
        copy.start()
    tok[:above, :] = edge[...]
    for copy in first:
        copy.wait()
    weights[0].start()

    def conv(source, at, tap, off):
        total = off
        for k in range(KERNEL):
            begin = above - (KERNEL - 1) + k
            total = total + tap[k : k + 1, at] * source[begin : begin + rows, at]
        return silu(total).astype(BF16)

    padded_bc[...] = dot(tok[...], w_bc[...]).astype(BF16).astype(F32)
    steps = lax.dot_general(
        tok[above:, :], w_step[...], (((1,), (1,)), ((), ())), preferred_element_type=F32
    )

    weights[0].wait()
    weights[1].start()
    maps = conv(padded_bc, slice(0, 2 * STATE), taps_bc, offset_bc[...])
    maps_ref[...] = maps
    read_ref[...] = maps[:, STATE:]
    v = steps + step_bias[...]
    dt = jnp.maximum(v, 0.0) + jnp.log1p(jnp.exp(-jnp.abs(v)))
    log_decay = -jnp.exp(decay_log[...]) * dt
    cum_ref[...] = jnp.zeros_like(cum_ref)
    dt_ref[...] = jnp.zeros_like(dt_ref)
    lead_ref[...] = jnp.zeros_like(lead_ref)
    dt_ref[:, :heads] = dt
    row = lax.broadcasted_iota(jnp.int32, (SPAN, SPAN), 0)
    col = lax.broadcasted_iota(jnp.int32, (SPAN, SPAN), 1)
    lower = (row >= col).astype(F32)
    lead = jnp.zeros((1, heads), F32)
    for s in range(spans):
        at = slice(s * SPAN, (s + 1) * SPAN)
        write_t[s] = jnp.transpose(maps[at, :STATE].astype(F32)).astype(BF16)
        cum = jnp.dot(
            lower, log_decay[at], preferred_element_type=F32, precision=lax.Precision.HIGHEST
        )
        cum_ref[at, :heads] = cum
        lead_ref[at, :heads] = jnp.exp(cum + lead)
        last = cum[SPAN - 1 :, :]
        lead = lead + last
        ends[at, :heads] = jnp.exp(last - cum) * dt[at]
        gone[s : s + 1, :heads] = jnp.exp(last)
    gone[spans : spans + 1, :heads] = jnp.exp(lead)
    padded[:, :side] = dot(tok[...], w_wide[0]).astype(BF16).astype(F32)

    def states(begin, end):
        at = slice(begin, end)
        count = (end - begin) // LANES
        to = begin // LANES
        x = conv(padded, at, taps, offset[:, at])
        x_ref[:, at] = x

        def wide(value):
            return jnp.concatenate(
                [
                    lane_pair(value[:, h : h + 1], value[:, h + 1 : h + 2])
                    for h in range(begin // HEADDIM, end // HEADDIM, 2)
                ],
                axis=1,
            )

        running = jnp.zeros((STATE, end - begin), F32)
        for s in range(spans):
            if s > 0:
                for t in range(count):
                    prior_ref[s - 1, to + t] = running[:, t * LANES : (t + 1) * LANES].astype(BF16)
            span = slice(s * SPAN, (s + 1) * SPAN)
            here = x[span].astype(F32) * wide(ends[span, :])
            running = wide(gone[s : s + 1, :]) * running + dot(write_t[s], here.astype(BF16))
        total = wide(gone[spans : spans + 1, :])
        for t in range(count):
            part = slice(t * LANES, (t + 1) * LANES)
            local_out[to + t] = running[:, part].astype(BF16)
            decay_out[to + t] = jnp.broadcast_to(total[:, part], (8, LANES))

    def side_states(k):
        for begin in range(k * side, (k + 1) * side, BLOCK):
            states(begin, min(begin + BLOCK, (k + 1) * side))

    def side_copies(k):
        at = slice(k * side, (k + 1) * side)
        tiles = slice(k * side // LANES, (k + 1) * side // LANES)
        return [
            pltpu.make_async_copy(x_ref.at[:, at], x_hbm.at[:, at], sems.at[24 + k]),
            pltpu.make_async_copy(prior_ref.at[:, tiles], prior_hbm.at[:, tiles], sems.at[26 + k]),
        ]

    def gate_copy(k):
        at = slice(k * side, (k + 1) * side)
        return pltpu.make_async_copy(gate_ref.at[:, at], gate_out.at[:, at], sems.at[12 + k])

    weights[1].wait()
    weights[2].start()
    stored = [
        pltpu.make_async_copy(source, target, sems.at[5 + k])
        for k, (source, target) in enumerate(
            (
                (maps_ref, maps_hbm), (read_ref, read_hbm), (cum_ref, cum_hbm), (dt_ref, dt_hbm),
                (lead_ref, lead_hbm),
            )
        )
    ]
    for copy in stored:
        copy.start()
    side_states(0)
    padded[:, side:] = dot(tok[...], w_wide[1]).astype(BF16).astype(F32)

    weights[2].wait()
    weights[3].start()
    for copy in side_copies(0):
        copy.start()
    side_states(1)
    gate_ref[:, :side] = dot(tok[above:, :], w_wide[2]).astype(BF16)

    weights[3].wait()
    late = side_copies(1) + [gate_copy(0)]
    for copy in late:
        copy.start()
    gate_ref[:, side:] = dot(tok[above:, :], w_wide[3]).astype(BF16)
    gate_copy(1).start()
    for copy in stored + side_copies(0) + late + [gate_copy(1)]:
        copy.wait()


def first_part(edge, tokens, w_bc, w_step, w_in, w_gate, *small):
    rows, width = tokens.shape
    above = edge.shape[0]
    channels = w_in.shape[1]
    spans = rows // SPAN
    tiles = channels // LANES
    vmem = pl.BlockSpec(memory_space=pltpu.VMEM)
    hbm = pl.BlockSpec(memory_space=pltpu.HBM)
    kept = [
        ((rows, channels), BF16),
        ((rows, 2 * STATE), BF16),
        ((rows, STATE), BF16),
        ((rows, LANES), F32),
        ((rows, LANES), F32),
        ((rows, LANES), F32),
        ((spans - 1, tiles, STATE, LANES), BF16),
        ((rows, channels), BF16),
    ]
    return pl.pallas_call(
        first_kernel,
        in_specs=[vmem] + [hbm] * (5 + len(small)),
        out_specs=[hbm] * len(kept) + [vmem] * 2,
        out_shape=[pltpu.HBM(*a) for a in kept]
        + [
            jax.ShapeDtypeStruct((tiles, STATE, LANES), BF16),
            jax.ShapeDtypeStruct((tiles, 8, LANES), F32),
        ],
        scratch_shapes=[
            pltpu.VMEM((above + rows, width), BF16),
            pltpu.VMEM(w_bc.shape, BF16),
            pltpu.VMEM(w_step.shape, BF16),
            pltpu.VMEM((4, width, channels // 2), BF16),
            pltpu.VMEM((above + rows, channels), F32),
            pltpu.VMEM((above + rows, 2 * STATE), F32),
            pltpu.VMEM((rows, LANES), F32),
            pltpu.VMEM((8, LANES), F32),
            pltpu.VMEM((spans, STATE, SPAN), BF16),
            *[pltpu.VMEM(*a) for a in kept],
            *[pltpu.VMEM(a.shape, F32) for a in small],
            pltpu.SemaphoreType.DMA((28,)),
        ],
        compiler_params=pltpu.CompilerParams(vmem_limit_bytes=FIRST_LIMIT),
        cost_estimate=pl.CostEstimate(
            flops=2 * rows * width * (2 * channels + BLOCK + LANES),
            bytes_accessed=2 * width * (rows + 2 * channels + BLOCK),
            transcendentals=0,
        ),
        name="first",
    )(edge, *in_hbm(tokens, w_bc, w_step, w_in, w_gate, *small))


def inside_kernel(first, x_ref, bc_ref, cum_ref, dt_ref, prior_ref, skip_ref, out_ref):
    tiles = x_ref.shape[1] // LANES
    row = lax.broadcasted_iota(jnp.int32, (SPAN, SPAN), 0)
    col = lax.broadcasted_iota(jnp.int32, (SPAN, SPAN), 1)
    lane = lax.broadcasted_iota(jnp.int32, (SPAN, LANES), 1)
    write = bc_ref[:, :STATE]
    read = bc_ref[:, STATE:]
    scores = lax.dot_general(read, write, (((1,), (1,)), ((), ())), preferred_element_type=F32)
    scores = jnp.where(row >= col, scores, 0.0)
    cum = cum_ref[...]
    cum_t = jnp.transpose(cum)
    dt_t = jnp.transpose(dt_ref[...])
    grown = jnp.where(pl.program_id(0) + first > 0, jnp.exp(cum), 0.0)
    for t in range(tiles):
        at = slice(t * LANES, (t + 1) * LANES)
        x = x_ref[:, at]
        both = []
        for h in (2 * t, 2 * t + 1):
            gap = jnp.minimum(cum[:, h : h + 1] - cum_t[h : h + 1, :], 0.0)
            both.append((scores * jnp.exp(gap) * dt_t[h : h + 1, :]).astype(BF16))
        zero = jnp.zeros_like(x)
        stacked = jnp.concatenate(
            [jnp.where(lane < HEADDIM, x, zero), jnp.where(lane < HEADDIM, zero, x)], axis=0
        )
        total = dot(jnp.concatenate(both, axis=1), stacked)
        total = total + skip_ref[:, at] * x.astype(F32)
        scale = jnp.where(
            lane < HEADDIM, grown[:, 2 * t : 2 * t + 1], grown[:, 2 * t + 1 : 2 * t + 2]
        )
        out_ref[:, at] = total + scale * dot(read, prior_ref[0, t])


def inside(first, count, x, bc, cum, dt, prior, skip):
    channels = x.shape[1]
    tiles = channels // LANES
    at = lambda s: (s + first, 0)
    return pl.pallas_call(
        functools.partial(inside_kernel, first),
        grid=(count,),
        in_specs=[
            pl.BlockSpec((SPAN, channels), at),
            pl.BlockSpec((SPAN, 2 * STATE), at),
            pl.BlockSpec((SPAN, LANES), at),
            pl.BlockSpec((SPAN, LANES), at),
            pl.BlockSpec((1, tiles, STATE, LANES), lambda s: (jnp.maximum(s + first - 1, 0), 0, 0, 0)),
            pl.BlockSpec((1, channels), lambda s: (0, 0)),
        ],
        out_specs=pl.BlockSpec((SPAN, channels), lambda s: (s, 0)),
        out_shape=pltpu.HBM((count * SPAN, channels), F32),
        compiler_params=pltpu.CompilerParams(vmem_limit_bytes=INSIDE_LIMIT),
        cost_estimate=pl.CostEstimate(
            flops=1_000_000, bytes_accessed=1_000_000, transcendentals=0
        ),
        name="inside",
    )(*in_hbm(x, bc, cum, dt, prior), skip)


def split3(v):
    high = v.astype(BF16)
    rest = v - high.astype(F32)
    mid = rest.astype(BF16)
    return high, mid, (rest - mid.astype(F32)).astype(BF16)


def joined(message, rows):
    return (
        message[rows : rows + 1].astype(F32)
        + message[rows + 1 : rows + 2].astype(F32)
        + message[rows + 2 : rows + 3].astype(F32)
    )


def squares_rows(total):
    index = lax.broadcasted_iota(jnp.int32, (16, LANES), 0)
    high, mid, low = (p.astype(F32) for p in split3(total))
    out = jnp.where(index == 0, high, jnp.where(index == 1, mid, jnp.where(index == 2, low, 0.0)))
    return out.astype(BF16)


def ready_kernel(
    which, read_hbm, lead_hbm, low_hbm, high_hbm, gate_hbm, w_hbm,
    read_ref, lead_ref, local_ref, gate_ref, w_ref, sems,
):
    copies = rows_copies(
        which[0], (read_hbm, lead_hbm, gate_hbm), (read_ref, lead_ref, gate_ref), 0, sems
    )
    local = local_copies(which[0], low_hbm, high_hbm, local_ref, 0, sems.at[3])
    weights = pltpu.make_async_copy(w_hbm, w_ref, sems.at[4])
    weights.start()
    for copy in copies:
        copy.start()
    start_local(which[0], local)
    for copy in copies:
        copy.wait()
    local[0].wait()
    weights.wait()


def rows_copies(span, sources, targets, place, sems):
    at = pl.ds(pl.multiple_of(span * SPAN, SPAN), SPAN)
    return [
        pltpu.make_async_copy(
            source.at[at, :], target.at[pl.ds(place * SPAN, SPAN), :], sems.at[k]
        )
        for k, (source, target) in enumerate(zip(sources, targets))
    ]


def local_copies(span, low, high, target, place, sem):
    half = low.shape[0] // SPAN
    to = target.at[pl.ds(place * SPAN, SPAN), :]
    out = []
    for source, start in ((low, 0), (high, half)):
        row = pl.multiple_of(jnp.clip(span - start, 0, half - 1) * SPAN, SPAN)
        out.append(pltpu.make_async_copy(source.at[pl.ds(row, SPAN), :], to, sem))
    return out + [half]


def start_local(span, local):
    low, high, half = local
    pl.when(span < half)(low.start)
    pl.when(span >= half)(high.start)


def ready(which, read, lead, low, high, gate, weight):
    channels = gate.shape[1]
    vmem = pl.BlockSpec(memory_space=pltpu.VMEM)
    hbm = pl.BlockSpec(memory_space=pltpu.HBM)
    return pl.pallas_call(
        ready_kernel,
        in_specs=[pl.BlockSpec(memory_space=pltpu.SMEM)] + [hbm] * 6,
        out_specs=[vmem] * 5,
        out_shape=[
            jax.ShapeDtypeStruct((SPAN, STATE), BF16),
            jax.ShapeDtypeStruct((SPAN, LANES), F32),
            jax.ShapeDtypeStruct((SPAN, channels), F32),
            jax.ShapeDtypeStruct((SPAN, channels), BF16),
            jax.ShapeDtypeStruct(weight.shape, BF16),
        ],
        scratch_shapes=[pltpu.SemaphoreType.DMA((5,))],
        compiler_params=pltpu.CompilerParams(vmem_limit_bytes=SMALL_LIMIT),
        cost_estimate=pl.CostEstimate(flops=1000000, bytes_accessed=10**6, transcendentals=0),
        name="ready",
    )(which, *in_hbm(read, lead, low, high, gate, weight))


def tail_kernel(inner_total, has_rows, count, *refs):
    if has_rows:
        read_ref, lead_ref, local_ref, gate_ref, state_ref, norm_ref, w_ref, *outs, gated = refs
    else:
        (which, read_hbm, lead_hbm, low_hbm, high_hbm, gate_hbm, state_ref, norm_ref, w_hbm,
         *outs, read_ref, lead_ref, local_ref, gate_ref, gated, w_ref, sems, w_sems) = refs
        waits = []
        for i in range(count):
            copies = rows_copies(
                which[i], (read_hbm, lead_hbm, gate_hbm), (read_ref, lead_ref, gate_ref), i,
                sems.at[i],
            )
            local = local_copies(which[i], low_hbm, high_hbm, local_ref, i, sems.at[i, 3])
            for copy in copies:
                copy.start()
            start_local(which[i], local)
            waits.append(copies + local[:1])
        weights = []
        for side in range(2):
            at = slice(side * w_hbm.shape[1] // 2, (side + 1) * w_hbm.shape[1] // 2)
            weights.append(
                pltpu.make_async_copy(w_hbm.at[:, at], w_ref.at[:, at], w_sems.at[side])
            )
        weights[0].start()
    channels = local_ref.shape[1]
    tiles = channels // LANES
    width = w_ref.shape[1]
    side_tiles = width // 2 // LANES
    side_rows = side_tiles * SPAN
    sums = []
    for i in range(count):
        if not has_rows:
            for copy in waits[i]:
                copy.wait()
            if i == count - 1:
                weights[1].start()
        rows = slice(i * SPAN, (i + 1) * SPAN)
        read = read_ref[rows, :]
        lead = lead_ref[rows, :]
        squares = jnp.zeros((SPAN, LANES), F32)
        for t in range(tiles):
            at = slice(t * LANES, (t + 1) * LANES)
            scale = lane_pair(lead[:, 2 * t : 2 * t + 1], lead[:, 2 * t + 1 : 2 * t + 2])
            mixed = local_ref[rows, at] + scale * dot(read, state_ref[t])
            pre = mixed * silu(gate_ref[rows, at].astype(F32))
            squares = squares + pre * pre
            gated[rows, at] = (pre * norm_ref[:, at]).astype(BF16)
        total = jnp.sum(squares, axis=1, keepdims=True) * (1.0 / inner_total)
        sums.append(jnp.transpose(jnp.broadcast_to(total, (SPAN, LANES)))[:1])
    for j in range(width // BLOCK):
        if not has_rows and j * BLOCK % (width // 2) == 0:
            weights[j * BLOCK // (width // 2)].wait()
        part = dot(gated[...], w_ref[:, j * BLOCK : (j + 1) * BLOCK]).astype(outs[0].dtype)
        for u in range(BLOCK // LANES):
            side, tile = divmod(j * (BLOCK // LANES) + u, side_tiles)
            for i in range(count):
                outs[2 * i + side][tile * SPAN : (tile + 1) * SPAN, :] = part[
                    i * SPAN : (i + 1) * SPAN, u * LANES : (u + 1) * LANES
                ]
    for i in range(count):
        for side in range(2):
            out = outs[2 * i + side]
            if out.shape[0] == side_rows + 16:
                out[side_rows:, :] = squares_rows(sums[i])
    if len(outs) > 2 * count:
        outs[2 * count][...] = jnp.broadcast_to(sums[0], (8, LANES))


def tail(which, rows_in, state, norm, weight, squares_in):
    count = 1 if which is None else which.shape[0]
    channels, width = weight.shape
    side_rows = width // 2 // LANES * SPAN
    vmem = pl.BlockSpec(memory_space=pltpu.VMEM)
    hbm = pl.BlockSpec(memory_space=pltpu.HBM)
    shapes = []
    for i in range(count):
        for side in range(2):
            extra = 16 if (i, side) in squares_in else 0
            shapes.append(jax.ShapeDtypeStruct((side_rows + extra, LANES), BF16))
    if not squares_in:
        shapes.append(jax.ShapeDtypeStruct((8, LANES), F32))
    rows = count * SPAN
    gated = pltpu.VMEM((rows, channels), BF16)
    if which is None:
        in_specs, args, scratch = [vmem] * 4, list(rows_in), [gated]
    else:
        in_specs = [pl.BlockSpec(memory_space=pltpu.SMEM)] + [hbm] * 5
        args = [which, *in_hbm(*rows_in)]
        scratch = [
            pltpu.VMEM((rows, STATE), BF16),
            pltpu.VMEM((rows, LANES), F32),
            pltpu.VMEM((rows, channels), F32),
            pltpu.VMEM((rows, channels), BF16),
            gated,
            pltpu.VMEM(weight.shape, BF16),
            pltpu.SemaphoreType.DMA((count, 4)),
            pltpu.SemaphoreType.DMA((2,)),
        ]
    return pl.pallas_call(
        functools.partial(tail_kernel, HEADS * HEADDIM, which is None, count),
        in_specs=in_specs + [vmem] * 2 + [vmem if which is None else hbm],
        out_specs=[vmem] * len(shapes),
        out_shape=shapes,
        scratch_shapes=scratch,
        compiler_params=pltpu.CompilerParams(vmem_limit_bytes=TAIL_LIMIT),
        cost_estimate=pl.CostEstimate(flops=1000000, bytes_accessed=10**6, transcendentals=0),
    )(*args, state, norm, *([weight] if which is None else in_hbm(weight)))


def merge_kernel(a_ref, b_ref, b_squares, out_ref):
    rows = a_ref.shape[0] - 16
    out_ref[:rows, :] = (a_ref[:rows, :].astype(F32) + b_ref[:rows, :].astype(F32)).astype(BF16)
    total = joined(a_ref, rows)
    if b_squares:
        total = total + joined(b_ref, rows)
    out_ref[rows:, :] = squares_rows(total)


def merge(near, relayed, with_squares):
    vmem = pl.BlockSpec(memory_space=pltpu.VMEM)

    def body(a_ref, b_ref, out_ref):
        merge_kernel(a_ref, b_ref, with_squares, out_ref)

    return pl.pallas_call(
        body,
        in_specs=[vmem] * 2,
        out_specs=vmem,
        out_shape=jax.ShapeDtypeStruct(near.shape, BF16),
        compiler_params=pltpu.CompilerParams(vmem_limit_bytes=SMALL_LIMIT),
        cost_estimate=pl.CostEstimate(flops=1000000, bytes_accessed=10**6, transcendentals=0),
    )(near, relayed)


def final_kernel(own_l, own_r, own_sq, up, down, direct_l, direct_r, out_ref):
    rows = own_l.shape[0]
    tiles = rows // SPAN
    total = own_sq[0:1, :] + joined(up, rows) + joined(down, rows)
    scale = lax.rsqrt(total + 0.25)
    column = jnp.transpose(jnp.broadcast_to(scale, (LANES, SPAN)))
    for side, parts in enumerate(((own_l, up, direct_l), (own_r, direct_r, down))):
        for t in range(tiles):
            at = slice(t * SPAN, (t + 1) * SPAN)
            added = sum(p[at, :].astype(F32) for p in parts)
            to = slice((side * tiles + t) * LANES, (side * tiles + t + 1) * LANES)
            out_ref[:, to] = (added * column).astype(BF16)


def final(*parts):
    vmem = pl.BlockSpec(memory_space=pltpu.VMEM)
    tiles = parts[0].shape[0] // SPAN
    return pl.pallas_call(
        final_kernel,
        in_specs=[vmem] * len(parts),
        out_specs=vmem,
        out_shape=jax.ShapeDtypeStruct((SPAN, 2 * tiles * LANES), BF16),
        compiler_params=pltpu.CompilerParams(vmem_limit_bytes=SMALL_LIMIT),
        cost_estimate=pl.CostEstimate(flops=1000000, bytes_accessed=10**6, transcendentals=0),
        name="final",
    )(*parts)


def ring(value, axis, distance):
    size = lax.axis_size(axis)
    return lax.ppermute(value, axis, [(i, (i + distance) % size) for i in range(size)])


def pick(values, index):
    out = values[0]
    for k in range(1, len(values)):
        out = jnp.where(index == k, values[k], out)
    return out


def packed(state, decay):
    tiles = state.shape[0]
    high = decay.astype(BF16)
    low = (decay - high.astype(F32)).astype(BF16)
    spare = jnp.zeros((16 - 2 * tiles, LANES), BF16)
    return jnp.concatenate([state.astype(BF16).reshape(-1, LANES), high, low, spare], 0)


def unpacked(message, tiles):
    rows = message.shape[0] - 16
    state = message[:rows].reshape(tiles, rows // tiles, LANES).astype(F32)
    high = message[rows : rows + tiles].astype(F32)
    low = message[rows + tiles : rows + 2 * tiles].astype(F32)
    return state, (high + low)[:, None, :]


def incoming_state(local, decay):
    z_axis, y_axis, c_axis = SEQ
    z, y, c = (lax.axis_index(a) for a in SEQ)
    ys, zs = lax.axis_size(y_axis), lax.axis_size(z_axis)
    tiles = local.shape[0] // 2
    first = c == 0
    here = jnp.where(first, local[:tiles], local[tiles:])
    there = jnp.where(first, local[tiles:], local[:tiles])
    here_d = jnp.where(first, decay[:tiles], decay[tiles:])
    there_d = jnp.where(first, decay[tiles:], decay[:tiles])

    got = ring(packed(there, there_d), c_axis, 1)
    other, other_d = unpacked(got, tiles)
    here, here_d = here.astype(F32), here_d[:, None, :]
    s0, d0 = jnp.where(first, here, other), jnp.where(first, here_d, other_d)
    s1, d1 = jnp.where(first, other, here), jnp.where(first, other_d, here_d)
    chip, chip_d = d1 * s0 + s1, d0 * d1

    part = STATE // ys
    quarters = [chip[:, q * part : (q + 1) * part] for q in range(ys)]
    sent = [pick(quarters, (y + k) % ys) for k in range(ys)]
    messages = [packed(sent[k], chip_d[:, 0]) for k in range(1, ys)]
    got = [ring(message, y_axis, k + 1) for k, message in enumerate(messages)]
    got = [unpacked(message, tiles) for message in got]
    by_shift = [(sent[0], chip_d)] + got
    states = [pick([g[0] for g in by_shift], (y - q) % ys) for q in range(ys)]
    decays = [pick([g[1] for g in by_shift], (y - q) % ys) for q in range(ys)]
    plane, plane_d = states[0], decays[0]
    for q in range(1, ys):
        plane, plane_d = decays[q] * plane + states[q], decays[q] * plane_d

    message = packed(plane, plane_d[:, 0])
    got = [ring(message, z_axis, k) for k in range(1, zs)]
    got = [unpacked(message, tiles) for message in got]
    before = jnp.zeros_like(plane)
    for q in range(zs - 1):
        s = pick([g[0] for g in got], z - q - 1)
        d = pick([g[1] for g in got], z - q - 1)
        before = jnp.where(q < z, d * before + s, before)

    prefix = [before]
    for q in range(ys - 1):
        prefix.append(decays[q] * prefix[-1] + states[q])
    sent = [pick(prefix, (y + k) % ys).astype(BF16) for k in range(ys)]
    got = [sent[0]] + [ring(sent[k], y_axis, k) for k in range(1, ys)]
    chip_in = jnp.concatenate([pick(got, (y - q) % ys) for q in range(ys)], axis=1)
    second_in = (d0 * chip_in.astype(F32) + s0).astype(BF16)
    mine = jnp.where(first, chip_in, second_in)
    message = jnp.where(first, second_in, chip_in)
    got = ring(message, c_axis, 1)
    return jnp.concatenate([jnp.where(first, mine, got), jnp.where(first, got, mine)], axis=0)


def per_device(
    tokens,
    proj_inner,
    proj_gate,
    proj_bc,
    proj_step,
    conv_inner,
    conv_bc,
    offset_inner,
    offset_bc,
    step_bias,
    decay_log,
    skip_gain,
    norm_weight,
    out_weight,
):
    rows = tokens.shape[0]
    spans = rows // SPAN
    devices = lax.axis_size(SEQ)
    edge = lax.ppermute(tokens[rows - EDGE :], SEQ, [(i, i + 1) for i in range(devices - 1)])
    x, bc, read, cum, dt, lead, prior, gate, local, decay = first_part(
        edge, tokens, proj_bc, proj_step.T, proj_inner, proj_gate, conv_inner, offset_inner[None],
        conv_bc, offset_bc[None], step_bias[None], decay_log[None],
    )
    state = incoming_state(local, decay[:, 0])
    skip = jnp.repeat(skip_gain, HEADDIM)[None]
    inner = []
    for part in range(2):
        half = spans // 2
        inner.append(inside(part * half, half, x, bc, cum, dt, prior, skip))

    head = lax.axis_index("head")
    size = lax.axis_size("head")

    def order(*which):
        return jnp.stack([(head + k) & (size - 1) for k in which]).astype(jnp.int32)

    norm = norm_weight[None]
    sources = (read, lead, *inner, gate)
    *far_rows, far_weight = ready(order(2), *sources, out_weight)

    def moved(value, distance):
        return ring(value, "head", distance)

    far_left, far_right = tail(None, far_rows, state, norm, far_weight, {(0, 0), (0, 1)})
    relay_up = moved(far_left, 1)
    relay_down = moved(far_right, -1)
    next_left, next_right, last_left, last_right = tail(
        order(1, 3), sources, state, norm, out_weight, {(0, 0), (1, 1)}
    )
    direct_up = moved(next_right, 1)
    direct_down = moved(last_left, -1)
    own_left, own_right, own_squares = tail(order(0), sources, state, norm, out_weight, set())
    up = merge(next_left, relay_up, True)
    up = moved(up, 1)
    down = merge(last_right, relay_down, False)
    down = moved(down, -1)
    return final(own_left, own_right, own_squares, up, down, direct_down, direct_up)


def solution(mesh):
    torus = Mesh(
        mesh.devices.reshape(4, 4, 2, mesh.shape["head"]), ("seq_0", "seq_1", "seq_2", "head")
    )
    return jax.shard_map(
        per_device,
        mesh=torus,
        in_specs=(
            P(SEQ, None),
            P(None, "head"),
            P(None, "head"),
            P(),
            P(None, "head"),
            P(None, "head"),
            P(),
            P("head"),
            P(),
            P("head"),
            P("head"),
            P("head"),
            P("head"),
            P("head", None),
        ),
        out_specs=P(SEQ_HEAD, None),
        check_vma=False,
    )
```

```python
import functools

import jax
import jax.numpy as jnp
from jax import lax
from jax.experimental import pallas as pl
from jax.experimental.pallas import tpu as pltpu
from jax.sharding import Mesh
from jax.sharding import PartitionSpec as P


HEADS = 80
HEADDIM = 64
STATE = 128
SPAN = 128
LANES = 128
EDGE = 16
BLOCK = 256
SEQ = ("seq_0", "seq_1", "seq_2")
SEQ_HEAD = ("seq_0", "seq_1", "seq_2", "head")

MIB = 2**20
FIRST_LIMIT = 48 * MIB
INSIDE_LIMIT = 12 * MIB
TAIL_LIMIT = 16 * MIB
SMALL_LIMIT = 8 * MIB


F32 = jnp.float32
BF16 = jnp.bfloat16


def in_hbm(*arrays):
    return [pltpu.with_memory_space_constraint(a, pltpu.HBM) for a in arrays]


def dot(a, b):
    return jnp.dot(a, b, preferred_element_type=F32)


def silu(v):
    half = 0.5 * v
    return half + half * jnp.tanh(half)


def lane_pair(first, second):
    lane = lax.broadcasted_iota(jnp.int32, (first.shape[0], LANES), 1)
    return jnp.where(lane < HEADDIM, first, second)


def first_kernel(
    edge, tok_hbm, bc_hbm, step_hbm, in_hbm, gate_hbm, s0, s1, s2, s3, s4, s5,
    x_hbm, maps_hbm, read_hbm, cum_hbm, dt_hbm, lead_hbm, prior_hbm, gate_out, local_out, decay_out,
    tok, w_bc, w_step, w_in, w_gate, padded, padded_bc,
    x_ref, maps_ref, read_ref, cum_ref, dt_ref, lead_ref, prior_ref, gate_ref,
    taps, offset, taps_bc, offset_bc, step_bias, decay_log, sems,
):
    rows = x_ref.shape[0]
    above = edge.shape[0]
    channels = x_ref.shape[1]
    heads = step_bias.shape[1]
    spans = rows // SPAN
    per = BLOCK // HEADDIM
    tiles = BLOCK // LANES

    first = [
        pltpu.make_async_copy(tok_hbm, tok.at[pl.ds(above, rows), :], sems.at[0]),
        pltpu.make_async_copy(bc_hbm, w_bc, sems.at[1]),
        pltpu.make_async_copy(step_hbm, w_step, sems.at[2]),
    ]
    inner_copy = pltpu.make_async_copy(in_hbm, w_in, sems.at[3])
    gate_copy = pltpu.make_async_copy(gate_hbm, w_gate, sems.at[4])
    small = (taps, offset, taps_bc, offset_bc, step_bias, decay_log)
    for k, (source, target) in enumerate(zip((s0, s1, s2, s3, s4, s5), small)):
        first.append(pltpu.make_async_copy(source, target, sems.at[14 + k]))
    for copy in first:
        copy.start()
    tok[:above, :] = edge[...]
    for copy in first:
        copy.wait()
    inner_copy.start()

    def conv(source, at, tap, off):
        x = source[:, at]
        half = 0.5 * tap[:, at]
        one = pltpu.roll(x, 1, 0)
        older = half[0:1] * one + half[1:2] * x
        newer = half[2:3] * one + half[3:4] * x + 0.5 * off
        v = pltpu.roll(older, 2, 0)[above:] + newer[above:]
        return (v + v * jnp.tanh(v)).astype(BF16)

    padded_bc[...] = dot(tok[...], w_bc[...]).astype(BF16).astype(F32)
    steps = lax.dot_general(
        tok[above:, :], w_step[...], (((1,), (1,)), ((), ())), preferred_element_type=F32
    )
    inner_copy.wait()
    gate_copy.start()
    padded[...] = dot(tok[...], w_in[...]).astype(BF16).astype(F32)

    maps = conv(padded_bc, slice(0, 2 * STATE), taps_bc, offset_bc[...])
    maps_ref[...] = maps
    read_ref[...] = maps[:, STATE:]
    v = steps + step_bias[...]
    dt = jnp.maximum(v, 0.0) + jnp.log1p(jnp.exp(-jnp.abs(v)))
    log_decay = -jnp.exp(decay_log[...]) * dt
    cum_ref[...] = jnp.zeros_like(cum_ref)
    dt_ref[...] = jnp.zeros_like(dt_ref)
    lead_ref[...] = jnp.zeros_like(lead_ref)
    dt_ref[:, :heads] = dt
    row = lax.broadcasted_iota(jnp.int32, (SPAN, SPAN), 0)
    col = lax.broadcasted_iota(jnp.int32, (SPAN, SPAN), 1)
    lower = (row >= col).astype(F32)
    lead = jnp.zeros((1, heads), F32)
    ends, gone, write_t = [], [], []
    for s in range(spans):
        at = slice(s * SPAN, (s + 1) * SPAN)
        write_t.append(jnp.transpose(maps[at, :STATE].astype(F32)).astype(BF16))
        cum = jnp.dot(
            lower, log_decay[at], preferred_element_type=F32, precision=lax.Precision.HIGHEST
        )
        cum_ref[at, :heads] = cum
        lead_ref[at, :heads] = jnp.exp(cum + lead)
        last = cum[SPAN - 1 :, :]
        lead = lead + last
        ends.append(jnp.exp(last - cum) * dt[at])
        gone.append(jnp.exp(last))
    gone.append(jnp.exp(lead))

    gate_copy.wait()
    early = [
        pltpu.make_async_copy(source, target, sems.at[5 + k])
        for k, (source, target) in enumerate(
            (
                (maps_ref, maps_hbm), (read_ref, read_hbm), (cum_ref, cum_hbm), (dt_ref, dt_hbm),
                (lead_ref, lead_hbm),
            )
        )
    ]
    for copy in early:
        copy.start()
    half = rows // 2
    gate_ref[:half, :] = dot(tok[above : above + half, :], w_gate[...]).astype(BF16)
    for g in range(channels // BLOCK):
        at = slice(g * BLOCK, (g + 1) * BLOCK)
        x = conv(padded, at, taps, offset[:, at])
        x_ref[:, at] = x
        running = jnp.zeros((STATE, BLOCK), F32)
        for s in range(spans):
            if s > 0:
                for t in range(tiles):
                    prior_ref[s - 1, g * tiles + t] = running[
                        :, t * LANES : (t + 1) * LANES
                    ].astype(BF16)

            def wide(value):
                return jnp.concatenate(
                    [
                        lane_pair(value[:, h : h + 1], value[:, h + 1 : h + 2])
                        for h in range(g * per, (g + 1) * per, 2)
                    ],
                    axis=1,
                )

            here = x[s * SPAN : (s + 1) * SPAN].astype(F32)
            local = dot(write_t[s], (here * wide(ends[s])).astype(BF16))
            running = wide(gone[s]) * running + local
        for t in range(tiles):
            to = g * tiles + t
            local_out[to] = running[:, t * LANES : (t + 1) * LANES].astype(BF16)
            h = g * per + 2 * t
            decay_out[to] = jnp.broadcast_to(
                lane_pair(gone[spans][:, h : h + 1], gone[spans][:, h + 1 : h + 2]), (8, LANES)
            )
    late = [
        pltpu.make_async_copy(x_ref, x_hbm, sems.at[10]),
        pltpu.make_async_copy(prior_ref, prior_hbm, sems.at[11]),
    ]
    for k in range(2):
        at = slice(k * half, (k + 1) * half)
        late.append(
            pltpu.make_async_copy(gate_ref.at[at, :], gate_out.at[at, :], sems.at[12 + k])
        )
    for copy in late[:3]:
        copy.start()
    gate_ref[half:, :] = dot(tok[above + half :, :], w_gate[...]).astype(BF16)
    late[3].start()
    for copy in early + late:
        copy.wait()


def first_part(edge, tokens, w_bc, w_step, w_in, w_gate, *small):
    rows, width = tokens.shape
    above = edge.shape[0]
    channels = w_in.shape[1]
    spans = rows // SPAN
    tiles = channels // LANES
    vmem = pl.BlockSpec(memory_space=pltpu.VMEM)
    hbm = pl.BlockSpec(memory_space=pltpu.HBM)
    kept = [
        ((rows, channels), BF16),
        ((rows, 2 * STATE), BF16),
        ((rows, STATE), BF16),
        ((rows, LANES), F32),
        ((rows, LANES), F32),
        ((rows, LANES), F32),
        ((spans - 1, tiles, STATE, LANES), BF16),
        ((rows, channels), BF16),
    ]
    return pl.pallas_call(
        first_kernel,
        in_specs=[vmem] + [hbm] * (5 + len(small)),
        out_specs=[hbm] * len(kept) + [vmem] * 2,
        out_shape=[pltpu.HBM(*a) for a in kept]
        + [
            jax.ShapeDtypeStruct((tiles, STATE, LANES), BF16),
            jax.ShapeDtypeStruct((tiles, 8, LANES), F32),
        ],
        scratch_shapes=[
            pltpu.VMEM((above + rows, width), BF16),
            pltpu.VMEM(w_bc.shape, BF16),
            pltpu.VMEM(w_step.shape, BF16),
            pltpu.VMEM(w_in.shape, BF16),
            pltpu.VMEM(w_gate.shape, BF16),
            pltpu.VMEM((above + rows, channels), F32),
            pltpu.VMEM((above + rows, 2 * STATE), F32),
            *[pltpu.VMEM(*a) for a in kept],
            *[pltpu.VMEM(a.shape, F32) for a in small],
            pltpu.SemaphoreType.DMA((20,)),
        ],
        compiler_params=pltpu.CompilerParams(vmem_limit_bytes=FIRST_LIMIT),
        cost_estimate=pl.CostEstimate(
            flops=2 * rows * width * (2 * channels + BLOCK + LANES),
            bytes_accessed=2 * width * (rows + 2 * channels + BLOCK),
            transcendentals=0,
        ),
        name="first",
    )(edge, *in_hbm(tokens, w_bc, w_step, w_in, w_gate, *small))


def inside_kernel(first, x_ref, bc_ref, cum_ref, dt_ref, prior_ref, skip_ref, out_ref):
    tiles = x_ref.shape[1] // LANES
    row = lax.broadcasted_iota(jnp.int32, (SPAN, SPAN), 0)
    col = lax.broadcasted_iota(jnp.int32, (SPAN, SPAN), 1)
    lane = lax.broadcasted_iota(jnp.int32, (SPAN, LANES), 1)
    write = bc_ref[:, :STATE]
    read = bc_ref[:, STATE:]
    scores = lax.dot_general(read, write, (((1,), (1,)), ((), ())), preferred_element_type=F32)
    scores = jnp.where(row >= col, scores, 0.0)
    cum = cum_ref[...]
    cum_t = jnp.transpose(cum)
    dt_t = jnp.transpose(dt_ref[...])
    grown = jnp.where(pl.program_id(0) + first > 0, jnp.exp(cum), 0.0)
    for t in range(tiles):
        at = slice(t * LANES, (t + 1) * LANES)
        x = x_ref[:, at]
        both = []
        for h in (2 * t, 2 * t + 1):
            gap = jnp.minimum(cum[:, h : h + 1] - cum_t[h : h + 1, :], 0.0)
            both.append((scores * jnp.exp(gap) * dt_t[h : h + 1, :]).astype(BF16))
        zero = jnp.zeros_like(x)
        stacked = jnp.concatenate(
            [jnp.where(lane < HEADDIM, x, zero), jnp.where(lane < HEADDIM, zero, x)], axis=0
        )
        total = dot(jnp.concatenate(both, axis=1), stacked)
        total = total + skip_ref[:, at] * x.astype(F32)
        scale = jnp.where(
            lane < HEADDIM, grown[:, 2 * t : 2 * t + 1], grown[:, 2 * t + 1 : 2 * t + 2]
        )
        out_ref[:, at] = total + scale * dot(read, prior_ref[0, t])


def inside(first, count, x, bc, cum, dt, prior, skip):
    channels = x.shape[1]
    tiles = channels // LANES
    at = lambda s: (s + first, 0)
    return pl.pallas_call(
        functools.partial(inside_kernel, first),
        grid=(count,),
        in_specs=[
            pl.BlockSpec((SPAN, channels), at),
            pl.BlockSpec((SPAN, 2 * STATE), at),
            pl.BlockSpec((SPAN, LANES), at),
            pl.BlockSpec((SPAN, LANES), at),
            pl.BlockSpec((1, tiles, STATE, LANES), lambda s: (jnp.maximum(s + first - 1, 0), 0, 0, 0)),
            pl.BlockSpec((1, channels), lambda s: (0, 0)),
        ],
        out_specs=pl.BlockSpec((SPAN, channels), lambda s: (s, 0)),
        out_shape=pltpu.HBM((count * SPAN, channels), F32),
        compiler_params=pltpu.CompilerParams(vmem_limit_bytes=INSIDE_LIMIT),
        cost_estimate=pl.CostEstimate(
            flops=1_000_000, bytes_accessed=1_000_000, transcendentals=0
        ),
        name="inside",
    )(*in_hbm(x, bc, cum, dt, prior), skip)


def split3(v):
    high = v.astype(BF16)
    rest = v - high.astype(F32)
    mid = rest.astype(BF16)
    return high, mid, (rest - mid.astype(F32)).astype(BF16)


def joined(message, rows):
    return (
        message[rows : rows + 1].astype(F32)
        + message[rows + 1 : rows + 2].astype(F32)
        + message[rows + 2 : rows + 3].astype(F32)
    )


def squares_rows(total):
    index = lax.broadcasted_iota(jnp.int32, (16, LANES), 0)
    high, mid, low = (p.astype(F32) for p in split3(total))
    out = jnp.where(index == 0, high, jnp.where(index == 1, mid, jnp.where(index == 2, low, 0.0)))
    return out.astype(BF16)


def ready_kernel(
    which, read_hbm, lead_hbm, low_hbm, high_hbm, gate_hbm, w_hbm,
    read_ref, lead_ref, local_ref, gate_ref, w_ref, sems,
):
    copies = rows_copies(
        which[0], (read_hbm, lead_hbm, gate_hbm), (read_ref, lead_ref, gate_ref), 0, sems
    )
    local = local_copies(which[0], low_hbm, high_hbm, local_ref, 0, sems.at[3])
    weights = pltpu.make_async_copy(w_hbm, w_ref, sems.at[4])
    weights.start()
    for copy in copies:
        copy.start()
    start_local(which[0], local)
    for copy in copies:
        copy.wait()
    local[0].wait()
    weights.wait()


def rows_copies(span, sources, targets, place, sems):
    at = pl.ds(pl.multiple_of(span * SPAN, SPAN), SPAN)
    return [
        pltpu.make_async_copy(
            source.at[at, :], target.at[pl.ds(place * SPAN, SPAN), :], sems.at[k]
        )
        for k, (source, target) in enumerate(zip(sources, targets))
    ]


def local_copies(span, low, high, target, place, sem):
    half = low.shape[0] // SPAN
    to = target.at[pl.ds(place * SPAN, SPAN), :]
    out = []
    for source, start in ((low, 0), (high, half)):
        row = pl.multiple_of(jnp.clip(span - start, 0, half - 1) * SPAN, SPAN)
        out.append(pltpu.make_async_copy(source.at[pl.ds(row, SPAN), :], to, sem))
    return out + [half]


def start_local(span, local):
    low, high, half = local
    pl.when(span < half)(low.start)
    pl.when(span >= half)(high.start)


def ready(which, read, lead, low, high, gate, weight):
    channels = gate.shape[1]
    vmem = pl.BlockSpec(memory_space=pltpu.VMEM)
    hbm = pl.BlockSpec(memory_space=pltpu.HBM)
    return pl.pallas_call(
        ready_kernel,
        in_specs=[pl.BlockSpec(memory_space=pltpu.SMEM)] + [hbm] * 6,
        out_specs=[vmem] * 5,
        out_shape=[
            jax.ShapeDtypeStruct((SPAN, STATE), BF16),
            jax.ShapeDtypeStruct((SPAN, LANES), F32),
            jax.ShapeDtypeStruct((SPAN, channels), F32),
            jax.ShapeDtypeStruct((SPAN, channels), BF16),
            jax.ShapeDtypeStruct(weight.shape, BF16),
        ],
        scratch_shapes=[pltpu.SemaphoreType.DMA((5,))],
        compiler_params=pltpu.CompilerParams(vmem_limit_bytes=SMALL_LIMIT),
        cost_estimate=pl.CostEstimate(flops=1000000, bytes_accessed=10**6, transcendentals=0),
        name="ready",
    )(which, *in_hbm(read, lead, low, high, gate, weight))


def tail_kernel(inner_total, has_rows, count, *refs):
    if has_rows:
        read_ref, lead_ref, local_ref, gate_ref, state_ref, norm_ref, w_ref, *outs, gated = refs
    else:
        (which, read_hbm, lead_hbm, low_hbm, high_hbm, gate_hbm, state_ref, norm_ref, w_hbm,
         *outs, read_ref, lead_ref, local_ref, gate_ref, gated, w_ref, sems, w_sems) = refs
        waits = []
        for i in range(count):
            copies = rows_copies(
                which[i], (read_hbm, lead_hbm, gate_hbm), (read_ref, lead_ref, gate_ref), i,
                sems.at[i],
            )
            local = local_copies(which[i], low_hbm, high_hbm, local_ref, i, sems.at[i, 3])
            for copy in copies:
                copy.start()
            start_local(which[i], local)
            waits.append(copies + local[:1])
        weights = []
        for side in range(2):
            at = slice(side * w_hbm.shape[1] // 2, (side + 1) * w_hbm.shape[1] // 2)
            weights.append(
                pltpu.make_async_copy(w_hbm.at[:, at], w_ref.at[:, at], w_sems.at[side])
            )
        weights[0].start()
    channels = local_ref.shape[1]
    tiles = channels // LANES
    width = w_ref.shape[1]
    side_tiles = width // 2 // LANES
    side_rows = side_tiles * SPAN
    sums = []
    for i in range(count):
        if not has_rows:
            for copy in waits[i]:
                copy.wait()
            if i == count - 1:
                weights[1].start()
        rows = slice(i * SPAN, (i + 1) * SPAN)
        read = read_ref[rows, :]
        lead = lead_ref[rows, :]
        squares = jnp.zeros((SPAN, LANES), F32)
        for t in range(tiles):
            at = slice(t * LANES, (t + 1) * LANES)
            scale = lane_pair(lead[:, 2 * t : 2 * t + 1], lead[:, 2 * t + 1 : 2 * t + 2])
            mixed = local_ref[rows, at] + scale * dot(read, state_ref[t])
            pre = mixed * silu(gate_ref[rows, at].astype(F32))
            squares = squares + pre * pre
            gated[rows, at] = (pre * norm_ref[:, at]).astype(BF16)
        total = jnp.sum(squares, axis=1, keepdims=True) * (1.0 / inner_total)
        sums.append(jnp.transpose(jnp.broadcast_to(total, (SPAN, LANES)))[:1])
    for j in range(width // BLOCK):
        if not has_rows and j * BLOCK % (width // 2) == 0:
            weights[j * BLOCK // (width // 2)].wait()
        part = dot(gated[...], w_ref[:, j * BLOCK : (j + 1) * BLOCK]).astype(outs[0].dtype)
        for u in range(BLOCK // LANES):
            side, tile = divmod(j * (BLOCK // LANES) + u, side_tiles)
            for i in range(count):
                outs[2 * i + side][tile * SPAN : (tile + 1) * SPAN, :] = part[
                    i * SPAN : (i + 1) * SPAN, u * LANES : (u + 1) * LANES
                ]
    for i in range(count):
        for side in range(2):
            out = outs[2 * i + side]
            if out.shape[0] == side_rows + 16:
                out[side_rows:, :] = squares_rows(sums[i])
    if len(outs) > 2 * count:
        outs[2 * count][...] = jnp.broadcast_to(sums[0], (8, LANES))


def tail(which, rows_in, state, norm, weight, squares_in):
    count = 1 if which is None else which.shape[0]
    channels, width = weight.shape
    side_rows = width // 2 // LANES * SPAN
    vmem = pl.BlockSpec(memory_space=pltpu.VMEM)
    hbm = pl.BlockSpec(memory_space=pltpu.HBM)
    shapes = []
    for i in range(count):
        for side in range(2):
            extra = 16 if (i, side) in squares_in else 0
            shapes.append(jax.ShapeDtypeStruct((side_rows + extra, LANES), BF16))
    if not squares_in:
        shapes.append(jax.ShapeDtypeStruct((8, LANES), F32))
    rows = count * SPAN
    gated = pltpu.VMEM((rows, channels), BF16)
    if which is None:
        in_specs, args, scratch = [vmem] * 4, list(rows_in), [gated]
    else:
        in_specs = [pl.BlockSpec(memory_space=pltpu.SMEM)] + [hbm] * 5
        args = [which, *in_hbm(*rows_in)]
        scratch = [
            pltpu.VMEM((rows, STATE), BF16),
            pltpu.VMEM((rows, LANES), F32),
            pltpu.VMEM((rows, channels), F32),
            pltpu.VMEM((rows, channels), BF16),
            gated,
            pltpu.VMEM(weight.shape, BF16),
            pltpu.SemaphoreType.DMA((count, 4)),
            pltpu.SemaphoreType.DMA((2,)),
        ]
    return pl.pallas_call(
        functools.partial(tail_kernel, HEADS * HEADDIM, which is None, count),
        in_specs=in_specs + [vmem] * 2 + [vmem if which is None else hbm],
        out_specs=[vmem] * len(shapes),
        out_shape=shapes,
        scratch_shapes=scratch,
        compiler_params=pltpu.CompilerParams(vmem_limit_bytes=TAIL_LIMIT),
        cost_estimate=pl.CostEstimate(flops=1000000, bytes_accessed=10**6, transcendentals=0),
    )(*args, state, norm, *([weight] if which is None else in_hbm(weight)))


def merge_kernel(a_ref, b_ref, b_squares, out_ref):
    rows = a_ref.shape[0] - 16
    out_ref[:rows, :] = (a_ref[:rows, :].astype(F32) + b_ref[:rows, :].astype(F32)).astype(BF16)
    total = joined(a_ref, rows)
    if b_squares:
        total = total + joined(b_ref, rows)
    out_ref[rows:, :] = squares_rows(total)


def merge(near, relayed, with_squares):
    vmem = pl.BlockSpec(memory_space=pltpu.VMEM)

    def body(a_ref, b_ref, out_ref):
        merge_kernel(a_ref, b_ref, with_squares, out_ref)

    return pl.pallas_call(
        body,
        in_specs=[vmem] * 2,
        out_specs=vmem,
        out_shape=jax.ShapeDtypeStruct(near.shape, BF16),
        compiler_params=pltpu.CompilerParams(vmem_limit_bytes=SMALL_LIMIT),
        cost_estimate=pl.CostEstimate(flops=1000000, bytes_accessed=10**6, transcendentals=0),
    )(near, relayed)


def final_kernel(own_l, own_r, own_sq, up, down, direct_l, direct_r, out_ref):
    rows = own_l.shape[0]
    tiles = rows // SPAN
    total = own_sq[0:1, :] + joined(up, rows) + joined(down, rows)
    scale = lax.rsqrt(total + 0.25)
    column = jnp.transpose(jnp.broadcast_to(scale, (LANES, SPAN)))
    for side, parts in enumerate(((own_l, up, direct_l), (own_r, direct_r, down))):
        for t in range(tiles):
            at = slice(t * SPAN, (t + 1) * SPAN)
            added = sum(p[at, :].astype(F32) for p in parts)
            to = slice((side * tiles + t) * LANES, (side * tiles + t + 1) * LANES)
            out_ref[:, to] = (added * column).astype(BF16)


def final(*parts):
    vmem = pl.BlockSpec(memory_space=pltpu.VMEM)
    tiles = parts[0].shape[0] // SPAN
    return pl.pallas_call(
        final_kernel,
        in_specs=[vmem] * len(parts),
        out_specs=vmem,
        out_shape=jax.ShapeDtypeStruct((SPAN, 2 * tiles * LANES), BF16),
        compiler_params=pltpu.CompilerParams(vmem_limit_bytes=SMALL_LIMIT),
        cost_estimate=pl.CostEstimate(flops=1000000, bytes_accessed=10**6, transcendentals=0),
        name="final",
    )(*parts)


def ring(value, axis, distance):
    size = lax.axis_size(axis)
    return lax.ppermute(value, axis, [(i, (i + distance) % size) for i in range(size)])


def pick(values, index):
    out = values[0]
    for k in range(1, len(values)):
        out = jnp.where(index == k, values[k], out)
    return out


def packed(state, decay):
    tiles = state.shape[0]
    high = decay.astype(BF16)
    low = (decay - high.astype(F32)).astype(BF16)
    spare = jnp.zeros((16 - 2 * tiles, LANES), BF16)
    return jnp.concatenate([state.astype(BF16).reshape(-1, LANES), high, low, spare], 0)


def unpacked(message, tiles):
    rows = message.shape[0] - 16
    state = message[:rows].reshape(tiles, rows // tiles, LANES).astype(F32)
    high = message[rows : rows + tiles].astype(F32)
    low = message[rows + tiles : rows + 2 * tiles].astype(F32)
    return state, (high + low)[:, None, :]


def incoming_state(local, decay):
    z_axis, y_axis, c_axis = SEQ
    z, y, c = (lax.axis_index(a) for a in SEQ)
    ys, zs = lax.axis_size(y_axis), lax.axis_size(z_axis)
    tiles = local.shape[0] // 2
    first = c == 0
    here = jnp.where(first, local[:tiles], local[tiles:])
    there = jnp.where(first, local[tiles:], local[:tiles])
    here_d = jnp.where(first, decay[:tiles], decay[tiles:])
    there_d = jnp.where(first, decay[tiles:], decay[:tiles])

    got = ring(packed(there, there_d), c_axis, 1)
    other, other_d = unpacked(got, tiles)
    here, here_d = here.astype(F32), here_d[:, None, :]
    s0, d0 = jnp.where(first, here, other), jnp.where(first, here_d, other_d)
    s1, d1 = jnp.where(first, other, here), jnp.where(first, other_d, here_d)
    chip, chip_d = d1 * s0 + s1, d0 * d1

    part = STATE // ys
    quarters = [chip[:, q * part : (q + 1) * part] for q in range(ys)]
    sent = [pick(quarters, (y + k) % ys) for k in range(ys)]
    messages = [packed(sent[k], chip_d[:, 0]) for k in range(1, ys)]
    got = [ring(message, y_axis, k + 1) for k, message in enumerate(messages)]
    got = [unpacked(message, tiles) for message in got]
    by_shift = [(sent[0], chip_d)] + got
    states = [pick([g[0] for g in by_shift], (y - q) % ys) for q in range(ys)]
    decays = [pick([g[1] for g in by_shift], (y - q) % ys) for q in range(ys)]
    plane, plane_d = states[0], decays[0]
    for q in range(1, ys):
        plane, plane_d = decays[q] * plane + states[q], decays[q] * plane_d

    message = packed(plane, plane_d[:, 0])
    got = [ring(message, z_axis, k) for k in range(1, zs)]
    got = [unpacked(message, tiles) for message in got]
    before = jnp.zeros_like(plane)
    for q in range(zs - 1):
        s = pick([g[0] for g in got], z - q - 1)
        d = pick([g[1] for g in got], z - q - 1)
        before = jnp.where(q < z, d * before + s, before)

    prefix = [before]
    for q in range(ys - 1):
        prefix.append(decays[q] * prefix[-1] + states[q])
    sent = [pick(prefix, (y + k) % ys).astype(BF16) for k in range(ys)]
    got = [sent[0]] + [ring(sent[k], y_axis, k) for k in range(1, ys)]
    chip_in = jnp.concatenate([pick(got, (y - q) % ys) for q in range(ys)], axis=1)
    second_in = (d0 * chip_in.astype(F32) + s0).astype(BF16)
    mine = jnp.where(first, chip_in, second_in)
    message = jnp.where(first, second_in, chip_in)
    got = ring(message, c_axis, 1)
    return jnp.concatenate([jnp.where(first, mine, got), jnp.where(first, got, mine)], axis=0)


def per_device(
    tokens,
    proj_inner,
    proj_gate,
    proj_bc,
    proj_step,
    conv_inner,
    conv_bc,
    offset_inner,
    offset_bc,
    step_bias,
    decay_log,
    skip_gain,
    norm_weight,
    out_weight,
):
    rows = tokens.shape[0]
    spans = rows // SPAN
    devices = lax.axis_size(SEQ)
    edge = lax.ppermute(tokens[rows - EDGE :], SEQ, [(i, i + 1) for i in range(devices - 1)])
    x, bc, read, cum, dt, lead, prior, gate, local, decay = first_part(
        edge, tokens, proj_bc, proj_step.T, proj_inner, proj_gate, conv_inner, offset_inner[None],
        conv_bc, offset_bc[None], step_bias[None], decay_log[None],
    )
    state = incoming_state(local, decay[:, 0])
    skip = jnp.repeat(skip_gain, HEADDIM)[None]
    inner = []
    for part in range(2):
        half = spans // 2
        inner.append(inside(part * half, half, x, bc, cum, dt, prior, skip))

    head = lax.axis_index("head")
    size = lax.axis_size("head")

    def order(*which):
        return jnp.stack([(head + k) & (size - 1) for k in which]).astype(jnp.int32)

    norm = norm_weight[None]
    sources = (read, lead, *inner, gate)
    *far_rows, far_weight = ready(order(2), *sources, out_weight)

    def moved(value, distance):
        return ring(value, "head", distance)

    far_left, far_right = tail(None, far_rows, state, norm, far_weight, {(0, 0), (0, 1)})
    relay_up = moved(far_left, 1)
    relay_down = moved(far_right, -1)
    next_left, next_right, last_left, last_right = tail(
        order(1, 3), sources, state, norm, out_weight, {(0, 0), (1, 1)}
    )
    direct_up = moved(next_right, 1)
    direct_down = moved(last_left, -1)
    own_left, own_right, own_squares = tail(order(0), sources, state, norm, out_weight, set())
    up = merge(next_left, relay_up, True)
    up = moved(up, 1)
    down = merge(last_right, relay_down, False)
    down = moved(down, -1)
    return final(own_left, own_right, own_squares, up, down, direct_down, direct_up)


def solution(mesh):
    torus = Mesh(
        mesh.devices.reshape(4, 4, 2, mesh.shape["head"]), ("seq_0", "seq_1", "seq_2", "head")
    )
    return jax.shard_map(
        per_device,
        mesh=torus,
        in_specs=(
            P(SEQ, None),
            P(None, "head"),
            P(None, "head"),
            P(),
            P(None, "head"),
            P(None, "head"),
            P(),
            P("head"),
            P(),
            P("head"),
            P("head"),
            P("head"),
            P("head"),
            P("head", None),
        ),
        out_specs=P(SEQ_HEAD, None),
        check_vma=False,
    )
```

```python
import functools

import jax
import jax.numpy as jnp
from jax import lax
from jax.experimental import pallas as pl
from jax.experimental.pallas import tpu as pltpu
from jax.sharding import Mesh
from jax.sharding import PartitionSpec as P


HEADS = 80
HEADDIM = 64
STATE = 128
SPAN = 128
LANES = 128
EDGE = 16
BLOCK = 256
SEQ = ("seq_0", "seq_1", "seq_2")
SEQ_HEAD = ("seq_0", "seq_1", "seq_2", "head")

MIB = 2**20
FIRST_LIMIT = 48 * MIB
INSIDE_LIMIT = 12 * MIB
TAIL_LIMIT = 16 * MIB
SMALL_LIMIT = 8 * MIB


F32 = jnp.float32
BF16 = jnp.bfloat16


def in_hbm(*arrays):
    return [pltpu.with_memory_space_constraint(a, pltpu.HBM) for a in arrays]


def dot(a, b):
    return jnp.dot(a, b, preferred_element_type=F32)


def silu(v):
    half = 0.5 * v
    return half + half * jnp.tanh(half)


def lane_pair(first, second):
    lane = lax.broadcasted_iota(jnp.int32, (first.shape[0], LANES), 1)
    return jnp.where(lane < HEADDIM, first, second)


def first_kernel(
    edge, tok_hbm, bc_hbm, step_hbm, in_hbm, gate_hbm, s0, s1, s2, s3, s4, s5,
    x_hbm, maps_hbm, read_hbm, cum_hbm, dt_hbm, lead_hbm, prior_hbm, gate_out, local_out, decay_out,
    tok, w_bc, w_step, w_in, w_gate, padded, padded_bc,
    x_ref, maps_ref, read_ref, cum_ref, dt_ref, lead_ref, prior_ref, gate_ref,
    taps, offset, taps_bc, offset_bc, step_bias, decay_log, sems,
):
    rows = x_ref.shape[0]
    above = edge.shape[0]
    channels = x_ref.shape[1]
    heads = step_bias.shape[1]
    spans = rows // SPAN
    per = BLOCK // HEADDIM
    tiles = BLOCK // LANES

    first = [
        pltpu.make_async_copy(tok_hbm, tok.at[pl.ds(above, rows), :], sems.at[0]),
        pltpu.make_async_copy(bc_hbm, w_bc, sems.at[1]),
        pltpu.make_async_copy(step_hbm, w_step, sems.at[2]),
    ]
    inner_copy = pltpu.make_async_copy(in_hbm, w_in, sems.at[3])
    gate_copy = pltpu.make_async_copy(gate_hbm, w_gate, sems.at[4])
    small = (taps, offset, taps_bc, offset_bc, step_bias, decay_log)
    for k, (source, target) in enumerate(zip((s0, s1, s2, s3, s4, s5), small)):
        first.append(pltpu.make_async_copy(source, target, sems.at[14 + k]))
    for copy in first:
        copy.start()
    tok[:above, :] = edge[...]
    for copy in first:
        copy.wait()
    inner_copy.start()

    def conv(source, at, tap, off):
        x = source[:, at]
        half = 0.5 * tap[:, at]
        one = pltpu.roll(x, 1, 0)
        older = half[0:1] * one + half[1:2] * x
        newer = half[2:3] * one + half[3:4] * x + 0.5 * off
        v = pltpu.roll(older, 2, 0)[above:] + newer[above:]
        return (v + v * jnp.tanh(v)).astype(BF16)

    padded_bc[...] = dot(tok[...], w_bc[...]).astype(BF16).astype(F32)
    steps = lax.dot_general(
        tok[above:, :], w_step[...], (((1,), (1,)), ((), ())), preferred_element_type=F32
    )
    inner_copy.wait()
    gate_copy.start()
    padded[...] = dot(tok[...], w_in[...]).astype(BF16).astype(F32)

    maps = conv(padded_bc, slice(0, 2 * STATE), taps_bc, offset_bc[...])
    maps_ref[...] = maps
    read_ref[...] = maps[:, STATE:]
    v = steps + step_bias[...]
    dt = jnp.maximum(v, 0.0) + jnp.log1p(jnp.exp(-jnp.abs(v)))
    log_decay = -jnp.exp(decay_log[...]) * dt
    cum_ref[...] = jnp.zeros_like(cum_ref)
    dt_ref[...] = jnp.zeros_like(dt_ref)
    lead_ref[...] = jnp.zeros_like(lead_ref)
    dt_ref[:, :heads] = dt
    row = lax.broadcasted_iota(jnp.int32, (SPAN, SPAN), 0)
    col = lax.broadcasted_iota(jnp.int32, (SPAN, SPAN), 1)
    lower = (row >= col).astype(F32)
    lead = jnp.zeros((1, heads), F32)
    ends, gone, write_t = [], [], []
    for s in range(spans):
        at = slice(s * SPAN, (s + 1) * SPAN)
        write_t.append(jnp.transpose(maps[at, :STATE].astype(F32)).astype(BF16))
        cum = jnp.dot(
            lower, log_decay[at], preferred_element_type=F32, precision=lax.Precision.HIGHEST
        )
        cum_ref[at, :heads] = cum
        lead_ref[at, :heads] = jnp.exp(cum + lead)
        last = cum[SPAN - 1 :, :]
        lead = lead + last
        ends.append(jnp.exp(last - cum) * dt[at])
        gone.append(jnp.exp(last))
    gone.append(jnp.exp(lead))

    gate_copy.wait()
    early = [
        pltpu.make_async_copy(source, target, sems.at[5 + k])
        for k, (source, target) in enumerate(
            (
                (maps_ref, maps_hbm), (read_ref, read_hbm), (cum_ref, cum_hbm), (dt_ref, dt_hbm),
                (lead_ref, lead_hbm),
            )
        )
    ]
    for copy in early:
        copy.start()
    half = rows // 2
    gate_ref[:half, :] = dot(tok[above : above + half, :], w_gate[...]).astype(BF16)
    for g in range(channels // BLOCK):
        at = slice(g * BLOCK, (g + 1) * BLOCK)
        here = [offset[t : t + 1, :] for t in range(at.start // LANES, at.stop // LANES)]
        x = conv(padded, at, taps, jnp.concatenate(here, axis=1))
        x_ref[:, at] = x
        running = jnp.zeros((STATE, BLOCK), F32)
        for s in range(spans):
            if s > 0:
                for t in range(tiles):
                    prior_ref[s - 1, g * tiles + t] = running[
                        :, t * LANES : (t + 1) * LANES
                    ].astype(BF16)

            def wide(value):
                return jnp.concatenate(
                    [
                        lane_pair(value[:, h : h + 1], value[:, h + 1 : h + 2])
                        for h in range(g * per, (g + 1) * per, 2)
                    ],
                    axis=1,
                )

            here = x[s * SPAN : (s + 1) * SPAN].astype(F32)
            local = dot(write_t[s], (here * wide(ends[s])).astype(BF16))
            running = wide(gone[s]) * running + local
        for t in range(tiles):
            to = g * tiles + t
            local_out[to] = running[:, t * LANES : (t + 1) * LANES].astype(BF16)
            h = g * per + 2 * t
            decay_out[to] = jnp.broadcast_to(
                lane_pair(gone[spans][:, h : h + 1], gone[spans][:, h + 1 : h + 2]), (8, LANES)
            )
    late = [
        pltpu.make_async_copy(x_ref, x_hbm, sems.at[10]),
        pltpu.make_async_copy(prior_ref, prior_hbm, sems.at[11]),
    ]
    for k in range(2):
        at = slice(k * half, (k + 1) * half)
        late.append(
            pltpu.make_async_copy(gate_ref.at[at, :], gate_out.at[at, :], sems.at[12 + k])
        )
    for copy in late[:3]:
        copy.start()
    gate_ref[half:, :] = dot(tok[above + half :, :], w_gate[...]).astype(BF16)
    late[3].start()
    for copy in early + late:
        copy.wait()


def first_part(edge, tokens, w_bc, w_step, w_in, w_gate, *small):
    rows, width = tokens.shape
    above = edge.shape[0]
    channels = w_in.shape[1]
    spans = rows // SPAN
    tiles = channels // LANES
    vmem = pl.BlockSpec(memory_space=pltpu.VMEM)
    hbm = pl.BlockSpec(memory_space=pltpu.HBM)
    kept = [
        ((rows, channels), BF16),
        ((rows, 2 * STATE), BF16),
        ((rows, STATE), BF16),
        ((rows, LANES), F32),
        ((rows, LANES), F32),
        ((rows, LANES), F32),
        ((spans - 1, tiles, STATE, LANES), BF16),
        ((rows, channels), BF16),
    ]
    return pl.pallas_call(
        first_kernel,
        in_specs=[vmem] + [hbm] * (5 + len(small)),
        out_specs=[hbm] * len(kept) + [vmem] * 2,
        out_shape=[pltpu.HBM(*a) for a in kept]
        + [
            jax.ShapeDtypeStruct((tiles, STATE, LANES), BF16),
            jax.ShapeDtypeStruct((tiles, 8, LANES), F32),
        ],
        scratch_shapes=[
            pltpu.VMEM((above + rows, width), BF16),
            pltpu.VMEM(w_bc.shape, BF16),
            pltpu.VMEM(w_step.shape, BF16),
            pltpu.VMEM(w_in.shape, BF16),
            pltpu.VMEM(w_gate.shape, BF16),
            pltpu.VMEM((above + rows, channels), F32),
            pltpu.VMEM((above + rows, 2 * STATE), F32),
            *[pltpu.VMEM(*a) for a in kept],
            *[pltpu.VMEM(a.shape, F32) for a in small],
            pltpu.SemaphoreType.DMA((20,)),
        ],
        compiler_params=pltpu.CompilerParams(vmem_limit_bytes=FIRST_LIMIT),
        cost_estimate=pl.CostEstimate(
            flops=2 * rows * width * (2 * channels + BLOCK + LANES),
            bytes_accessed=2 * width * (rows + 2 * channels + BLOCK),
            transcendentals=0,
        ),
        name="first",
    )(edge, *in_hbm(tokens, w_bc, w_step, w_in, w_gate, *small))


def inside_kernel(first, x_ref, bc_ref, cum_ref, dt_ref, prior_ref, skip_ref, out_ref):
    tiles = x_ref.shape[1] // LANES
    row = lax.broadcasted_iota(jnp.int32, (SPAN, SPAN), 0)
    col = lax.broadcasted_iota(jnp.int32, (SPAN, SPAN), 1)
    lane = lax.broadcasted_iota(jnp.int32, (SPAN, LANES), 1)
    write = bc_ref[:, :STATE]
    read = bc_ref[:, STATE:]
    scores = lax.dot_general(read, write, (((1,), (1,)), ((), ())), preferred_element_type=F32)
    scores = jnp.where(row >= col, scores, 0.0)
    cum = cum_ref[...]
    cum_t = jnp.transpose(cum)
    dt_t = jnp.transpose(dt_ref[...])
    grown = jnp.where(pl.program_id(0) + first > 0, jnp.exp(cum), 0.0)
    for t in range(tiles):
        at = slice(t * LANES, (t + 1) * LANES)
        x = x_ref[:, at]
        both = []
        for h in (2 * t, 2 * t + 1):
            gap = jnp.minimum(cum[:, h : h + 1] - cum_t[h : h + 1, :], 0.0)
            both.append((scores * jnp.exp(gap) * dt_t[h : h + 1, :]).astype(BF16))
        zero = jnp.zeros_like(x)
        stacked = jnp.concatenate(
            [jnp.where(lane < HEADDIM, x, zero), jnp.where(lane < HEADDIM, zero, x)], axis=0
        )
        total = dot(jnp.concatenate(both, axis=1), stacked)
        total = total + skip_ref[:, at] * x.astype(F32)
        scale = jnp.where(
            lane < HEADDIM, grown[:, 2 * t : 2 * t + 1], grown[:, 2 * t + 1 : 2 * t + 2]
        )
        out_ref[:, at] = total + scale * dot(read, prior_ref[0, t])


def inside(first, count, x, bc, cum, dt, prior, skip):
    channels = x.shape[1]
    tiles = channels // LANES
    at = lambda s: (s + first, 0)
    return pl.pallas_call(
        functools.partial(inside_kernel, first),
        grid=(count,),
        in_specs=[
            pl.BlockSpec((SPAN, channels), at),
            pl.BlockSpec((SPAN, 2 * STATE), at),
            pl.BlockSpec((SPAN, LANES), at),
            pl.BlockSpec((SPAN, LANES), at),
            pl.BlockSpec((1, tiles, STATE, LANES), lambda s: (jnp.maximum(s + first - 1, 0), 0, 0, 0)),
            pl.BlockSpec((1, channels), lambda s: (0, 0)),
        ],
        out_specs=pl.BlockSpec((SPAN, channels), lambda s: (s, 0)),
        out_shape=pltpu.HBM((count * SPAN, channels), F32),
        compiler_params=pltpu.CompilerParams(vmem_limit_bytes=INSIDE_LIMIT),
        cost_estimate=pl.CostEstimate(
            flops=1_000_000, bytes_accessed=1_000_000, transcendentals=0
        ),
        name="inside",
    )(*in_hbm(x, bc, cum, dt, prior), skip)


def split3(v):
    high = v.astype(BF16)
    rest = v - high.astype(F32)
    mid = rest.astype(BF16)
    return high, mid, (rest - mid.astype(F32)).astype(BF16)


def joined(message, rows):
    return (
        message[rows : rows + 1].astype(F32)
        + message[rows + 1 : rows + 2].astype(F32)
        + message[rows + 2 : rows + 3].astype(F32)
    )


def squares_rows(total):
    index = lax.broadcasted_iota(jnp.int32, (16, LANES), 0)
    high, mid, low = (p.astype(F32) for p in split3(total))
    out = jnp.where(index == 0, high, jnp.where(index == 1, mid, jnp.where(index == 2, low, 0.0)))
    return out.astype(BF16)


def ready_kernel(
    which, read_hbm, lead_hbm, low_hbm, high_hbm, gate_hbm, w_hbm,
    read_ref, lead_ref, local_ref, gate_ref, w_ref, sems,
):
    copies = rows_copies(
        which[0], (read_hbm, lead_hbm, gate_hbm), (read_ref, lead_ref, gate_ref), 0, sems
    )
    local = local_copies(which[0], low_hbm, high_hbm, local_ref, 0, sems.at[3])
    weights = pltpu.make_async_copy(w_hbm, w_ref, sems.at[4])
    weights.start()
    for copy in copies:
        copy.start()
    start_local(which[0], local)
    for copy in copies:
        copy.wait()
    local[0].wait()
    weights.wait()


def rows_copies(span, sources, targets, place, sems):
    at = pl.ds(pl.multiple_of(span * SPAN, SPAN), SPAN)
    return [
        pltpu.make_async_copy(
            source.at[at, :], target.at[pl.ds(place * SPAN, SPAN), :], sems.at[k]
        )
        for k, (source, target) in enumerate(zip(sources, targets))
    ]


def local_copies(span, low, high, target, place, sem):
    half = low.shape[0] // SPAN
    to = target.at[pl.ds(place * SPAN, SPAN), :]
    out = []
    for source, start in ((low, 0), (high, half)):
        row = pl.multiple_of(jnp.clip(span - start, 0, half - 1) * SPAN, SPAN)
        out.append(pltpu.make_async_copy(source.at[pl.ds(row, SPAN), :], to, sem))
    return out + [half]


def start_local(span, local):
    low, high, half = local
    pl.when(span < half)(low.start)
    pl.when(span >= half)(high.start)


def ready(which, read, lead, low, high, gate, weight):
    channels = gate.shape[1]
    vmem = pl.BlockSpec(memory_space=pltpu.VMEM)
    hbm = pl.BlockSpec(memory_space=pltpu.HBM)
    return pl.pallas_call(
        ready_kernel,
        in_specs=[pl.BlockSpec(memory_space=pltpu.SMEM)] + [hbm] * 6,
        out_specs=[vmem] * 5,
        out_shape=[
            jax.ShapeDtypeStruct((SPAN, STATE), BF16),
            jax.ShapeDtypeStruct((SPAN, LANES), F32),
            jax.ShapeDtypeStruct((SPAN, channels), F32),
            jax.ShapeDtypeStruct((SPAN, channels), BF16),
            jax.ShapeDtypeStruct(weight.shape, BF16),
        ],
        scratch_shapes=[pltpu.SemaphoreType.DMA((5,))],
        compiler_params=pltpu.CompilerParams(vmem_limit_bytes=SMALL_LIMIT),
        cost_estimate=pl.CostEstimate(flops=1000000, bytes_accessed=10**6, transcendentals=0),
        name="ready",
    )(which, *in_hbm(read, lead, low, high, gate, weight))


def tail_kernel(inner_total, has_rows, count, *refs):
    if has_rows:
        read_ref, lead_ref, local_ref, gate_ref, state_ref, norm_ref, w_ref, *outs, gated = refs
    else:
        (which, read_hbm, lead_hbm, low_hbm, high_hbm, gate_hbm, state_ref, norm_ref, w_hbm,
         *outs, read_ref, lead_ref, local_ref, gate_ref, gated, w_ref, sems, w_sems) = refs
        waits = []
        for i in range(count):
            copies = rows_copies(
                which[i], (read_hbm, lead_hbm, gate_hbm), (read_ref, lead_ref, gate_ref), i,
                sems.at[i],
            )
            local = local_copies(which[i], low_hbm, high_hbm, local_ref, i, sems.at[i, 3])
            for copy in copies:
                copy.start()
            start_local(which[i], local)
            waits.append(copies + local[:1])
        weights = []
        for side in range(2):
            at = slice(side * w_hbm.shape[1] // 2, (side + 1) * w_hbm.shape[1] // 2)
            weights.append(
                pltpu.make_async_copy(w_hbm.at[:, at], w_ref.at[:, at], w_sems.at[side])
            )
        weights[0].start()
    channels = local_ref.shape[1]
    tiles = channels // LANES
    width = w_ref.shape[1]
    side_tiles = width // 2 // LANES
    side_rows = side_tiles * SPAN
    sums = []
    for i in range(count):
        if not has_rows:
            for copy in waits[i]:
                copy.wait()
            if i == count - 1:
                weights[1].start()
        rows = slice(i * SPAN, (i + 1) * SPAN)
        read = read_ref[rows, :]
        lead = lead_ref[rows, :]
        squares = jnp.zeros((SPAN, LANES), F32)
        for t in range(tiles):
            at = slice(t * LANES, (t + 1) * LANES)
            scale = lane_pair(lead[:, 2 * t : 2 * t + 1], lead[:, 2 * t + 1 : 2 * t + 2])
            mixed = local_ref[rows, at] + scale * dot(read, state_ref[t])
            pre = mixed * silu(gate_ref[rows, at].astype(F32))
            squares = squares + pre * pre
            gated[rows, at] = (pre * norm_ref[:, at]).astype(BF16)
        total = jnp.sum(squares, axis=1, keepdims=True) * (1.0 / inner_total)
        sums.append(jnp.transpose(jnp.broadcast_to(total, (SPAN, LANES)))[:1])
    for j in range(width // BLOCK):
        if not has_rows and j * BLOCK % (width // 2) == 0:
            weights[j * BLOCK // (width // 2)].wait()
        part = dot(gated[...], w_ref[:, j * BLOCK : (j + 1) * BLOCK]).astype(outs[0].dtype)
        for u in range(BLOCK // LANES):
            side, tile = divmod(j * (BLOCK // LANES) + u, side_tiles)
            for i in range(count):
                outs[2 * i + side][tile * SPAN : (tile + 1) * SPAN, :] = part[
                    i * SPAN : (i + 1) * SPAN, u * LANES : (u + 1) * LANES
                ]
    for i in range(count):
        for side in range(2):
            out = outs[2 * i + side]
            if out.shape[0] == side_rows + 16:
                out[side_rows:, :] = squares_rows(sums[i])
    if len(outs) > 2 * count:
        outs[2 * count][...] = jnp.broadcast_to(sums[0], (8, LANES))


def tail(which, rows_in, state, norm, weight, squares_in):
    count = 1 if which is None else which.shape[0]
    channels, width = weight.shape
    side_rows = width // 2 // LANES * SPAN
    vmem = pl.BlockSpec(memory_space=pltpu.VMEM)
    hbm = pl.BlockSpec(memory_space=pltpu.HBM)
    shapes = []
    for i in range(count):
        for side in range(2):
            extra = 16 if (i, side) in squares_in else 0
            shapes.append(jax.ShapeDtypeStruct((side_rows + extra, LANES), BF16))
    if not squares_in:
        shapes.append(jax.ShapeDtypeStruct((8, LANES), F32))
    rows = count * SPAN
    gated = pltpu.VMEM((rows, channels), BF16)
    if which is None:
        in_specs, args, scratch = [vmem] * 4, list(rows_in), [gated]
    else:
        in_specs = [pl.BlockSpec(memory_space=pltpu.SMEM)] + [hbm] * 5
        args = [which, *in_hbm(*rows_in)]
        scratch = [
            pltpu.VMEM((rows, STATE), BF16),
            pltpu.VMEM((rows, LANES), F32),
            pltpu.VMEM((rows, channels), F32),
            pltpu.VMEM((rows, channels), BF16),
            gated,
            pltpu.VMEM(weight.shape, BF16),
            pltpu.SemaphoreType.DMA((count, 4)),
            pltpu.SemaphoreType.DMA((2,)),
        ]
    return pl.pallas_call(
        functools.partial(tail_kernel, HEADS * HEADDIM, which is None, count),
        in_specs=in_specs + [vmem] * 2 + [vmem if which is None else hbm],
        out_specs=[vmem] * len(shapes),
        out_shape=shapes,
        scratch_shapes=scratch,
        compiler_params=pltpu.CompilerParams(vmem_limit_bytes=TAIL_LIMIT),
        cost_estimate=pl.CostEstimate(flops=1000000, bytes_accessed=10**6, transcendentals=0),
    )(*args, state, norm, *([weight] if which is None else in_hbm(weight)))


def merge_kernel(a_ref, b_ref, b_squares, out_ref):
    rows = a_ref.shape[0] - 16
    out_ref[:rows, :] = (a_ref[:rows, :].astype(F32) + b_ref[:rows, :].astype(F32)).astype(BF16)
    total = joined(a_ref, rows)
    if b_squares:
        total = total + joined(b_ref, rows)
    out_ref[rows:, :] = squares_rows(total)


def merge(near, relayed, with_squares):
    vmem = pl.BlockSpec(memory_space=pltpu.VMEM)

    def body(a_ref, b_ref, out_ref):
        merge_kernel(a_ref, b_ref, with_squares, out_ref)

    return pl.pallas_call(
        body,
        in_specs=[vmem] * 2,
        out_specs=vmem,
        out_shape=jax.ShapeDtypeStruct(near.shape, BF16),
        compiler_params=pltpu.CompilerParams(vmem_limit_bytes=SMALL_LIMIT),
        cost_estimate=pl.CostEstimate(flops=1000000, bytes_accessed=10**6, transcendentals=0),
    )(near, relayed)


def final_kernel(own_l, own_r, own_sq, up, down, direct_l, direct_r, out_ref):
    rows = own_l.shape[0]
    tiles = rows // SPAN
    total = own_sq[0:1, :] + joined(up, rows) + joined(down, rows)
    scale = lax.rsqrt(total + 0.25)
    column = jnp.transpose(jnp.broadcast_to(scale, (LANES, SPAN)))
    for side, parts in enumerate(((own_l, up, direct_l), (own_r, direct_r, down))):
        for t in range(tiles):
            at = slice(t * SPAN, (t + 1) * SPAN)
            added = sum(p[at, :].astype(F32) for p in parts)
            to = slice((side * tiles + t) * LANES, (side * tiles + t + 1) * LANES)
            out_ref[:, to] = (added * column).astype(BF16)


def final(*parts):
    vmem = pl.BlockSpec(memory_space=pltpu.VMEM)
    tiles = parts[0].shape[0] // SPAN
    return pl.pallas_call(
        final_kernel,
        in_specs=[vmem] * len(parts),
        out_specs=vmem,
        out_shape=jax.ShapeDtypeStruct((SPAN, 2 * tiles * LANES), BF16),
        compiler_params=pltpu.CompilerParams(vmem_limit_bytes=SMALL_LIMIT),
        cost_estimate=pl.CostEstimate(flops=1000000, bytes_accessed=10**6, transcendentals=0),
        name="final",
    )(*parts)


def ring(value, axis, distance):
    size = lax.axis_size(axis)
    return lax.ppermute(value, axis, [(i, (i + distance) % size) for i in range(size)])


def pick(values, index):
    out = values[0]
    for k in range(1, len(values)):
        out = jnp.where(index == k, values[k], out)
    return out


def packed(state, decay):
    tiles = state.shape[0]
    high = decay.astype(BF16)
    low = (decay - high.astype(F32)).astype(BF16)
    spare = jnp.zeros((16 - 2 * tiles, LANES), BF16)
    return jnp.concatenate([state.astype(BF16).reshape(-1, LANES), high, low, spare], 0)


def unpacked(message, tiles):
    rows = message.shape[0] - 16
    state = message[:rows].reshape(tiles, rows // tiles, LANES).astype(F32)
    high = message[rows : rows + tiles].astype(F32)
    low = message[rows + tiles : rows + 2 * tiles].astype(F32)
    return state, (high + low)[:, None, :]


def incoming_state(local, decay):
    z_axis, y_axis, c_axis = SEQ
    z, y, c = (lax.axis_index(a) for a in SEQ)
    ys, zs = lax.axis_size(y_axis), lax.axis_size(z_axis)
    tiles = local.shape[0] // 2
    first = c == 0
    here = jnp.where(first, local[:tiles], local[tiles:])
    there = jnp.where(first, local[tiles:], local[:tiles])
    here_d = jnp.where(first, decay[:tiles], decay[tiles:])
    there_d = jnp.where(first, decay[tiles:], decay[:tiles])

    got = ring(packed(there, there_d), c_axis, 1)
    other, other_d = unpacked(got, tiles)
    here, here_d = here.astype(F32), here_d[:, None, :]
    s0, d0 = jnp.where(first, here, other), jnp.where(first, here_d, other_d)
    s1, d1 = jnp.where(first, other, here), jnp.where(first, other_d, here_d)
    chip, chip_d = d1 * s0 + s1, d0 * d1

    part = STATE // ys
    quarters = [chip[:, q * part : (q + 1) * part] for q in range(ys)]
    sent = [pick(quarters, (y + k) % ys) for k in range(ys)]
    messages = [packed(sent[k], chip_d[:, 0]) for k in range(1, ys)]
    got = [ring(message, y_axis, k + 1) for k, message in enumerate(messages)]
    got = [unpacked(message, tiles) for message in got]
    by_shift = [(sent[0], chip_d)] + got
    states = [pick([g[0] for g in by_shift], (y - q) % ys) for q in range(ys)]
    decays = [pick([g[1] for g in by_shift], (y - q) % ys) for q in range(ys)]
    plane, plane_d = states[0], decays[0]
    for q in range(1, ys):
        plane, plane_d = decays[q] * plane + states[q], decays[q] * plane_d

    message = packed(plane, plane_d[:, 0])
    got = [ring(message, z_axis, k) for k in range(1, zs)]
    got = [unpacked(message, tiles) for message in got]
    before = jnp.zeros_like(plane)
    for q in range(zs - 1):
        s = pick([g[0] for g in got], z - q - 1)
        d = pick([g[1] for g in got], z - q - 1)
        before = jnp.where(q < z, d * before + s, before)

    prefix = [before]
    for q in range(ys - 1):
        prefix.append(decays[q] * prefix[-1] + states[q])
    sent = [pick(prefix, (y + k) % ys).astype(BF16) for k in range(ys)]
    got = [sent[0]] + [ring(sent[k], y_axis, k) for k in range(1, ys)]
    chip_in = jnp.concatenate([pick(got, (y - q) % ys) for q in range(ys)], axis=1)
    second_in = (d0 * chip_in.astype(F32) + s0).astype(BF16)
    mine = jnp.where(first, chip_in, second_in)
    message = jnp.where(first, second_in, chip_in)
    got = ring(message, c_axis, 1)
    return jnp.concatenate([jnp.where(first, mine, got), jnp.where(first, got, mine)], axis=0)


def per_device(
    tokens,
    proj_inner,
    proj_gate,
    proj_bc,
    proj_step,
    conv_inner,
    conv_bc,
    offset_inner,
    offset_bc,
    step_bias,
    decay_log,
    skip_gain,
    norm_weight,
    out_weight,
):
    rows = tokens.shape[0]
    spans = rows // SPAN
    devices = lax.axis_size(SEQ)
    edge = lax.ppermute(tokens[rows - EDGE :], SEQ, [(i, i + 1) for i in range(devices - 1)])
    x, bc, read, cum, dt, lead, prior, gate, local, decay = first_part(
        edge, tokens, proj_bc, proj_step.T, proj_inner, proj_gate, conv_inner, offset_inner.reshape(-1, LANES),
        conv_bc, offset_bc[None], step_bias[None], decay_log[None],
    )
    state = incoming_state(local, decay[:, 0])
    skip = jnp.repeat(skip_gain, HEADDIM)[None]
    inner = []
    for part in range(2):
        half = spans // 2
        inner.append(inside(part * half, half, x, bc, cum, dt, prior, skip))

    head = lax.axis_index("head")
    size = lax.axis_size("head")

    def order(*which):
        return jnp.stack([(head + k) & (size - 1) for k in which]).astype(jnp.int32)

    norm = norm_weight[None]
    sources = (read, lead, *inner, gate)
    *far_rows, far_weight = ready(order(2), *sources, out_weight)

    def moved(value, distance):
        return ring(value, "head", distance)

    far_left, far_right = tail(None, far_rows, state, norm, far_weight, {(0, 0), (0, 1)})
    relay_up = moved(far_left, 1)
    relay_down = moved(far_right, -1)
    next_left, next_right, last_left, last_right = tail(
        order(1, 3), sources, state, norm, out_weight, {(0, 0), (1, 1)}
    )
    direct_up = moved(next_right, 1)
    direct_down = moved(last_left, -1)
    own_left, own_right, own_squares = tail(order(0), sources, state, norm, out_weight, set())
    up = merge(next_left, relay_up, True)
    up = moved(up, 1)
    down = merge(last_right, relay_down, False)
    down = moved(down, -1)
    return final(own_left, own_right, own_squares, up, down, direct_down, direct_up)


def solution(mesh):
    torus = Mesh(
        mesh.devices.reshape(4, 4, 2, mesh.shape["head"]), ("seq_0", "seq_1", "seq_2", "head")
    )
    return jax.shard_map(
        per_device,
        mesh=torus,
        in_specs=(
            P(SEQ, None),
            P(None, "head"),
            P(None, "head"),
            P(),
            P(None, "head"),
            P(None, "head"),
            P(),
            P("head"),
            P(),
            P("head"),
            P("head"),
            P("head"),
            P("head"),
            P("head", None),
        ),
        out_specs=P(SEQ_HEAD, None),
        check_vma=False,
    )
```
